128 devices in a mesh: lat: 32 (over z, y, core), ch: 4 (over x).
Axes of the slice: x: 4, y: 4, z: 4, core: 2. Of those that a mesh axis runs over, the one named last changes fastest.
Arguments:
- state: float32 [1, 96, 180, 768], P(None, 'lat', None, 'ch'), may hold values from -30 to 30
- norm_gains: bfloat16 [2, 768], P(None, 'ch'), may hold values from 0.099609375 to 1.8984375
- channel_biases: bfloat16 [3, 768], P(None, 'ch'), may hold values from -2 to 2
- filter_in: float32 [2, 8, 96, 96], P(None, 'ch'), may hold values from -0.4375 to 0.4375
- filter_in_bias: float32 [2, 8, 96], P(None, 'ch'), may hold values from -2 to 2
- filter_out: float32 [2, 8, 96, 96], P(None, 'ch'), may hold values from -0.4375 to 0.4375
- filter_out_bias: float32 [2, 8, 96], P(None, 'ch'), may hold values from -2 to 2
- up_weight: bfloat16 [768, 3072], P(None, 'ch'), may hold values from -0.21875 to 0.21875
- up_bias: bfloat16 [3072], P('ch'), may hold values from -2 to 2
- down_weight: bfloat16 [3072, 768], P('ch'), may hold values from -0.109375 to 0.109375
Outputs:
- final_state: float32 [1, 96, 180, 768], P(None, 'lat', None, 'ch')
The draws below stay inside these ranges and needn't reach their ends.
All inputs are finite; a program needn't handle non-finite values.
Results may differ from the reference program's by a relative error of at most 0.0012.
Values may be sent and summed in bfloat16 or wider, within the bound.
A program may use at most 128 MiB of HBM per device.

```python
import math
import jax
import jax.numpy as jnp
from jax import lax

D = 768
FF = 3072
W = 180
NB = 8
M = 64
STEPS = 4
B = 1
H = 96
BS = 96


def draw_state(key, part):
    subkeys = jax.random.split(key, 3)
    channel_pos = jnp.arange(D).astype(jnp.float32) / D
    column_scale = 0.3 * jnp.exp(jax.random.uniform(subkeys[0], (D,), jnp.float32) * math.log(10.0)) * jnp.exp(channel_pos * 0.5 * math.log(3.0))
    channel_shift = 0.2 + 0.6 * channel_pos + 0.3 * jax.random.normal(subkeys[1], (D,), jnp.float32)
    value = jax.random.normal(subkeys[2], (B, H, W, D), jnp.float32) * column_scale + channel_shift
    return jnp.clip(value, -30.0, 30.0)


def block_scale(own_key, shape, cuts, smallest, high):
    level = 1.0
    for dim, shards_of in cuts:
        steps = jax.random.uniform(jax.random.fold_in(jax.random.fold_in(own_key, 6), dim), (shards_of,), jnp.float32, smallest / len(cuts), high / len(cuts))
        level = level * jnp.repeat(jnp.exp(steps), shape[dim] // shards_of).reshape((-1,) + (1,) * (len(shape) - 1 - dim))
    return level


def scatter_about(own_key, dims, scale, most, cuts=(), kind=jnp.bfloat16):
    values = scale * jax.random.normal(own_key, dims, jnp.float32)
    if cuts:
        values = values * block_scale(own_key, dims, cuts, -0.22, 0.18)
    return jnp.clip(values, -most, most).astype(kind)


def setup_inputs(seed: int = 0) -> dict:
    key_list = jax.random.split(jax.random.key(seed), 11)
    state = draw_state(jax.random.fold_in(key_list[10], 71), 0)
    norm_gains = jnp.clip(1.0 + 0.18 * jax.random.normal(key_list[1], (2, D), jnp.float32), 0.099609375, 1.8984375).astype(jnp.bfloat16)
    channel_biases = scatter_about(key_list[2], (3, D), 0.3, 2.0, ((1, 4),))
    filter_in = scatter_about(key_list[3], (2, NB, BS, BS), (2 * BS) ** -0.5, 0.4375, ((1, 4),), jnp.float32)
    filter_in_bias = scatter_about(key_list[4], (2, NB, BS), 0.3, 2.0, ((1, 4),), jnp.float32)
    filter_out = scatter_about(key_list[5], (2, NB, BS, BS), (2 * BS) ** -0.5, 0.4375, ((1, 4),), jnp.float32)
    filter_out_bias = scatter_about(key_list[6], (2, NB, BS), 0.3, 2.0, ((1, 4),), jnp.float32)
    up_weight = scatter_about(key_list[7], (D, FF), D ** -0.5, 0.21875, ((1, 4),))
    up_bias = scatter_about(key_list[8], (FF,), 0.3, 2.0, ((0, 4),))
    down_weight = scatter_about(key_list[9], (FF, D), FF ** -0.5, 0.109375, ((0, 4),))
    return dict(state=state, norm_gains=norm_gains, channel_biases=channel_biases, filter_in=filter_in, filter_in_bias=filter_in_bias, filter_out=filter_out, filter_out_bias=filter_out_bias, up_weight=up_weight, up_bias=up_bias, down_weight=down_weight)


EPS = 1e-05
SHRINK = 0.01
HIGH = lax.Precision.HIGHEST

def longitude_tables(width, modes):
    column = jnp.arange(width, dtype=jnp.int32)[:, None]
    order = jnp.arange(modes, dtype=jnp.int32)[None, :]
    angle = 2.0 * math.pi / width * (column * order % width).astype(jnp.float32)
    doubled = jnp.where(order == 0, 1.0, 2.0).astype(jnp.float32)
    return (jnp.cos(angle), jnp.sin(angle), jnp.cos(angle) * doubled, jnp.sin(angle) * doubled)

def latitude_tables(height):
    column = jnp.arange(height, dtype=jnp.int32)[:, None]
    order = jnp.arange(height, dtype=jnp.int32)[None, :]
    angle = 2.0 * math.pi / height * (column * order % height).astype(jnp.float32)
    return (jnp.cos(angle), jnp.sin(angle))

def layer_norm(values, gain, shift):
    mean = lax.optimization_barrier(jnp.sum(values, -1, keepdims=True)) / values.shape[-1]
    spread = lax.optimization_barrier(jnp.sum(values * values, -1, keepdims=True)) / values.shape[-1] - mean * mean
    return (values - mean) * lax.rsqrt(spread + EPS) * gain + shift

def soft_shrink(values):
    return jnp.where(values > SHRINK, values - SHRINK, jnp.where(values < -SHRINK, values + SHRINK, 0.0))

def block_apply(left, matrix):
    return jnp.einsum('bkmnj,nji->bkmni', left, matrix, precision=HIGH)

def spectral_mlp(real_part, imag_part, filter_in, filter_in_bias, filter_out, filter_out_bias):
    shape = real_part.shape
    blocks = filter_in.shape[1]
    size = filter_in.shape[2]
    real_blocks = real_part.reshape(shape[:-1] + (blocks, size))
    imag_blocks = imag_part.reshape(shape[:-1] + (blocks, size))
    first_real = jax.nn.relu(block_apply(real_blocks, filter_in[0]) - block_apply(imag_blocks, filter_in[1]) + filter_in_bias[0])
    first_imag = jax.nn.relu(block_apply(imag_blocks, filter_in[0]) + block_apply(real_blocks, filter_in[1]) + filter_in_bias[1])
    second_real = block_apply(first_real, filter_out[0]) - block_apply(first_imag, filter_out[1]) + filter_out_bias[0]
    second_imag = block_apply(first_imag, filter_out[0]) + block_apply(first_real, filter_out[1]) + filter_out_bias[1]
    return (soft_shrink(second_real).reshape(shape), soft_shrink(second_imag).reshape(shape))

def spectral_filter(normed, filter_in, filter_in_bias, filter_out, filter_out_bias):
    height = normed.shape[1]
    width = normed.shape[2]
    lon_cos, lon_sin, back_cos, back_sin = longitude_tables(width, M)
    lat_cos, lat_sin = latitude_tables(height)
    scale = 1.0 / math.sqrt(height * width)
    real_lon = jnp.einsum('bhwd,wm->bhmd', normed, lon_cos, precision=HIGH)
    imag_lon = -jnp.einsum('bhwd,wm->bhmd', normed, lon_sin, precision=HIGH)
    real_spec = (jnp.einsum('kh,bhmd->bkmd', lat_cos, real_lon, precision=HIGH) + jnp.einsum('kh,bhmd->bkmd', lat_sin, imag_lon, precision=HIGH)) * scale
    imag_spec = (jnp.einsum('kh,bhmd->bkmd', lat_cos, imag_lon, precision=HIGH) - jnp.einsum('kh,bhmd->bkmd', lat_sin, real_lon, precision=HIGH)) * scale
    out_real, out_imag = spectral_mlp(real_spec, imag_spec, filter_in, filter_in_bias, filter_out, filter_out_bias)
    real_rows = jnp.einsum('kh,bkmd->bhmd', lat_cos, out_real, precision=HIGH) - jnp.einsum('kh,bkmd->bhmd', lat_sin, out_imag, precision=HIGH)
    imag_rows = jnp.einsum('kh,bkmd->bhmd', lat_cos, out_imag, precision=HIGH) + jnp.einsum('kh,bkmd->bhmd', lat_sin, out_real, precision=HIGH)
    back = jnp.einsum('bhmd,wm->bhwd', real_rows, back_cos, precision=HIGH) - jnp.einsum('bhmd,wm->bhwd', imag_rows, back_sin, precision=HIGH)
    return back * scale

def reference(state, norm_gains, channel_biases, filter_in, filter_in_bias, filter_out, filter_out_bias, up_weight, up_bias, down_weight):
    gains = norm_gains.astype(jnp.float32)
    shifts = channel_biases.astype(jnp.float32)
    values = state
    for step_index in range(STEPS):
        normed = layer_norm(values, gains[0], shifts[0])
        values = values + spectral_filter(normed, filter_in, filter_in_bias, filter_out, filter_out_bias) + normed
        normed_two = layer_norm(values, gains[1], shifts[1]).astype(jnp.bfloat16)
        flat = normed_two.reshape(-1, normed_two.shape[-1])
        pre = jnp.dot(flat, up_weight, preferred_element_type=jnp.float32) + up_bias.astype(jnp.float32)
        hidden = jax.nn.gelu(pre, approximate=False).astype(jnp.bfloat16)
        mixed = jnp.dot(hidden, down_weight, preferred_element_type=jnp.float32) + shifts[2]
        values = values + mixed.reshape(values.shape)
    return values
```

```python
import math

import jax
import jax.numpy as jnp
import numpy as np
from jax import lax
from jax.experimental import pallas as pl
from jax.experimental.pallas import tpu as pltpu
from jax.sharding import PartitionSpec as P

D = 768
FF = 3072
W = 180
R = 192
H = 96
M = 64
NB = 8
BS = 96
STEPS = 4
NL = 32
NC = 4
ND = NL * NC
OWN = 3
G = 16
SCALE = 1.0 / math.sqrt(H * W)
EPS = 1e-05
SHRINK = 0.01
MESH = pl.DeviceIdType.MESH
BF = jnp.bfloat16
F32 = jnp.float32


def tables():
    modes = np.arange(M)
    w = np.arange(W)
    ang = 2.0 * np.pi / W * ((w[:, None] * modes[None, :]) % W)
    c, s = np.cos(ang), np.sin(ang)
    dbl = np.where(modes == 0, 1.0, 2.0)
    fwd = np.zeros((G, 2, 4, R))
    fwd[:, 0, :, :W] = c.T.reshape(G, 4, W)
    fwd[:, 1, :, :W] = -s.T.reshape(G, 4, W)
    back = np.zeros((R, G, 2, 4))
    back[:W, :, 0, :] = (c * dbl).reshape(W, G, 4)
    back[:W, :, 1, :] = -(s * dbl).reshape(W, G, 4)
    h = np.arange(H)
    ang = 2.0 * np.pi / H * ((h[:, None] * h[None, :]) % H)
    c, s = np.cos(ang), np.sin(ang)
    lat = np.zeros((2, H, H, 2))
    lat[0, :, :, 0] = c
    lat[0, :, :, 1] = s
    lat[1, :, :, 0] = -s
    lat[1, :, :, 1] = c
    lat = lat.reshape(192, 192)
    fwd, back = halves(fwd.reshape(128, R)), halves(back.reshape(R, 128))
    return (
        np.concatenate([fwd[0], fwd[1], fwd[0]], axis=1),
        np.concatenate(back, axis=1),
        np.stack(halves(lat)),
        np.stack(halves(lat.T)),
    )


def halves(a):
    a = np.asarray(a, np.float32)
    hi = a.astype(BF)
    return hi, (a - hi.astype(np.float32)).astype(BF)


def parts(v):
    hi = v.astype(BF)
    return hi, (v - hi.astype(F32)).astype(BF)


def spread_out(t_ref, o_ref):
    def iota(shape, dim):
        return lax.broadcasted_iota(jnp.int32, shape, dim)

    one = lambda m: jnp.where(m, 1.0, 0.0).astype(BF)
    rows = one(iota((768, 192), 0) // 4 == iota((768, 192), 1))
    cols = one(iota((192, 768), 1) // 4 == iota((192, 768), 0))
    keep = lax.rem(iota((192, 768), 0), 4) == lax.rem(iota((192, 768), 1), 4)
    for half in range(2):
        tall = jnp.dot(rows, t_ref[half], preferred_element_type=F32).astype(BF)
        for j in range(4):
            wide = jnp.dot(tall[j * 192:(j + 1) * 192], cols, preferred_element_type=F32)
            o_ref[half, j * 192:(j + 1) * 192, :] = jnp.where(keep, wide, 0.0).astype(BF)


def norm(v, gain, shift):
    mean = jnp.sum(v, -1, keepdims=True) / D
    spread = jnp.sum(v * v, -1, keepdims=True) / D - mean * mean
    return (v - mean) * lax.rsqrt(spread + EPS) * gain + shift


def kernel(
    state, small, fin, finb, fout, foutb, up, down, fwd, back, t_to, t_fro,
    out,
    xin, smalls, x, nb, fsend, frecv, bsend, brecv, w1, b1, w2, b2, par, hid, lat_to, lat_fro, n3,
    in_s, in_r, sm_s, sm_r, f_s, f_r, b_s, b_r, o_s, o_r,
):
    l = lax.axis_index("lat")
    c = lax.axis_index("ch")
    me = l * NC + c
    row = l * OWN + c
    blk = lax.rem(l, 2)
    owner = c < OWN

    def to_owner(i):
        return (
            pltpu.make_async_remote_copy(
                state.at[i], xin.at[c], in_s.at[i], in_r.at[c],
                device_id=(l, i), device_id_type=MESH),
            pltpu.make_async_remote_copy(
                small, smalls.at[c], sm_s.at[i], sm_r.at[c],
                device_id=(l, i), device_id_type=MESH),
        )

    for i in range(OWN):
        @pl.when(c != i)
        def _(i=i):
            a, b = to_owner(i)
            a.start()
            b.start()

        @pl.when(c == i)
        def _(i=i):
            pltpu.make_async_copy(state.at[i], xin.at[i], in_r.at[i]).start()
            pltpu.make_async_copy(small, smalls.at[i], sm_r.at[i]).start()

    for w_ref, b_ref, src, bsrc in ((w1, b1, fin, finb), (w2, b2, fout, foutb)):
        w_ref[...] = jnp.zeros_like(w_ref)
        b_ref[...] = jnp.zeros_like(b_ref)
        for at, re, im in zip((0, 256), parts(src[0, blk]), parts(src[1, blk])):
            w_ref[at:at + BS, 0:BS] = re
            w_ref[at:at + BS, 128:128 + BS] = im
            w_ref[at + 128:at + 128 + BS, 0:BS] = -im
            w_ref[at + 128:at + 128 + BS, 128:128 + BS] = re
        w_ref[512:768, :] = w_ref[0:256, :]
        b_ref[:, 0:BS] = bsrc[0, pl.ds(blk, 1), :]
        b_ref[:, 128:128 + BS] = bsrc[1, pl.ds(blk, 1), :]

    spread_out(t_to, lat_to)
    spread_out(t_fro, lat_fro)

    @pl.when(owner)
    def _():
        for j in range(NC):
            pltpu.make_async_copy(xin.at[j], xin.at[j], in_r.at[j]).wait()
            pltpu.make_async_copy(smalls.at[j], smalls.at[j], sm_r.at[j]).wait()
        par[0:5, :] = jnp.concatenate([smalls[j, 0:5, 0:192] for j in range(NC)], axis=1)
        x[0:W, :] = jnp.concatenate([xin[j] for j in range(NC)], axis=1)
        x[W:R, :] = jnp.zeros((R - W, D), F32)
        fsend[...] = jnp.zeros_like(fsend)

    for i in range(OWN):
        @pl.when(c != i)
        def _(i=i):
            a, b = to_owner(i)
            a.wait_send()
            b.wait_send()

    def step(s, carry):
        @pl.when(owner)
        def _():
            v = x[...]
            n = norm(v, par[0:1, :], par[2:3, :])
            x[...] = v + n
            hi, lo = parts(n)
            n3[0:R, :] = hi
            n3[R:2 * R, :] = hi
            n3[2 * R:3 * R, :] = lo
            lon = jnp.dot(fwd[...], n3[...], preferred_element_type=F32)
            for b in range(NB):
                fsend[b, :, :, 0:BS] = lon[:, b * BS:(b + 1) * BS].reshape(G, 8, BS).astype(BF)

            def send(i, carry):
                d = lax.rem(me + i, ND)
                dl, dc = d // NC, lax.rem(d, NC)
                src = fsend.at[2 * dc + lax.rem(dl, 2), dl // 2]

                pltpu.make_async_remote_copy(
                    src, frecv.at[row], f_s, f_r, device_id=(dl, dc), device_id_type=MESH).start()
                return carry

            lax.fori_loop(1, ND, send, 0)
            pltpu.make_async_copy(
                fsend.at[2 * c + blk, l // 2], frecv.at[row], f_r).start()

        pltpu.make_async_copy(frecv, frecv, f_r).wait()
        got = frecv[...].reshape(H * 8, 128)
        spec = jnp.dot(lat_to[0], got, preferred_element_type=F32)
        spec = (spec + jnp.dot(lat_to[1], got, preferred_element_type=F32)) * SCALE
        spec = jnp.concatenate([spec[0:384], spec[384:768]], axis=1)
        hi, lo = parts(spec)
        first = jnp.dot(jnp.concatenate([hi, hi, lo], axis=1), w1[...], preferred_element_type=F32) + b1[...]
        hi, lo = parts(jnp.maximum(first, 0.0))
        second = jnp.dot(jnp.concatenate([hi, hi, lo], axis=1), w2[...], preferred_element_type=F32) + b2[...]
        second = jnp.where(second > SHRINK, second - SHRINK,
                           jnp.where(second < -SHRINK, second + SHRINK, 0.0))
        hi, lo = parts(jnp.concatenate([second[:, 0:128], second[:, 128:256]], axis=0))
        both = jnp.dot(lat_fro[0], jnp.concatenate([hi, lo], axis=1), preferred_element_type=F32)
        rows = jnp.dot(lat_fro[1], hi, preferred_element_type=F32)
        rows = (rows + both[:, 0:128] + both[:, 128:256]).astype(BF)
        bsend[...] = rows.reshape(H, 8, 128)

        def sendb(i, carry):
            dl = lax.rem(l + i, NL)
            for dc in range(OWN):
                @pl.when(jnp.logical_or(dl != l, c != dc))
                def _():
                    pltpu.make_async_remote_copy(
                        bsend.at[dl * OWN + dc], brecv.at[2 * c + blk, l // 2], b_s, b_r,
                        device_id=(dl, dc), device_id_type=MESH).start()
            return carry

        lax.fori_loop(0, NL, sendb, 0)

        @pl.when(owner)
        def _():
            pltpu.make_async_copy(bsend.at[row], brecv.at[2 * c + blk, l // 2], b_r).start()
            pltpu.make_async_copy(brecv, brecv, b_r).wait()
            packed = jnp.concatenate(
                [brecv[b].reshape(128, 128)[:, 0:BS].astype(F32) for b in range(NB)], axis=1).astype(BF)
            packed = jnp.concatenate([packed, packed], axis=0)
            v = x[...] + jnp.dot(back[...], packed, preferred_element_type=F32) * SCALE
            x[...] = v
            nb[...] = norm(v, par[1:2, :], par[3:4, :]).astype(BF)
            for q in range(NC):
                for j in range(3):
                    pre = jnp.dot(nb[...], up[:, q * 768 + j * 256:q * 768 + (j + 1) * 256], preferred_element_type=F32)
                    pre = pre + smalls[q, 5:6, j * 256:(j + 1) * 256]
                    act = 0.5 * pre * (1.0 + lax.erf(pre * math.sqrt(0.5)))
                    hid[:, q * 768 + j * 256:q * 768 + (j + 1) * 256] = act.astype(BF)
            for j in range(3):
                cols = slice(j * 256, (j + 1) * 256)
                mixed = jnp.dot(hid[...], down[:, cols], preferred_element_type=F32)
                x[:, cols] = x[:, cols] + mixed + par[4:5, cols]
            pltpu.make_async_copy(fsend.at[0:7], fsend.at[0:7], f_s).wait()
            pltpu.make_async_copy(fsend.at[7, 0:15], fsend.at[7, 0:15], f_s).wait()
            pltpu.make_async_copy(bsend.at[0:95], bsend.at[0:95], b_s).wait()

        @pl.when(jnp.logical_not(owner))
        def _():
            pltpu.make_async_copy(bsend, bsend, b_s).wait()

        return carry

    lax.fori_loop(0, STEPS, step, 0)

    @pl.when(owner)
    def _():
        for j in range(NC):
            xin[j] = x[0:W, j * 192:(j + 1) * 192]

        for j in range(NC):
            @pl.when(c != j)
            def _(j=j):
                pltpu.make_async_remote_copy(
                    xin.at[j], out.at[c], o_s.at[j], o_r.at[c],
                    device_id=(l, j), device_id_type=MESH).start()

            @pl.when(c == j)
            def _(j=j):
                pltpu.make_async_copy(xin.at[j], out.at[c], o_r.at[c]).start()

    for i in range(OWN):
        pltpu.make_async_copy(out.at[i], out.at[i], o_r.at[i]).wait()

    @pl.when(owner)
    def _():
        for j in range(NC):
            @pl.when(c != j)
            def _(j=j):
                pltpu.make_async_copy(xin.at[j], xin.at[j], o_s.at[j]).wait()


def local(
    state, norm_gains, channel_biases, filter_in, filter_in_bias, filter_out, filter_out_bias,
    up_weight, up_bias, down_weight,
):
    up = lax.all_gather(up_weight, "ch", axis=1, tiled=True)
    down = lax.all_gather(down_weight, "ch", axis=0, tiled=True)
    small = jnp.zeros((8, D), F32)
    small = small.at[0:2, 0:192].set(norm_gains.astype(F32))
    small = small.at[2:5, 0:192].set(channel_biases.astype(F32))
    small = small.at[5, :].set(up_bias.astype(F32))
    fwd, back, t_to, t_fro = tables()
    vm = pl.BlockSpec(memory_space=pltpu.VMEM)
    anyspace = pl.BlockSpec(memory_space=pl.ANY)
    sem = pltpu.SemaphoreType.DMA
    result = pl.pallas_call(
        kernel,
        out_shape=jax.ShapeDtypeStruct((OWN, W, 192), F32),
        in_specs=[anyspace, vm] + [vm] * 10,
        out_specs=vm,
        scratch_shapes=[
            pltpu.VMEM((NC, W, 192), F32),
            pltpu.VMEM((NC, 8, D), F32),
            pltpu.VMEM((R, D), F32),
            pltpu.VMEM((R, D), BF),
            pltpu.VMEM((NB, G, 8, 128), BF),
            pltpu.VMEM((H, 8, 128), BF),
            pltpu.VMEM((H, 8, 128), BF),
            pltpu.VMEM((NB, G, 8, 128), BF),
            pltpu.VMEM((768, 256), BF),
            pltpu.VMEM((1, 256), F32),
            pltpu.VMEM((768, 256), BF),
            pltpu.VMEM((1, 256), F32),
            pltpu.VMEM((8, D), F32),
            pltpu.VMEM((R, FF), BF),
            pltpu.VMEM((2, 768, 768), BF),
            pltpu.VMEM((2, 768, 768), BF),
            pltpu.VMEM((3 * R, D), BF),
            sem((OWN,)), sem((NC,)), sem((OWN,)), sem((NC,)),
            sem, sem, sem, sem, sem((NC,)), sem((OWN,)),
        ],
        compiler_params=pltpu.CompilerParams(
            has_side_effects=True, vmem_limit_bytes=50 * 1024 * 1024),
        name="rollout",
    )(
        state[0], small, filter_in, filter_in_bias, filter_out, filter_out_bias,
        up, down, jnp.asarray(fwd), jnp.asarray(back), jnp.asarray(t_to), jnp.asarray(t_fro),
    )
    return result[None]


def solution(mesh):
    placed = (
        P(None, "lat", None, "ch"),
        P(None, "ch"),
        P(None, "ch"),
        P(None, "ch", None, None),
        P(None, "ch", None),
        P(None, "ch", None, None),
        P(None, "ch", None),
        P(None, "ch"),
        P("ch"),
        P("ch", None),
    )
    return jax.shard_map(
        local, mesh=mesh, in_specs=placed, out_specs=P(None, "lat", None, "ch"), check_vma=False
    )
```

```python
import math

import jax
import jax.numpy as jnp
import numpy as np
from jax import lax
from jax.experimental import pallas as pl
from jax.experimental.pallas import tpu as pltpu
from jax.sharding import PartitionSpec as P

D = 768
FF = 3072
W = 180
R = 192
H = 96
M = 64
NB = 8
BS = 96
STEPS = 4
NL = 32
NC = 4
ND = NL * NC
OWN = 3
G = 16
SCALE = 1.0 / math.sqrt(H * W)
EPS = 1e-05
SHRINK = 0.01
MESH = pl.DeviceIdType.MESH
BF = jnp.bfloat16
F32 = jnp.float32


def tables():
    modes = np.arange(M)
    w = np.arange(W)
    ang = 2.0 * np.pi / W * ((w[:, None] * modes[None, :]) % W)
    c, s = np.cos(ang), np.sin(ang)
    dbl = np.where(modes == 0, 1.0, 2.0)
    fwd = np.zeros((G, 2, 4, R))
    fwd[:, 0, :, :W] = c.T.reshape(G, 4, W)
    fwd[:, 1, :, :W] = -s.T.reshape(G, 4, W)
    back = np.zeros((R, G, 2, 4))
    back[:W, :, 0, :] = (c * dbl).reshape(W, G, 4)
    back[:W, :, 1, :] = -(s * dbl).reshape(W, G, 4)
    h = np.arange(H)
    ang = 2.0 * np.pi / H * ((h[:, None] * h[None, :]) % H)
    c, s = np.cos(ang), np.sin(ang)
    lat = np.zeros((2, H, H, 2))
    lat[0, :, :, 0] = c
    lat[0, :, :, 1] = s
    lat[1, :, :, 0] = -s
    lat[1, :, :, 1] = c
    lat = lat.reshape(192, 192)
    fwd, back = halves(fwd.reshape(128, R)), halves(back.reshape(R, 128))
    return (
        np.concatenate([fwd[0], fwd[1], fwd[0]], axis=1),
        np.concatenate(back, axis=1),
        np.stack(halves(lat)),
        np.stack(halves(lat.T)),
    )


def halves(a):
    a = np.asarray(a, np.float32)
    hi = a.astype(BF)
    return hi, (a - hi.astype(np.float32)).astype(BF)


def parts(v):
    hi = v.astype(BF)
    return hi, (v - hi.astype(F32)).astype(BF)


def spread_out(t_ref, o_ref):
    def iota(shape, dim):
        return lax.broadcasted_iota(jnp.int32, shape, dim)

    one = lambda m: jnp.where(m, 1.0, 0.0).astype(BF)
    rows = one(iota((768, 192), 0) // 4 == iota((768, 192), 1))
    cols = one(iota((192, 768), 1) // 4 == iota((192, 768), 0))
    keep = lax.rem(iota((192, 768), 0), 4) == lax.rem(iota((192, 768), 1), 4)
    for half in range(2):
        tall = jnp.dot(rows, t_ref[half], preferred_element_type=F32).astype(BF)
        for j in range(4):
            wide = jnp.dot(tall[j * 192:(j + 1) * 192], cols, preferred_element_type=F32)
            o_ref[half, j * 192:(j + 1) * 192, :] = jnp.where(keep, wide, 0.0).astype(BF)


def norm(v, gain, shift):
    mean = jnp.sum(v, -1, keepdims=True) / D
    spread = jnp.sum(v * v, -1, keepdims=True) / D - mean * mean
    return (v - mean) * lax.rsqrt(spread + EPS) * gain + shift


def kernel(
    state, small, fin, finb, fout, foutb, up, down, fwd, back, t_to, t_fro,
    out,
    xin, smalls, x, nb, fsend, frecv, bsend, brecv, w1, b1, w2, b2, par, hid, lat_to, lat_fro, n3, wts,
    in_s, in_r, sm_s, sm_r, f_s, f_r, b_s, b_r, o_s, o_r,
    own_r, wa_s, wa_r, wb_s, wb_r, wc_s, wc_r, wd_s, wd_r,
):
    l = lax.axis_index("lat")
    c = lax.axis_index("ch")
    me = l * NC + c
    row = l * OWN + c
    blk = lax.rem(l, 2)
    owner = c < OWN

    def to_owner(i):
        return (
            pltpu.make_async_remote_copy(
                state.at[i], xin.at[c], in_s.at[i], in_r.at[c],
                device_id=(l, i), device_id_type=MESH),
            pltpu.make_async_remote_copy(
                small, smalls.at[c], sm_s.at[i], sm_r.at[c],
                device_id=(l, i), device_id_type=MESH),
        )

    for i in range(OWN):
        @pl.when(c != i)
        def _(i=i):
            a, b = to_owner(i)
            a.start()
            b.start()

        @pl.when(c == i)
        def _(i=i):
            pltpu.make_async_copy(state.at[i], xin.at[i], in_r.at[i]).start()
            pltpu.make_async_copy(small, smalls.at[i], sm_r.at[i]).start()

    k = lax.rem(l, 2)
    cy = lax.rem(l // 2, 4)
    cz = l // 8
    py, pz = lax.rem(cy, 2), lax.rem(cz, 2)
    mine = 2 * pz + py
    at_y, at_z, at_d = 2 * pz + 1 - py, 2 * (1 - pz) + py, 2 * (1 - pz) + 1 - py
    shards = (up, down)

    def chip(dy, dz, core):
        return (lax.rem(cz + dz + 4, 4) * 4 + lax.rem(cy + dy + 4, 4)) * 2 + core

    def foreign(j):
        return lax.rem(c + 1 + j, NC)

    def take(sems, *at):
        ref = wts.at[0, 0, 0, pl.ds(0, 3)]
        pltpu.make_async_copy(ref, ref, sems.at[at]).wait()

    def pass_on(m, piece, axis, s_sem, r_sem):
        for j in range(3):
            for half, sign in ((0, 1), (1, -1)):
                ref = wts.at[foreign(j), m, k, piece, half]
                to = chip(sign, 0, k) if axis == 0 else chip(0, sign, k)
                pltpu.make_async_remote_copy(
                    ref, ref, s_sem, r_sem, device_id=(to, c), device_id_type=MESH).start()

    def share(m, piece, stage):
        for j in range(3):
            ref = wts.at[foreign(j), m, k, piece]
            pltpu.make_async_remote_copy(
                ref, ref, wd_s, wd_r.at[stage, m], device_id=(chip(0, 0, 1 - k), c), device_id_type=MESH).start()

    for m in range(2):
        for i in range(OWN):
            @pl.when(c != i)
            def _(m=m, i=i):
                pltpu.make_async_remote_copy(
                    shards[m].at[k, mine], wts.at[c, m, k, mine], wa_s.at[m, i], wa_r.at[m],
                    device_id=(l, i), device_id_type=MESH).start()

    @pl.when(owner)
    def _():
        for m in range(2):
            pltpu.make_async_copy(shards[m], wts.at[c, m], own_r.at[m]).start()

    def weights_1():
        for m in range(2):
            take(wa_r, m)
            pass_on(m, mine, 0, wb_s.at[m, 0], wb_r.at[m, 0])
            pass_on(m, mine, 1, wb_s.at[m, 1], wb_r.at[m, 1])
        for m in range(2):
            share(m, mine, 0)

    def weights_2():
        take(wb_r, 0, 1)
        pass_on(0, at_z, 0, wc_s.at[0], wc_r.at[0])
        take(wb_r, 1, 0)
        pass_on(1, at_y, 1, wc_s.at[1], wc_r.at[1])
        take(wb_r, 0, 0)
        take(wb_r, 1, 1)
        for m in range(2):
            share(m, at_y, 1)
            share(m, at_z, 2)

    def weights_3():
        for m in range(2):
            take(wc_r, m)
            share(m, at_d, 3)
        ref = wts.at[pl.ds(0, 3), 0]
        pltpu.make_async_copy(ref, ref, wd_s).wait()
        for m in range(2):
            pltpu.make_async_copy(wts.at[c, m], wts.at[c, m], own_r.at[m]).wait()
            for stage in range(4):
                take(wd_r, stage, m)
            for axis in range(2):
                take(wb_s, m, axis)
            take(wc_s, m)

    for w_ref, b_ref, src, bsrc in ((w1, b1, fin, finb), (w2, b2, fout, foutb)):
        w_ref[...] = jnp.zeros_like(w_ref)
        b_ref[...] = jnp.zeros_like(b_ref)
        for at, re, im in zip((0, 256), parts(src[0, blk]), parts(src[1, blk])):
            w_ref[at:at + BS, 0:BS] = re
            w_ref[at:at + BS, 128:128 + BS] = im
            w_ref[at + 128:at + 128 + BS, 0:BS] = -im
            w_ref[at + 128:at + 128 + BS, 128:128 + BS] = re
        w_ref[512:768, :] = w_ref[0:256, :]
        b_ref[:, 0:BS] = bsrc[0, pl.ds(blk, 1), :]
        b_ref[:, 128:128 + BS] = bsrc[1, pl.ds(blk, 1), :]

    spread_out(t_to, lat_to)
    spread_out(t_fro, lat_fro)

    @pl.when(owner)
    def _():
        for j in range(NC):
            pltpu.make_async_copy(xin.at[j], xin.at[j], in_r.at[j]).wait()
            pltpu.make_async_copy(smalls.at[j], smalls.at[j], sm_r.at[j]).wait()
        par[0:5, :] = jnp.concatenate([smalls[j, 0:5, 0:192] for j in range(NC)], axis=1)
        x[0:W, :] = jnp.concatenate([xin[j] for j in range(NC)], axis=1)
        x[W:R, :] = jnp.zeros((R - W, D), F32)
        fsend[...] = jnp.zeros_like(fsend)

    for i in range(OWN):
        @pl.when(c != i)
        def _(i=i):
            a, b = to_owner(i)
            a.wait_send()
            b.wait_send()

    def step(s, carry):
        @pl.when(owner)
        def _():
            v = x[...]
            n = norm(v, par[0:1, :], par[2:3, :])
            x[...] = v + n
            hi, lo = parts(n)
            n3[0:R, :] = hi
            n3[R:2 * R, :] = hi
            n3[2 * R:3 * R, :] = lo
            lon = jnp.dot(fwd[...], n3[...], preferred_element_type=F32)
            for b in range(NB):
                fsend[b, :, :, 0:BS] = lon[:, b * BS:(b + 1) * BS].reshape(G, 8, BS).astype(BF)

            def send(i, carry):
                d = lax.rem(me + i, ND)
                dl, dc = d // NC, lax.rem(d, NC)
                src = fsend.at[2 * dc + lax.rem(dl, 2), dl // 2]

                pltpu.make_async_remote_copy(
                    src, frecv.at[row], f_s, f_r, device_id=(dl, dc), device_id_type=MESH).start()
                return carry

            lax.fori_loop(1, ND, send, 0)
            pltpu.make_async_copy(
                fsend.at[2 * c + blk, l // 2], frecv.at[row], f_r).start()
            pl.when(s == 0)(weights_1)

        pltpu.make_async_copy(frecv, frecv, f_r).wait()
        got = frecv[...].reshape(H * 8, 128)
        spec = jnp.dot(lat_to[0], got, preferred_element_type=F32)
        spec = (spec + jnp.dot(lat_to[1], got, preferred_element_type=F32)) * SCALE
        spec = jnp.concatenate([spec[0:384], spec[384:768]], axis=1)
        hi, lo = parts(spec)
        first = jnp.dot(jnp.concatenate([hi, hi, lo], axis=1), w1[...], preferred_element_type=F32) + b1[...]
        hi, lo = parts(jnp.maximum(first, 0.0))
        second = jnp.dot(jnp.concatenate([hi, hi, lo], axis=1), w2[...], preferred_element_type=F32) + b2[...]
        second = jnp.where(second > SHRINK, second - SHRINK,
                           jnp.where(second < -SHRINK, second + SHRINK, 0.0))
        hi, lo = parts(jnp.concatenate([second[:, 0:128], second[:, 128:256]], axis=0))
        both = jnp.dot(lat_fro[0], jnp.concatenate([hi, lo], axis=1), preferred_element_type=F32)
        rows = jnp.dot(lat_fro[1], hi, preferred_element_type=F32)
        rows = (rows + both[:, 0:128] + both[:, 128:256]).astype(BF)
        bsend[...] = rows.reshape(H, 8, 128)

        def sendb(i, carry):
            dl = lax.rem(l + i, NL)
            for dc in range(OWN):
                @pl.when(jnp.logical_or(dl != l, c != dc))
                def _():
                    pltpu.make_async_remote_copy(
                        bsend.at[dl * OWN + dc], brecv.at[2 * c + blk, l // 2], b_s, b_r,
                        device_id=(dl, dc), device_id_type=MESH).start()
            return carry

        lax.fori_loop(0, NL, sendb, 0)

        @pl.when(owner)
        def _():
            pltpu.make_async_copy(bsend.at[row], brecv.at[2 * c + blk, l // 2], b_r).start()
            pl.when(s == 0)(weights_2)
            pltpu.make_async_copy(brecv, brecv, b_r).wait()
            packed = jnp.concatenate(
                [brecv[b].reshape(128, 128)[:, 0:BS].astype(F32) for b in range(NB)], axis=1).astype(BF)
            packed = jnp.concatenate([packed, packed], axis=0)
            v = x[...] + jnp.dot(back[...], packed, preferred_element_type=F32) * SCALE
            x[...] = v
            nb[...] = norm(v, par[1:2, :], par[3:4, :]).astype(BF)
            pl.when(s == 0)(weights_3)
            for q in range(NC):
                for j in range(3):
                    cols = slice(j * 256, (j + 1) * 256)
                    weight = wts[q, 0, :, :, :, :, cols].reshape(D, 256)
                    pre = jnp.dot(nb[...], weight, preferred_element_type=F32) + smalls[q, 5:6, cols]
                    act = 0.5 * pre * (1.0 + lax.erf(pre * math.sqrt(0.5)))
                    hid[:, q * 768 + j * 256:q * 768 + (j + 1) * 256] = act.astype(BF)
            for j in range(3):
                cols = slice(j * 256, (j + 1) * 256)
                weight = wts[:, 1, :, :, :, :, cols].reshape(FF, 256)
                mixed = jnp.dot(hid[...], weight, preferred_element_type=F32)
                x[:, cols] = x[:, cols] + mixed + par[4:5, cols]
            pltpu.make_async_copy(fsend.at[0:7], fsend.at[0:7], f_s).wait()
            pltpu.make_async_copy(fsend.at[7, 0:15], fsend.at[7, 0:15], f_s).wait()
            pltpu.make_async_copy(bsend.at[0:95], bsend.at[0:95], b_s).wait()

        @pl.when(jnp.logical_not(owner))
        def _():
            pltpu.make_async_copy(bsend, bsend, b_s).wait()

        return carry

    lax.fori_loop(0, STEPS, step, 0)

    for m in range(2):
        for i in range(OWN):
            @pl.when(c != i)
            def _(m=m, i=i):
                ref = shards[m].at[k, mine]
                pltpu.make_async_copy(ref, ref, wa_s.at[m, i]).wait()

    @pl.when(owner)
    def _():
        for j in range(NC):
            xin[j] = x[0:W, j * 192:(j + 1) * 192]

        for j in range(NC):
            @pl.when(c != j)
            def _(j=j):
                pltpu.make_async_remote_copy(
                    xin.at[j], out.at[c], o_s.at[j], o_r.at[c],
                    device_id=(l, j), device_id_type=MESH).start()

            @pl.when(c == j)
            def _(j=j):
                pltpu.make_async_copy(xin.at[j], out.at[c], o_r.at[c]).start()

    for i in range(OWN):
        pltpu.make_async_copy(out.at[i], out.at[i], o_r.at[i]).wait()

    @pl.when(owner)
    def _():
        for j in range(NC):
            @pl.when(c != j)
            def _(j=j):
                pltpu.make_async_copy(xin.at[j], xin.at[j], o_s.at[j]).wait()


def local(
    state, norm_gains, channel_biases, filter_in, filter_in_bias, filter_out, filter_out_bias,
    up_weight, up_bias, down_weight,
):
    up = up_weight.reshape(2, 4, 2, 48, 768)
    down = down_weight.reshape(2, 4, 2, 48, 768)
    small = jnp.zeros((8, D), F32)
    small = small.at[0:2, 0:192].set(norm_gains.astype(F32))
    small = small.at[2:5, 0:192].set(channel_biases.astype(F32))
    small = small.at[5, :].set(up_bias.astype(F32))
    fwd, back, t_to, t_fro = tables()
    vm = pl.BlockSpec(memory_space=pltpu.VMEM)
    anyspace = pl.BlockSpec(memory_space=pl.ANY)
    sem = pltpu.SemaphoreType.DMA
    result = pl.pallas_call(
        kernel,
        out_shape=jax.ShapeDtypeStruct((OWN, W, 192), F32),
        in_specs=[anyspace] + [vm] * 5 + [anyspace] * 2 + [vm] * 4,
        out_specs=vm,
        scratch_shapes=[
            pltpu.VMEM((NC, W, 192), F32),
            pltpu.VMEM((NC, 8, D), F32),
            pltpu.VMEM((R, D), F32),
            pltpu.VMEM((R, D), BF),
            pltpu.VMEM((NB, G, 8, 128), BF),
            pltpu.VMEM((H, 8, 128), BF),
            pltpu.VMEM((H, 8, 128), BF),
            pltpu.VMEM((NB, G, 8, 128), BF),
            pltpu.VMEM((768, 256), BF),
            pltpu.VMEM((1, 256), F32),
            pltpu.VMEM((768, 256), BF),
            pltpu.VMEM((1, 256), F32),
            pltpu.VMEM((8, D), F32),
            pltpu.VMEM((R, FF), BF),
            pltpu.VMEM((2, 768, 768), BF),
            pltpu.VMEM((2, 768, 768), BF),
            pltpu.VMEM((3 * R, D), BF),
            pltpu.VMEM((NC, 2, 2, 4, 2, 48, 768), BF),
            sem((OWN,)), sem((NC,)), sem((OWN,)), sem((NC,)),
            sem, sem, sem, sem, sem((NC,)), sem((OWN,)),
            sem((2,)), sem((2, OWN)), sem((2,)), sem((2, 2)), sem((2, 2)), sem((2,)), sem((2,)), sem, sem((4, 2)),
        ],
        compiler_params=pltpu.CompilerParams(
            has_side_effects=True, vmem_limit_bytes=50 * 1024 * 1024),
        name="rollout",
    )(
        state[0], small, filter_in, filter_in_bias, filter_out, filter_out_bias,
        up, down, jnp.asarray(fwd), jnp.asarray(back), jnp.asarray(t_to), jnp.asarray(t_fro),
    )
    return result[None]


def solution(mesh):
    placed = (
        P(None, "lat", None, "ch"),
        P(None, "ch"),
        P(None, "ch"),
        P(None, "ch", None, None),
        P(None, "ch", None),
        P(None, "ch", None, None),
        P(None, "ch", None),
        P(None, "ch"),
        P("ch"),
        P("ch", None),
    )
    return jax.shard_map(
        local, mesh=mesh, in_specs=placed, out_specs=P(None, "lat", None, "ch"), check_vma=False
    )
```

```python
import math

import jax
import jax.numpy as jnp
import numpy as np
from jax import lax
from jax.experimental import pallas as pl
from jax.experimental.pallas import tpu as pltpu
from jax.sharding import PartitionSpec as P

D = 768
FF = 3072
W = 180
R = 192
H = 96
M = 64
NB = 8
BS = 96
STEPS = 4
NL = 32
NC = 4
ND = NL * NC
OWN = 3
G = 16
SCALE = 1.0 / math.sqrt(H * W)
EPS = 1e-05
SHRINK = 0.01
MESH = pl.DeviceIdType.MESH
BF = jnp.bfloat16
F32 = jnp.float32


def tables():
    modes = np.arange(M)
    w = np.arange(W)
    ang = 2.0 * np.pi / W * ((w[:, None] * modes[None, :]) % W)
    c, s = np.cos(ang), np.sin(ang)
    dbl = np.where(modes == 0, 1.0, 2.0)
    fwd = np.zeros((G, 2, 4, R))
    fwd[:, 0, :, :W] = c.T.reshape(G, 4, W)
    fwd[:, 1, :, :W] = -s.T.reshape(G, 4, W)
    back = np.zeros((R, G, 2, 4))
    back[:W, :, 0, :] = (c * dbl).reshape(W, G, 4)
    back[:W, :, 1, :] = -(s * dbl).reshape(W, G, 4)
    h = np.arange(H)
    ang = 2.0 * np.pi / H * ((h[:, None] * h[None, :]) % H)
    c, s = np.cos(ang), np.sin(ang)
    lat = np.zeros((2, H, H, 2))
    lat[0, :, :, 0] = c
    lat[0, :, :, 1] = s
    lat[1, :, :, 0] = -s
    lat[1, :, :, 1] = c
    lat = lat.reshape(192, 192)
    fwd, back = halves(fwd.reshape(128, R)), halves(back.reshape(R, 128))
    return (
        np.concatenate([fwd[0], fwd[1], fwd[0]], axis=1),
        np.concatenate(back, axis=1),
        np.stack(halves(lat)),
        np.stack(halves(lat.T)),
    )


def halves(a):
    a = np.asarray(a, np.float32)
    hi = a.astype(BF)
    return hi, (a - hi.astype(np.float32)).astype(BF)


def parts(v):
    hi = v.astype(BF)
    return hi, (v - hi.astype(F32)).astype(BF)


def spread_out(t_ref, o_ref):
    def iota(shape, dim):
        return lax.broadcasted_iota(jnp.int32, shape, dim)

    one = lambda m: jnp.where(m, 1.0, 0.0).astype(BF)
    rows = one(iota((768, 192), 0) // 4 == iota((768, 192), 1))
    cols = one(iota((192, 768), 1) // 4 == iota((192, 768), 0))
    keep = lax.rem(iota((192, 768), 0), 4) == lax.rem(iota((192, 768), 1), 4)
    for half in range(2):
        tall = jnp.dot(rows, t_ref[half], preferred_element_type=F32).astype(BF)
        for j in range(4):
            wide = jnp.dot(tall[j * 192:(j + 1) * 192], cols, preferred_element_type=F32)
            o_ref[half, j * 192:(j + 1) * 192, :] = jnp.where(keep, wide, 0.0).astype(BF)


def norm(v, gain, shift):
    mean = jnp.sum(v, -1, keepdims=True) / D
    spread = jnp.sum(v * v, -1, keepdims=True) / D - mean * mean
    return (v - mean) * lax.rsqrt(spread + EPS) * gain + shift


def kernel(
    state, small, fin, finb, fout, foutb, up, down, fwd, back, t_to, t_fro,
    out,
    xin, smalls, x, nb, fsend, frecv, bsend, brecv, w1, b1, w2, b2, par, hid, lat_to, lat_fro, n3, wts, tall, stat, stats,
    in_s, in_r, sm_s, sm_r, f_s, f_r, b_s, b_r, o_s, o_r,
    own_r, wa_s, wa_r, wb_s, wb_r, wc_s, wc_r, wd_s, wd_r, st_s, st_r,
):
    l = lax.axis_index("lat")
    c = lax.axis_index("ch")
    me = l * NC + c
    row = l * OWN + c
    blk = lax.rem(l, 2)
    owner = c < OWN

    barrier = pltpu.get_barrier_semaphore()

    def greet(i, carry):
        d = lax.rem(me + i, ND)
        pl.semaphore_signal(barrier, inc=1, device_id=(d // NC, lax.rem(d, NC)), device_id_type=MESH)
        return carry

    lax.fori_loop(1, ND, greet, 0)

    def to_owner(i):
        return (
            pltpu.make_async_remote_copy(
                state.at[i], xin.at[c], in_s.at[i], in_r.at[c],
                device_id=(l, i), device_id_type=MESH),
            pltpu.make_async_remote_copy(
                small, smalls.at[c], sm_s.at[i], sm_r.at[c],
                device_id=(l, i), device_id_type=MESH),
        )

    k = lax.rem(l, 2)
    cy = lax.rem(l // 2, 4)
    cz = l // 8
    py, pz = lax.rem(cy, 2), lax.rem(cz, 2)
    mine = 2 * pz + py
    at_y, at_z, at_d = 2 * pz + 1 - py, 2 * (1 - pz) + py, 2 * (1 - pz) + 1 - py
    shards = (up, down)

    def chip(dy, dz, core):
        return (lax.rem(cz + dz + 4, 4) * 4 + lax.rem(cy + dy + 4, 4)) * 2 + core

    def foreign(j):
        return lax.rem(c + 1 + j, NC)

    def take(sems, *at):
        ref = wts.at[0, 0, 0, pl.ds(0, 3)]
        pltpu.make_async_copy(ref, ref, sems.at[at]).wait()

    def pass_on(m, piece, axis, s_sem, r_sem):
        for j in range(3):
            for half, sign in ((0, 1), (1, -1)):
                ref = wts.at[foreign(j), m, k, piece, half]
                to = chip(sign, 0, k) if axis == 0 else chip(0, sign, k)
                pltpu.make_async_remote_copy(
                    ref, ref, s_sem, r_sem, device_id=(to, c), device_id_type=MESH).start()

    def share(m, piece, stage):
        for j in range(3):
            ref = wts.at[foreign(j), m, k, piece]
            pltpu.make_async_remote_copy(
                ref, ref, wd_s, wd_r.at[stage, m], device_id=(chip(0, 0, 1 - k), c), device_id_type=MESH).start()

    def weights_1(m):
        take(wa_r, m)
        pass_on(m, mine, 0, wb_s.at[m, 0], wb_r.at[m, 0])
        pass_on(m, mine, 1, wb_s.at[m, 1], wb_r.at[m, 1])
        share(m, mine, 0)

    def weights_2(m):
        take(wb_r, m, 1 - m)
        pass_on(m, (at_z, at_y)[m], m, wc_s.at[m], wc_r.at[m])
        take(wb_r, m, m)
        share(m, at_y, 1)
        share(m, at_z, 2)

    def weights_3(m):
        take(wc_r, m)
        share(m, at_d, 3)

    def weights_4(m):
        pltpu.make_async_copy(wts.at[c, m], wts.at[c, m], own_r.at[m]).wait()
        for stage in range(4):
            take(wd_r, stage, m)

    for w_ref, b_ref, src, bsrc in ((w1, b1, fin, finb), (w2, b2, fout, foutb)):
        w_ref[...] = jnp.zeros_like(w_ref)
        b_ref[...] = jnp.zeros_like(b_ref)
        for at, re, im in zip((0, 256), parts(src[0, blk]), parts(src[1, blk])):
            w_ref[at:at + BS, 0:BS] = re
            w_ref[at:at + BS, 128:128 + BS] = im
            w_ref[at + 128:at + 128 + BS, 0:BS] = -im
            w_ref[at + 128:at + 128 + BS, 128:128 + BS] = re
        w_ref[512:768, :] = w_ref[0:256, :]
        b_ref[:, 0:BS] = bsrc[0, pl.ds(blk, 1), :]
        b_ref[:, 128:128 + BS] = bsrc[1, pl.ds(blk, 1), :]

    spread_out(t_to, lat_to)
    spread_out(t_fro, lat_fro)

    fsend[...] = jnp.zeros_like(fsend)
    n3[...] = jnp.zeros_like(n3)
    tall[...] = jnp.zeros_like(tall)
    lane = lax.broadcasted_iota(jnp.int32, (W, 128), 1)
    for r in range(OWN):
        v = state[r]
        total = jnp.sum(v, -1, keepdims=True)
        squares = jnp.sum(v * v, -1, keepdims=True)
        tall[r * R:r * R + W, :] = jnp.where(lane == 0, total, jnp.where(lane == 1, squares, 0.0))
    stat[...] = tall[...].T[0:8, :]

    @pl.when(owner)
    def _():
        for m in range(2):
            pltpu.make_async_copy(shards[m], wts.at[c, m], own_r.at[m]).start()

    pl.semaphore_wait(barrier, ND - 1)
    for j in range(NC):
        @pl.when(c != j)
        def _(j=j):
            pltpu.make_async_remote_copy(
                stat, stats.at[c], st_s.at[j], st_r.at[c], device_id=(l, j), device_id_type=MESH).start()

        @pl.when(c == j)
        def _(j=j):
            pltpu.make_async_copy(stat, stats.at[j], st_r.at[j]).start()

    for m in range(2):
        for i in range(OWN):
            @pl.when(c != i)
            def _(m=m, i=i):
                pltpu.make_async_remote_copy(
                    shards[m].at[k, mine], wts.at[c, m, k, mine], wa_s.at[m, i], wa_r.at[m],
                    device_id=(l, i), device_id_type=MESH).start()

    for i in range(OWN):
        @pl.when(c != i)
        def _(i=i):
            a, b = to_owner(i)
            a.start()
            b.start()

        @pl.when(c == i)
        def _(i=i):
            pltpu.make_async_copy(state.at[i], xin.at[i], in_r.at[i]).start()
            pltpu.make_async_copy(small, smalls.at[i], sm_r.at[i]).start()

    for j in range(NC):
        pltpu.make_async_copy(stats.at[j], stats.at[j], st_r.at[j]).wait()
    total = (stats[0] + stats[1]) + (stats[2] + stats[3])
    mean = total[0:1] / D
    spread = lax.rsqrt(total[1:2] / D - mean * mean + EPS)
    line = lax.broadcasted_iota(jnp.int32, (128, 640), 0)
    tall[...] = jnp.where(line == 0, mean, jnp.where(line == 1, spread, 0.0)).T
    for r in range(OWN):
        at = slice(r * R, r * R + W)
        n = (state[r] - tall[at, 0:1]) * tall[at, 1:2] * small[0:1, 0:192] + small[2:3, 0:192]
        hi, lo = parts(n)
        n3[0:W, 0:192] = hi
        n3[R:R + W, 0:192] = hi
        n3[2 * R:2 * R + W, 0:192] = lo
        lon = jnp.dot(fwd[...], n3[:, 0:192], preferred_element_type=F32)
        for j in range(2):
            fsend[2 * r + j, :, :, 0:BS] = lon[:, j * BS:(j + 1) * BS].reshape(G, 8, BS).astype(BF)

    def send_first(i, carry):
        dl = lax.rem(l + i, NL)
        for r in range(OWN):
            pltpu.make_async_remote_copy(
                fsend.at[2 * r + lax.rem(dl, 2), dl // 2], frecv.at[l * OWN + r], f_s, f_r,
                device_id=(dl, c), device_id_type=MESH).start()
        return carry

    lax.fori_loop(1, NL, send_first, 0)
    for r in range(OWN):
        pltpu.make_async_copy(fsend.at[2 * r + blk, l // 2], frecv.at[l * OWN + r], f_r).start()
    pl.when(owner)(lambda: weights_1(0))

    def own_row():
        for j in range(NC):
            pltpu.make_async_copy(xin.at[j], xin.at[j], in_r.at[j]).wait()
            pltpu.make_async_copy(smalls.at[j], smalls.at[j], sm_r.at[j]).wait()
        par[0:5, :] = jnp.concatenate([smalls[j, 0:5, 0:192] for j in range(NC)], axis=1)
        v = jnp.concatenate([xin[j] for j in range(NC)], axis=1)
        x[0:W, :] = v + norm(v, par[0:1, :], par[2:3, :])
        x[W:R, :] = jnp.zeros((R - W, D), F32)

    def send_row():
        v = x[...]
        n = norm(v, par[0:1, :], par[2:3, :])
        x[...] = v + n
        hi, lo = parts(n)
        n3[0:R, :] = hi
        n3[R:2 * R, :] = hi
        n3[2 * R:3 * R, :] = lo
        lon = jnp.dot(fwd[...], n3[...], preferred_element_type=F32)
        for b in range(NB):
            fsend[b, :, :, 0:BS] = lon[:, b * BS:(b + 1) * BS].reshape(G, 8, BS).astype(BF)

        def send(i, carry):
            d = lax.rem(me + i, ND)
            dl, dc = d // NC, lax.rem(d, NC)
            src = fsend.at[2 * dc + lax.rem(dl, 2), dl // 2]

            pltpu.make_async_remote_copy(
                src, frecv.at[row], f_s, f_r, device_id=(dl, dc), device_id_type=MESH).start()
            return carry

        lax.fori_loop(1, ND, send, 0)
        pltpu.make_async_copy(
            fsend.at[2 * c + blk, l // 2], frecv.at[row], f_r).start()

    def step(s, carry):
        pltpu.make_async_copy(frecv, frecv, f_r).wait()
        got = frecv[...].reshape(H * 8, 128)
        spec = jnp.dot(lat_to[0], got, preferred_element_type=F32)
        spec = (spec + jnp.dot(lat_to[1], got, preferred_element_type=F32)) * SCALE
        spec = jnp.concatenate([spec[0:384], spec[384:768]], axis=1)
        hi, lo = parts(spec)
        first = jnp.dot(jnp.concatenate([hi, hi, lo], axis=1), w1[...], preferred_element_type=F32) + b1[...]
        hi, lo = parts(jnp.maximum(first, 0.0))
        second = jnp.dot(jnp.concatenate([hi, hi, lo], axis=1), w2[...], preferred_element_type=F32) + b2[...]
        second = jnp.where(second > SHRINK, second - SHRINK,
                           jnp.where(second < -SHRINK, second + SHRINK, 0.0))
        hi, lo = parts(jnp.concatenate([second[:, 0:128], second[:, 128:256]], axis=0))
        both = jnp.dot(lat_fro[0], jnp.concatenate([hi, lo], axis=1), preferred_element_type=F32)
        rows = jnp.dot(lat_fro[1], hi, preferred_element_type=F32)
        rows = (rows + both[:, 0:128] + both[:, 128:256]).astype(BF)
        bsend[...] = rows.reshape(H, 8, 128)

        def sendb(i, carry):
            dl = lax.rem(l + i, NL)
            for dc in range(OWN):
                @pl.when(jnp.logical_or(dl != l, c != dc))
                def _():
                    pltpu.make_async_remote_copy(
                        bsend.at[dl * OWN + dc], brecv.at[2 * c + blk, l // 2], b_s, b_r,
                        device_id=(dl, dc), device_id_type=MESH).start()
            return carry

        lax.fori_loop(0, NL, sendb, 0)

        @pl.when(owner)
        def _():
            pltpu.make_async_copy(bsend.at[row], brecv.at[2 * c + blk, l // 2], b_r).start()

            @pl.when(s == 0)
            def _():
                weights_1(1)
                weights_2(0)
                own_row()
                weights_3(0)

            pltpu.make_async_copy(brecv, brecv, b_r).wait()

            @pl.when(s == 0)
            def _():
                weights_2(1)

            packed = jnp.concatenate(
                [brecv[b].reshape(128, 128)[:, 0:BS].astype(F32) for b in range(NB)], axis=1).astype(BF)
            packed = jnp.concatenate([packed, packed], axis=0)
            v = x[...] + jnp.dot(back[...], packed, preferred_element_type=F32) * SCALE
            x[...] = v
            nb[...] = norm(v, par[1:2, :], par[3:4, :]).astype(BF)

            @pl.when(s == 0)
            def _():
                weights_4(0)

            for q in range(NC):
                for j in range(3):
                    cols = slice(j * 256, (j + 1) * 256)
                    weight = wts[q, 0, :, :, :, :, cols].reshape(D, 256)
                    pre = jnp.dot(nb[...], weight, preferred_element_type=F32) + smalls[q, 5:6, cols]
                    act = 0.5 * pre * (1.0 + lax.erf(pre * math.sqrt(0.5)))
                    hid[:, q * 768 + j * 256:q * 768 + (j + 1) * 256] = act.astype(BF)

            @pl.when(s == 0)
            def _():
                weights_3(1)
                weights_4(1)

            for j in range(3):
                cols = slice(j * 256, (j + 1) * 256)
                weight = wts[:, 1, :, :, :, :, cols].reshape(FF, 256)
                mixed = jnp.dot(hid[...], weight, preferred_element_type=F32)
                x[:, cols] = x[:, cols] + mixed + par[4:5, cols]

            @pl.when(s < STEPS - 1)
            def _():
                sent_f(s)
                send_row()

            pltpu.make_async_copy(bsend.at[0:95], bsend.at[0:95], b_s).wait()

        @pl.when(jnp.logical_not(owner))
        def _():
            pl.when(s == 0)(lambda: sent_f(s))
            pltpu.make_async_copy(bsend, bsend, b_s).wait()

        return carry

    def sent_f(s):
        @pl.when(s == 0)
        def _():
            pltpu.make_async_copy(bsend.at[0:93], bsend.at[0:93], f_s).wait()

        @pl.when(s > 0)
        def _():
            pltpu.make_async_copy(fsend.at[0:7], fsend.at[0:7], f_s).wait()
            pltpu.make_async_copy(fsend.at[7, 0:15], fsend.at[7, 0:15], f_s).wait()

    lax.fori_loop(0, STEPS, step, 0)

    @pl.when(owner)
    def _():
        sent_f(1)
        ref = wts.at[pl.ds(0, 3), 0]
        pltpu.make_async_copy(ref, ref, wd_s).wait()
        for m in range(2):
            for axis in range(2):
                take(wb_s, m, axis)
            take(wc_s, m)

    for i in range(OWN):
        @pl.when(c != i)
        def _(i=i):
            a, b = to_owner(i)
            a.wait_send()
            b.wait_send()

    for j in range(NC):
        @pl.when(c != j)
        def _(j=j):
            pltpu.make_async_copy(stat, stat, st_s.at[j]).wait()

    for m in range(2):
        for i in range(OWN):
            @pl.when(c != i)
            def _(m=m, i=i):
                ref = shards[m].at[k, mine]
                pltpu.make_async_copy(ref, ref, wa_s.at[m, i]).wait()

    @pl.when(owner)
    def _():
        for j in range(NC):
            xin[j] = x[0:W, j * 192:(j + 1) * 192]

        for j in range(NC):
            @pl.when(c != j)
            def _(j=j):
                pltpu.make_async_remote_copy(
                    xin.at[j], out.at[c], o_s.at[j], o_r.at[c],
                    device_id=(l, j), device_id_type=MESH).start()

            @pl.when(c == j)
            def _(j=j):
                pltpu.make_async_copy(xin.at[j], out.at[c], o_r.at[c]).start()

    for i in range(OWN):
        pltpu.make_async_copy(out.at[i], out.at[i], o_r.at[i]).wait()

    @pl.when(owner)
    def _():
        for j in range(NC):
            @pl.when(c != j)
            def _(j=j):
                pltpu.make_async_copy(xin.at[j], xin.at[j], o_s.at[j]).wait()


def local(
    state, norm_gains, channel_biases, filter_in, filter_in_bias, filter_out, filter_out_bias,
    up_weight, up_bias, down_weight,
):
    up = up_weight.reshape(2, 4, 2, 48, 768)
    down = down_weight.reshape(2, 4, 2, 48, 768)
    small = jnp.zeros((8, D), F32)
    small = small.at[0:2, 0:192].set(norm_gains.astype(F32))
    small = small.at[2:5, 0:192].set(channel_biases.astype(F32))
    small = small.at[5, :].set(up_bias.astype(F32))
    fwd, back, t_to, t_fro = tables()
    vm = pl.BlockSpec(memory_space=pltpu.VMEM)
    anyspace = pl.BlockSpec(memory_space=pl.ANY)
    sem = pltpu.SemaphoreType.DMA
    result = pl.pallas_call(
        kernel,
        out_shape=jax.ShapeDtypeStruct((OWN, W, 192), F32),
        in_specs=[vm] + [vm] * 5 + [anyspace] * 2 + [vm] * 4,
        out_specs=vm,
        scratch_shapes=[
            pltpu.VMEM((NC, W, 192), F32),
            pltpu.VMEM((NC, 8, D), F32),
            pltpu.VMEM((R, D), F32),
            pltpu.VMEM((R, D), BF),
            pltpu.VMEM((NB, G, 8, 128), BF),
            pltpu.VMEM((H, 8, 128), BF),
            pltpu.VMEM((H, 8, 128), BF),
            pltpu.VMEM((NB, G, 8, 128), BF),
            pltpu.VMEM((768, 256), BF),
            pltpu.VMEM((1, 256), F32),
            pltpu.VMEM((768, 256), BF),
            pltpu.VMEM((1, 256), F32),
            pltpu.VMEM((8, D), F32),
            pltpu.VMEM((R, FF), BF),
            pltpu.VMEM((2, 768, 768), BF),
            pltpu.VMEM((2, 768, 768), BF),
            pltpu.VMEM((3 * R, D), BF),
            pltpu.VMEM((NC, 2, 2, 4, 2, 48, 768), BF),
            pltpu.VMEM((640, 128), F32),
            pltpu.VMEM((8, 640), F32),
            pltpu.VMEM((NC, 8, 640), F32),
            sem((OWN,)), sem((NC,)), sem((OWN,)), sem((NC,)),
            sem, sem, sem, sem, sem((NC,)), sem((OWN,)),
            sem((2,)), sem((2, OWN)), sem((2,)), sem((2, 2)), sem((2, 2)), sem((2,)), sem((2,)), sem, sem((4, 2)), sem((NC,)), sem((NC,)),
        ],
        compiler_params=pltpu.CompilerParams(
            collective_id=0, has_side_effects=True, vmem_limit_bytes=50 * 1024 * 1024),
        name="rollout",
    )(
        state[0], small, filter_in, filter_in_bias, filter_out, filter_out_bias,
        up, down, jnp.asarray(fwd), jnp.asarray(back), jnp.asarray(t_to), jnp.asarray(t_fro),
    )
    return result[None]


def solution(mesh):
    placed = (
        P(None, "lat", None, "ch"),
        P(None, "ch"),
        P(None, "ch"),
        P(None, "ch", None, None),
        P(None, "ch", None),
        P(None, "ch", None, None),
        P(None, "ch", None),
        P(None, "ch"),
        P("ch"),
        P("ch", None),
    )
    return jax.shard_map(
        local, mesh=mesh, in_specs=placed, out_specs=P(None, "lat", None, "ch"), check_vma=False
    )
```

```python
import itertools
import math

import jax
import jax.numpy as jnp
import numpy as np
from jax import lax
from jax.experimental import pallas as pl
from jax.experimental.pallas import tpu as pltpu
from jax.sharding import PartitionSpec as P

D = 768
FF = 3072
W = 180
R = 192
H = 96
M = 64
NB = 8
BS = 96
STEPS = 4
NL = 32
NC = 4
ND = NL * NC
OWN = 3
G = 16
SCALE = 1.0 / math.sqrt(H * W)
EPS = 1e-05
SHRINK = 0.01
HOPS = (0, 1, 2, 1)
OTHERS = sorted(
    (o for o in itertools.product(range(4), range(4), range(4), range(2)) if any(o)),
    key=lambda o: -(HOPS[o[0]] + HOPS[o[1]] + HOPS[o[2]] + 0.3 * o[3]),
)
MESH = pl.DeviceIdType.MESH
BF = jnp.bfloat16
F32 = jnp.float32


def tables():
    modes = np.arange(M)
    w = np.arange(W)
    ang = 2.0 * np.pi / W * ((w[:, None] * modes[None, :]) % W)
    c, s = np.cos(ang), np.sin(ang)
    dbl = np.where(modes == 0, 1.0, 2.0)
    fwd = np.zeros((G, 2, 4, R))
    fwd[:, 0, :, :W] = c.T.reshape(G, 4, W)
    fwd[:, 1, :, :W] = -s.T.reshape(G, 4, W)
    back = np.zeros((R, G, 2, 4))
    back[:W, :, 0, :] = (c * dbl).reshape(W, G, 4)
    back[:W, :, 1, :] = -(s * dbl).reshape(W, G, 4)
    h = np.arange(H)
    ang = 2.0 * np.pi / H * ((h[:, None] * h[None, :]) % H)
    c, s = np.cos(ang), np.sin(ang)
    to = np.block([[c, s], [-s, c]])
    fro = to.T
    fwd, back = halves(fwd.reshape(128, R)), halves(back.reshape(R, 128))
    return (
        np.concatenate([fwd[0], fwd[1], fwd[0]], axis=1),
        np.concatenate(back, axis=1),
        np.concatenate(halves(to), axis=1),
        np.concatenate([halves(fro)[0], halves(fro)[1], halves(fro)[0]], axis=1),
    )


def halves(a):
    a = np.asarray(a, np.float32)
    hi = a.astype(BF)
    return hi, (a - hi.astype(np.float32)).astype(BF)


def parts(v):
    hi = v.astype(BF)
    return hi, (v - hi.astype(F32)).astype(BF)


def norm(v, gain, shift):
    mean = jnp.sum(v, -1, keepdims=True) / D
    spread = jnp.sum(v * v, -1, keepdims=True) / D - mean * mean
    return (v - mean) * lax.rsqrt(spread + EPS) * gain + shift


def kernel(
    state_h, gains_h, biases_h, fin_h, finb_h, fout_h, foutb_h, up, upb_h, down, fwd_h, back_h, to_h, fro_h,
    out,
    state, gains, biases, fin, finb, fout, foutb, upb, fwd, back, t_to, t_fro, small, h_s,
    xin, smalls, x, nb, fsend, frecv, bsend, brecv, w1, b1, w2, b2, par, hid, g32, n3, wts, tall, stat, stats,
    in_s, in_r, sm_s, sm_r, f_s, f_r, b_s, b_r, o_s, o_r,
    own_r, wa_s, wa_r, wb_s, wb_r, wc_s, wc_r, wd_s, wd_r, st_s, st_r,
):
    l = lax.axis_index("lat")
    c = lax.axis_index("ch")
    me = l * NC + c
    row = l * OWN + c
    blk = lax.rem(l, 2)
    owner = c < OWN

    k = lax.rem(l, 2)
    cy = lax.rem(l // 2, 4)
    cz = l // 8
    xs = [lax.rem(c + i, 4) for i in range(4)]
    groups = [[lax.rem(cz + i, 4) * 4 + lax.rem(cy + j, 4) for j in range(4)] for i in range(4)]
    cores = (k, 1 - k)

    fetches = [
        pltpu.make_async_copy(src, dst, h_s.at[i])
        for i, (src, dst) in enumerate((
            (to_h, t_to), (fro_h, t_fro), (fin_h, fin), (fout_h, fout), (finb_h, finb), (foutb_h, foutb),
            (gains_h, gains), (biases_h, biases), (upb_h, upb), (fwd_h, fwd), (back_h, back), (state_h, state)))
    ]
    for fetch in fetches:
        fetch.start()

    barrier = pltpu.get_barrier_semaphore()
    for dx, dy, dz, dk in OTHERS:
        pl.semaphore_signal(
            barrier, inc=1, device_id=(groups[dz][dy] * 2 + cores[dk], xs[dx]), device_id_type=MESH)

    def to_owner(i):
        return (
            pltpu.make_async_remote_copy(
                state.at[i], xin.at[c], in_s.at[i], in_r.at[c],
                device_id=(l, i), device_id_type=MESH),
            pltpu.make_async_remote_copy(
                small, smalls.at[c], sm_s.at[i], sm_r.at[c],
                device_id=(l, i), device_id_type=MESH),
        )

    py, pz = lax.rem(cy, 2), lax.rem(cz, 2)
    mine = 2 * pz + py
    at_y, at_z, at_d = 2 * pz + 1 - py, 2 * (1 - pz) + py, 2 * (1 - pz) + 1 - py
    shards = (up, down)

    def foreign(j):
        return lax.rem(c + 1 + j, NC)

    three = wts.at[0, 0, 0, pl.ds(0, 3)]

    def take(sems, *at):
        pltpu.make_async_copy(three, three, sems.at[at]).wait()

    def pass_on(m, piece, axis, s_sem, r_sem):
        for j in range(3):
            for half, sign in ((0, 1), (1, 3)):
                ref = wts.at[foreign(j), m, k, piece, half]
                to = groups[(0, sign)[axis]][(sign, 0)[axis]] * 2 + k
                pltpu.make_async_remote_copy(
                    ref, ref, s_sem, r_sem, device_id=(to, c), device_id_type=MESH).start()

    def share(m, piece, stage):
        for j in range(3):
            ref = wts.at[foreign(j), m, k, piece]
            pltpu.make_async_remote_copy(
                ref, ref, wd_s, wd_r.at[stage, m], device_id=(groups[0][0] * 2 + 1 - k, c), device_id_type=MESH).start()

    def weights_0(m):
        for i in range(OWN):
            @pl.when(c != i)
            def _(i=i):
                pltpu.make_async_remote_copy(
                    shards[m].at[k, mine], wts.at[c, m, k, mine], wa_s.at[m, i], wa_r.at[m],
                    device_id=(l, i), device_id_type=MESH).start()

    def sent_weights(m):
        for i in range(OWN):
            @pl.when(c != i)
            def _(i=i):
                ref = shards[m].at[k, mine]
                pltpu.make_async_copy(ref, ref, wa_s.at[m, i]).wait()

    def weights_1(m):
        take(wa_r, m)
        for axis in range(2):
            pass_on(m, mine, axis, wb_s.at[m, axis], wb_r.at[m, axis])
        share(m, mine, 0)

    def weights_2(m):
        take(wb_r, m, 1 - m)
        pass_on(m, (at_z, at_y)[m], m, wc_s.at[m], wc_r.at[m])
        share(m, (at_z, at_y)[m], 2)
        take(wb_r, m, m)
        share(m, (at_y, at_z)[m], 1)

    def weights_3(m):
        take(wc_r, m)
        share(m, at_d, 3)

    def weights_4(m):
        pltpu.make_async_copy(wts.at[c, m], wts.at[c, m], own_r.at[m]).wait()
        for stage in range(4):
            take(wd_r, stage, m)

    fsend[...] = jnp.zeros_like(fsend)
    n3[...] = jnp.zeros_like(n3)
    tall[...] = jnp.zeros_like(tall)
    small[...] = jnp.zeros_like(small)
    for fetch in fetches:
        fetch.wait()
    small[0:2, 0:192] = gains[...].astype(F32)
    small[2:5, 0:192] = biases[...].astype(F32)
    small[5:6, :] = upb[...].astype(F32).reshape(1, D)
    for w_ref, b_ref, src, bsrc in ((w1, b1, fin, finb), (w2, b2, fout, foutb)):
        w_ref[...] = jnp.zeros_like(w_ref)
        b_ref[...] = jnp.zeros_like(b_ref)
        for at, re, im in zip((0, 256), parts(src[0, blk]), parts(src[1, blk])):
            w_ref[at:at + BS, 0:BS] = re
            w_ref[at:at + BS, 128:128 + BS] = im
            w_ref[at + 128:at + 128 + BS, 0:BS] = -im
            w_ref[at + 128:at + 128 + BS, 128:128 + BS] = re
        w_ref[512:768, :] = w_ref[0:256, :]
        b_ref[:, 0:BS] = bsrc[0, pl.ds(blk, 1), :]
        b_ref[:, 128:128 + BS] = bsrc[1, pl.ds(blk, 1), :]


    lane = lax.broadcasted_iota(jnp.int32, (W, 128), 1)
    for r in range(OWN):
        v = state[r]
        total = jnp.sum(v, -1, keepdims=True)
        squares = jnp.sum(v * v, -1, keepdims=True)
        tall[r * R:r * R + W, :] = jnp.where(lane == 0, total, jnp.where(lane == 1, squares, 0.0))
    stat[...] = tall[...].T[0:8, :]

    @pl.when(owner)
    def _():
        for m in range(2):
            pltpu.make_async_copy(shards[m], wts.at[c, m], own_r.at[m]).start()

    pl.semaphore_wait(barrier, ND - 1)
    for j in range(NC):
        @pl.when(c != j)
        def _(j=j):
            pltpu.make_async_remote_copy(
                stat, stats.at[c], st_s.at[j], st_r.at[c], device_id=(l, j), device_id_type=MESH).start()

        @pl.when(c == j)
        def _(j=j):
            pltpu.make_async_copy(stat, stats.at[j], st_r.at[j]).start()

    weights_0(0)
    for j in range(NC):
        pltpu.make_async_copy(stats.at[j], stats.at[j], st_r.at[j]).wait()
    sent_weights(0)
    weights_0(1)
    total = (stats[0] + stats[1]) + (stats[2] + stats[3])
    mean = total[0:1] / D
    spread = lax.rsqrt(total[1:2] / D - mean * mean + EPS)
    line = lax.broadcasted_iota(jnp.int32, (128, 640), 0)
    tall[...] = jnp.where(line == 0, mean, jnp.where(line == 1, spread, 0.0)).T
    for r in range(OWN):
        at = slice(r * R, r * R + W)
        n = (state[r] - tall[at, 0:1]) * tall[at, 1:2] * small[0:1, 0:192] + small[2:3, 0:192]
        hi, lo = parts(n)
        n3[0:W, 0:192] = hi
        n3[R:R + W, 0:192] = hi
        n3[2 * R:2 * R + W, 0:192] = lo
        lon = jnp.dot(fwd[...], n3[:, 0:192], preferred_element_type=F32)
        for j in range(2):
            fsend[2 * r + j, :, :, 0:BS] = lon[:, j * BS:(j + 1) * BS].reshape(G, 8, BS).astype(BF)

    for dx, dy, dz, dk in OTHERS:
        if dx:
            continue
        for r in range(OWN):
            pltpu.make_async_remote_copy(
                fsend.at[2 * r + cores[dk], groups[dz][dy]], frecv.at[l * OWN + r], f_s, f_r,
                device_id=(groups[dz][dy] * 2 + cores[dk], c), device_id_type=MESH).start()
    for r in range(OWN):
        pltpu.make_async_copy(fsend.at[2 * r + blk, l // 2], frecv.at[l * OWN + r], f_r).start()
    pl.when(owner)(lambda: weights_1(0))

    def send_state():
        for i in range(OWN):
            @pl.when(c != i)
            def _(i=i):
                a, b = to_owner(i)
                a.start()
                b.start()

            @pl.when(c == i)
            def _(i=i):
                pltpu.make_async_copy(state.at[i], xin.at[i], in_r.at[i]).start()
                pltpu.make_async_copy(small, smalls.at[i], sm_r.at[i]).start()

    def own_row():
        for j in range(NC):
            pltpu.make_async_copy(xin.at[j], xin.at[j], in_r.at[j]).wait()
            pltpu.make_async_copy(smalls.at[j], smalls.at[j], sm_r.at[j]).wait()
        par[0:5, :] = jnp.concatenate([smalls[j, 0:5, 0:192] for j in range(NC)], axis=1)
        v = jnp.concatenate([xin[j] for j in range(NC)], axis=1)
        x[0:W, :] = v + norm(v, par[0:1, :], par[2:3, :])
        x[W:R, :] = jnp.zeros((R - W, D), F32)

    def send_row():
        v = x[...]
        n = norm(v, par[0:1, :], par[2:3, :])
        x[...] = v + n
        hi, lo = parts(n)
        n3[0:R, :] = hi
        n3[R:2 * R, :] = hi
        n3[2 * R:3 * R, :] = lo
        lon = jnp.dot(fwd[...], n3[...], preferred_element_type=F32)
        for b in range(NB):
            fsend[b, :, :, 0:BS] = lon[:, b * BS:(b + 1) * BS].reshape(G, 8, BS).astype(BF)

        for dx, dy, dz, dk in OTHERS:
            pltpu.make_async_remote_copy(
                fsend.at[2 * xs[dx] + cores[dk], groups[dz][dy]], frecv.at[row], f_s, f_r,
                device_id=(groups[dz][dy] * 2 + cores[dk], xs[dx]), device_id_type=MESH).start()
        pltpu.make_async_copy(
            fsend.at[2 * c + blk, l // 2], frecv.at[row], f_r).start()

    def step(s, carry):
        pltpu.make_async_copy(frecv, frecv, f_r).wait()
        g32[...] = frecv[...].reshape(H * 8, 128).astype(F32)
        got = jnp.concatenate(
            [jnp.concatenate([g32[pl.ds(4 * i + m, H, stride=8), :] for m in range(4)], axis=1) for i in range(2)],
            axis=0).astype(BF)
        got = jnp.concatenate([got, got], axis=0)
        spec = jnp.dot(t_to[...], got, preferred_element_type=F32) * SCALE
        spec = jnp.concatenate(
            [jnp.concatenate([spec[i * H:(i + 1) * H, m * 128:(m + 1) * 128] for i in range(2)], axis=1)
             for m in range(4)], axis=0)
        hi, lo = parts(spec)
        first = jnp.dot(jnp.concatenate([hi, hi, lo], axis=1), w1[...], preferred_element_type=F32) + b1[...]
        hi, lo = parts(jnp.maximum(first, 0.0))
        second = jnp.dot(jnp.concatenate([hi, hi, lo], axis=1), w2[...], preferred_element_type=F32) + b2[...]
        second = jnp.where(second > SHRINK, second - SHRINK,
                           jnp.where(second < -SHRINK, second + SHRINK, 0.0))
        second = jnp.concatenate(
            [jnp.concatenate([second[m * H:(m + 1) * H, i * 128:(i + 1) * 128] for m in range(4)], axis=1)
             for i in range(2)], axis=0)
        hi, lo = parts(second)
        rows = jnp.dot(t_fro[...], jnp.concatenate([hi, hi, lo], axis=0), preferred_element_type=F32)
        for i in range(2):
            for m in range(4):
                g32[pl.ds(4 * i + m, H, stride=8), :] = rows[i * H:(i + 1) * H, m * 128:(m + 1) * 128]
        bsend[...] = g32[...].reshape(H, 8, 128).astype(BF)

        for dx, dy, dz, dk in OTHERS:
            dl, dc = groups[dz][dy] * 2 + cores[dk], xs[dx]

            @pl.when(dc < OWN)
            def _(dl=dl, dc=dc):
                pltpu.make_async_remote_copy(
                    bsend.at[dl * OWN + dc], brecv.at[2 * c + blk, l // 2], b_s, b_r,
                    device_id=(dl, dc), device_id_type=MESH).start()

        @pl.when(owner)
        def _():
            pltpu.make_async_copy(bsend.at[row], brecv.at[2 * c + blk, l // 2], b_r).start()

            @pl.when(s == 0)
            def _():
                weights_1(1)
                sent_weights(1)
                send_state()
                weights_2(0)
                weights_2(1)
                weights_3(0)
                own_row()

            pltpu.make_async_copy(brecv, brecv, b_r).wait()

            packed = jnp.concatenate(
                [brecv[b].reshape(128, 128)[:, 0:BS].astype(F32) for b in range(NB)], axis=1).astype(BF)
            packed = jnp.concatenate([packed, packed], axis=0)
            v = x[...] + jnp.dot(back[...], packed, preferred_element_type=F32) * SCALE
            x[...] = v
            nb[...] = norm(v, par[1:2, :], par[3:4, :]).astype(BF)

            @pl.when(s == 0)
            def _():
                weights_4(0)

            for q in range(NC):
                for j in range(3):
                    cols = slice(j * 256, (j + 1) * 256)
                    weight = wts[q, 0, :, :, :, :, cols].reshape(D, 256)
                    pre = jnp.dot(nb[...], weight, preferred_element_type=F32) + smalls[q, 5:6, cols]
                    act = 0.5 * pre * (1.0 + lax.erf(pre * math.sqrt(0.5)))
                    hid[:, q * 768 + j * 256:q * 768 + (j + 1) * 256] = act.astype(BF)

            @pl.when(s == 0)
            def _():
                weights_3(1)
                weights_4(1)

            for j in range(3):
                cols = slice(j * 256, (j + 1) * 256)
                weight = wts[:, 1, :, :, :, :, cols].reshape(FF, 256)
                x[:, cols] = x[:, cols] + jnp.dot(hid[...], weight, preferred_element_type=F32) + par[4:5, cols]

            @pl.when(s < STEPS - 1)
            def _():
                sent_f(s)
                send_row()

            pltpu.make_async_copy(bsend.at[0:95], bsend.at[0:95], b_s).wait()

        @pl.when(jnp.logical_not(owner))
        def _():
            @pl.when(s == 0)
            def _():
                sent_weights(1)
                send_state()
                sent_f(s)

            pltpu.make_async_copy(bsend, bsend, b_s).wait()

        return carry

    def sent_f(s):
        @pl.when(s == 0)
        def _():
            pltpu.make_async_copy(bsend.at[0:93], bsend.at[0:93], f_s).wait()

        @pl.when(s > 0)
        def _():
            pltpu.make_async_copy(fsend.at[0:7], fsend.at[0:7], f_s).wait()
            pltpu.make_async_copy(fsend.at[7, 0:15], fsend.at[7, 0:15], f_s).wait()

    lax.fori_loop(0, STEPS, step, 0)

    @pl.when(owner)
    def _():
        sent_f(1)
        ref = wts.at[pl.ds(0, 3), 0]
        pltpu.make_async_copy(ref, ref, wd_s).wait()
        for m in range(2):
            for axis in range(2):
                take(wb_s, m, axis)
            take(wc_s, m)

    for i in range(OWN):
        @pl.when(c != i)
        def _(i=i):
            a, b = to_owner(i)
            a.wait_send()
            b.wait_send()

    for j in range(NC):
        @pl.when(c != j)
        def _(j=j):
            pltpu.make_async_copy(stat, stat, st_s.at[j]).wait()

    @pl.when(owner)
    def _():
        for j in range(NC):
            xin[j] = x[0:W, j * 192:(j + 1) * 192]
        for j in range(NC):
            @pl.when(c != j)
            def _(j=j):
                pltpu.make_async_remote_copy(
                    xin.at[j], out.at[c], o_s.at[j], o_r.at[c],
                    device_id=(l, j), device_id_type=MESH).start()

        pltpu.make_async_copy(xin.at[c], out.at[c], o_r.at[c]).start()

    for i in range(OWN):
        pltpu.make_async_copy(out.at[i], out.at[i], o_r.at[i]).wait()

    @pl.when(owner)
    def _():
        for j in range(NC):
            @pl.when(c != j)
            def _(j=j):
                pltpu.make_async_copy(xin.at[0], xin.at[0], o_s.at[j]).wait()


def local(
    state, norm_gains, channel_biases, filter_in, filter_in_bias, filter_out, filter_out_bias,
    up_weight, up_bias, down_weight,
):
    up = up_weight.reshape(2, 4, 2, 48, 768)
    down = down_weight.reshape(2, 4, 2, 48, 768)
    fwd, back, t_to, t_fro = tables()
    vm = pl.BlockSpec(memory_space=pltpu.VMEM)
    hbm = pl.BlockSpec(memory_space=pltpu.HBM)
    sem = pltpu.SemaphoreType.DMA
    result = pl.pallas_call(
        kernel,
        out_shape=jax.ShapeDtypeStruct((OWN, W, 192), F32),
        in_specs=[hbm] * 14,
        out_specs=vm,
        scratch_shapes=[
            pltpu.VMEM((OWN, W, 192), F32),
            pltpu.VMEM((2, 192), BF),
            pltpu.VMEM((3, 192), BF),
            pltpu.VMEM((2, 2, BS, BS), F32),
            pltpu.VMEM((2, 2, BS), F32),
            pltpu.VMEM((2, 2, BS, BS), F32),
            pltpu.VMEM((2, 2, BS), F32),
            pltpu.VMEM((D,), BF),
            pltpu.VMEM((128, 3 * R), BF),
            pltpu.VMEM((R, 256), BF),
            pltpu.VMEM((192, 384), BF),
            pltpu.VMEM((192, 576), BF),
            pltpu.VMEM((8, D), F32),
            sem((12,)),
            pltpu.VMEM((NC, W, 192), F32),
            pltpu.VMEM((NC, 8, D), F32),
            pltpu.VMEM((R, D), F32),
            pltpu.VMEM((R, D), BF),
            pltpu.VMEM((NB, G, 8, 128), BF),
            pltpu.VMEM((H, 8, 128), BF),
            pltpu.VMEM((H, 8, 128), BF),
            pltpu.VMEM((NB, G, 8, 128), BF),
            pltpu.VMEM((768, 256), BF),
            pltpu.VMEM((1, 256), F32),
            pltpu.VMEM((768, 256), BF),
            pltpu.VMEM((1, 256), F32),
            pltpu.VMEM((8, D), F32),
            pltpu.VMEM((R, FF), BF),
            pltpu.VMEM((768, 128), F32),
            pltpu.VMEM((3 * R, D), BF),
            pltpu.VMEM((NC, 2, 2, 4, 2, 48, 768), BF),
            pltpu.VMEM((640, 128), F32),
            pltpu.VMEM((8, 640), F32),
            pltpu.VMEM((NC, 8, 640), F32),
            sem((OWN,)), sem((NC,)), sem((OWN,)), sem((NC,)),
            sem, sem, sem, sem, sem((NC,)), sem((OWN,)),
            sem((2,)), sem((2, OWN)), sem((2,)), sem((2, 2)), sem((2, 2)), sem((2,)), sem((2,)), sem, sem((4, 2)), sem((NC,)), sem((NC,)),
        ],
        compiler_params=pltpu.CompilerParams(
            collective_id=0, has_side_effects=True, vmem_limit_bytes=64 * 1024 * 1024 - 65536),
        name="rollout",
    )(
        state[0], norm_gains, channel_biases, filter_in, filter_in_bias, filter_out, filter_out_bias,
        up, up_bias, down, jnp.asarray(fwd), jnp.asarray(back), jnp.asarray(t_to), jnp.asarray(t_fro),
    )
    return result[None]


def solution(mesh):
    placed = (
        P(None, "lat", None, "ch"),
        P(None, "ch"),
        P(None, "ch"),
        P(None, "ch", None, None),
        P(None, "ch", None),
        P(None, "ch", None, None),
        P(None, "ch", None),
        P(None, "ch"),
        P("ch"),
        P("ch", None),
    )
    return jax.shard_map(
        local, mesh=mesh, in_specs=placed, out_specs=P(None, "lat", None, "ch"), check_vma=False
    )
```

```python
import itertools
import math

import jax
import jax.numpy as jnp
import numpy as np
from jax import lax
from jax.experimental import pallas as pl
from jax.experimental.pallas import tpu as pltpu
from jax.sharding import PartitionSpec as P

D = 768
FF = 3072
W = 180
R = 192
H = 96
M = 64
NB = 8
BS = 96
STEPS = 4
NL = 32
NC = 4
ND = NL * NC
OWN = 3
G = 16
SCALE = 1.0 / math.sqrt(H * W)
EPS = 1e-05
SHRINK = 0.01
HOPS = (0, 1, 2, 1)
OTHERS = sorted(
    (o for o in itertools.product(range(4), range(4), range(4), range(2)) if any(o)),
    key=lambda o: -(HOPS[o[0]] + HOPS[o[1]] + HOPS[o[2]] + 0.3 * o[3]),
)
MESH = pl.DeviceIdType.MESH
BF = jnp.bfloat16
F32 = jnp.float32


def tables():
    modes = np.arange(M)
    w = np.arange(W)
    ang = 2.0 * np.pi / W * ((w[:, None] * modes[None, :]) % W)
    c, s = np.cos(ang), np.sin(ang)
    dbl = np.where(modes == 0, 1.0, 2.0)
    fwd = np.zeros((G, 2, 4, R))
    fwd[:, 0, :, :W] = c.T.reshape(G, 4, W)
    fwd[:, 1, :, :W] = -s.T.reshape(G, 4, W)
    back = np.zeros((R, G, 2, 4))
    back[:W, :, 0, :] = (c * dbl).reshape(W, G, 4)
    back[:W, :, 1, :] = -(s * dbl).reshape(W, G, 4)
    h = np.arange(H)
    ang = 2.0 * np.pi / H * ((h[:, None] * h[None, :]) % H)
    c, s = np.cos(ang), np.sin(ang)
    to = np.block([[c, s], [-s, c]])
    fro = to.T
    fwd, back = halves(fwd.reshape(128, R)), halves(back.reshape(R, 128))
    return (
        np.concatenate([fwd[0], fwd[1], fwd[0]], axis=1),
        np.concatenate(back, axis=1),
        np.concatenate(halves(to), axis=1),
        np.concatenate([halves(fro)[0], halves(fro)[1], halves(fro)[0]], axis=1),
    )


def halves(a):
    a = np.asarray(a, np.float32)
    hi = a.astype(BF)
    return hi, (a - hi.astype(np.float32)).astype(BF)


def parts(v):
    hi = v.astype(BF)
    return hi, (v - hi.astype(F32)).astype(BF)


def norm(v, gain, shift):
    mean = jnp.sum(v, -1, keepdims=True) / D
    spread = jnp.sum(v * v, -1, keepdims=True) / D - mean * mean
    return (v - mean) * lax.rsqrt(spread + EPS) * gain + shift


def kernel(
    state_h, gains_h, biases_h, fin_h, finb_h, fout_h, foutb_h, up, upb_h, down, fwd_h, back_h, to_h, fro_h,
    out,
    lines, state, gains, biases, fin, finb, fout, foutb, upb, fwd, back, t_to, t_fro, small, h_s,
    xin, ends, smalls, x, nb, fsend, frecv, bsend, brecv, w1, b1, w2, b2, par, hid, g32, n3, wts, tall, stat, stats,
    in_s, in_r, sm_s, sm_r, f_s, f_r, b_s, b_r, o_s, o_r,
    own_r, wa_s, wa_r, wb_s, wb_r, wc_s, wc_r, wd_s, wd_r, st_s, st_r,
):
    l = lax.axis_index("lat")
    c = lax.axis_index("ch")
    me = l * NC + c
    row = l * OWN + c
    blk = lax.rem(l, 2)
    owner = c < OWN

    k = lax.rem(l, 2)
    cy = lax.rem(l // 2, 4)
    cz = l // 8
    xs = [lax.rem(c + i, 4) for i in range(4)]
    groups = [[lax.rem(cz + i, 4) * 4 + lax.rem(cy + j, 4) for j in range(4)] for i in range(4)]
    cores = (k, 1 - k)

    fetches = [
        pltpu.make_async_copy(src, dst, h_s.at[i])
        for i, (src, dst) in enumerate((
            (to_h, t_to), (fro_h, t_fro), (fin_h, fin), (fout_h, fout), (finb_h, finb), (foutb_h, foutb),
            (gains_h, gains), (biases_h, biases), (upb_h, upb), (fwd_h, fwd), (back_h, back), (state_h, lines)))
    ]
    for fetch in fetches:
        fetch.start()

    barrier = pltpu.get_barrier_semaphore()
    for dx, dy, dz, dk in OTHERS:
        pl.semaphore_signal(
            barrier, inc=1, device_id=(groups[dz][dy] * 2 + cores[dk], xs[dx]), device_id_type=MESH)

    def to_owner(i):
        return (
            pltpu.make_async_remote_copy(
                state.at[i], xin.at[c], in_s.at[i], in_r.at[c],
                device_id=(l, i), device_id_type=MESH),
            pltpu.make_async_remote_copy(
                small, smalls.at[c], sm_s.at[i], sm_r.at[c],
                device_id=(l, i), device_id_type=MESH),
        )

    py, pz = lax.rem(cy, 2), lax.rem(cz, 2)
    mine = 2 * pz + py
    at_y, at_z, at_d = 2 * pz + 1 - py, 2 * (1 - pz) + py, 2 * (1 - pz) + 1 - py
    shards = (up, down)

    def foreign(j):
        return lax.rem(c + 1 + j, NC)

    three = wts.at[0, 0, 0, pl.ds(0, 3), 0]

    def take(sems, *at):
        pltpu.make_async_copy(three, three, sems.at[at] if at else sems).wait()

    def pass_on(t, piece, axis, s_sem, r_sem):
        for j in range(3):
            for half, sign in ((0, 1), (1, 3)):
                ref = wts.at[foreign(j), t // 2, k, piece, t % 2, :, pl.ds(half * 384, 384)]
                to = groups[(0, sign)[axis]][(sign, 0)[axis]] * 2 + k
                pltpu.make_async_remote_copy(
                    ref, ref, s_sem, r_sem, device_id=(to, c), device_id_type=MESH).start()

    def share(t, piece, stage):
        for j in range(3):
            ref = wts.at[foreign(j), t // 2, k, piece, t % 2]
            pltpu.make_async_remote_copy(
                ref, ref, wd_s, wd_r.at[t, stage], device_id=(groups[0][0] * 2 + 1 - k, c),
                device_id_type=MESH).start()

    @pl.when(owner)
    def _():
        for m in range(2):
            pltpu.make_async_copy(shards[m], wts.at[c, m], own_r.at[m]).start()

    def weights_0(t):
        for i in range(OWN):
            @pl.when(c != i)
            def _(i=i):
                pltpu.make_async_remote_copy(
                    shards[t // 2].at[k, mine, t % 2], wts.at[c, t // 2, k, mine, t % 2],
                    wa_s.at[t, i], wa_r.at[t], device_id=(l, i), device_id_type=MESH).start()

    def sent_weights(t):
        for i in range(OWN):
            @pl.when(c != i)
            def _(i=i):
                ref = shards[t // 2].at[k, mine, t % 2]
                pltpu.make_async_copy(ref, ref, wa_s.at[t, i]).wait()

    def weights_1(t):
        take(wa_r, t)
        for axis in range(2):
            pass_on(t, mine, axis, wb_s.at[t, axis], wb_r.at[t, axis])
        share(t, mine, 0)

    def weights_2(t):
        u = t % 2
        take(wb_r, t, 1 - u)
        pass_on(t, (at_z, at_y)[u], u, wc_s.at[t], wc_r.at[t])
        share(t, (at_z, at_y)[u], 2)
        take(wb_r, t, u)
        share(t, (at_y, at_z)[u], 1)

    def weights_3(t):
        take(wc_r, t)
        share(t, at_d, 3)

    def weights_4(m):
        pltpu.make_async_copy(wts.at[c, m], wts.at[c, m], own_r.at[m]).wait()
        for t in (2 * m, 2 * m + 1):
            for stage in range(4):
                take(wd_r, t, stage)

    fsend[...] = jnp.zeros_like(fsend)
    n3[...] = jnp.zeros_like(n3)
    tall[...] = jnp.zeros_like(tall)
    small[...] = jnp.zeros_like(small)
    for fetch in fetches:
        fetch.wait()
    state[...] = lines[...].reshape(OWN, W, 192)
    small[0:2, 0:192] = gains[...].astype(F32)
    small[2:5, 0:192] = biases[...].astype(F32)
    small[5:6, :] = upb[...].astype(F32).reshape(1, D)
    for w_ref, b_ref, src, bsrc in ((w1, b1, fin, finb), (w2, b2, fout, foutb)):
        w_ref[...] = jnp.zeros_like(w_ref)
        b_ref[...] = jnp.zeros_like(b_ref)
        for at, re, im in zip((0, 256), parts(src[0, blk]), parts(src[1, blk])):
            w_ref[at:at + BS, 0:BS] = re
            w_ref[at:at + BS, 128:128 + BS] = im
            w_ref[at + 128:at + 128 + BS, 0:BS] = -im
            w_ref[at + 128:at + 128 + BS, 128:128 + BS] = re
        w_ref[512:768, :] = w_ref[0:256, :]
        b_ref[:, 0:BS] = bsrc[0, pl.ds(blk, 1), :]
        b_ref[:, 128:128 + BS] = bsrc[1, pl.ds(blk, 1), :]


    lane = lax.broadcasted_iota(jnp.int32, (W, 128), 1)
    for r in range(OWN):
        v = state[r]
        total = jnp.sum(v, -1, keepdims=True)
        squares = jnp.sum(v * v, -1, keepdims=True)
        tall[r * R:r * R + W, :] = jnp.where(lane == 0, total, jnp.where(lane == 1, squares, 0.0))
    stat[...] = tall[...].T[0:8, :]

    pl.semaphore_wait(barrier, ND - 1)
    for j in range(NC):
        @pl.when(c != j)
        def _(j=j):
            pltpu.make_async_remote_copy(
                stat, stats.at[c], st_s.at[j], st_r.at[c], device_id=(l, j), device_id_type=MESH).start()

        @pl.when(c == j)
        def _(j=j):
            pltpu.make_async_copy(stat, stats.at[j], st_r.at[j]).start()

    weights_0(0)
    for j in range(NC):
        pltpu.make_async_copy(stats.at[j], stats.at[j], st_r.at[j]).wait()
    weights_0(1)
    total = (stats[0] + stats[1]) + (stats[2] + stats[3])
    mean = total[0:1] / D
    spread = lax.rsqrt(total[1:2] / D - mean * mean + EPS)
    line = lax.broadcasted_iota(jnp.int32, (128, 640), 0)
    tall[...] = jnp.where(line == 0, mean, jnp.where(line == 1, spread, 0.0)).T
    for r in range(OWN):
        at = slice(r * R, r * R + W)
        n = (state[r] - tall[at, 0:1]) * tall[at, 1:2] * small[0:1, 0:192] + small[2:3, 0:192]
        hi, lo = parts(n)
        n3[0:W, 0:192] = hi
        n3[R:R + W, 0:192] = hi
        n3[2 * R:2 * R + W, 0:192] = lo
        lon = jnp.dot(fwd[...], n3[:, 0:192], preferred_element_type=F32)
        for j in range(2):
            fsend[2 * r + j, :, :, 0:BS] = lon[:, j * BS:(j + 1) * BS].reshape(G, 8, BS).astype(BF)

    for dx, dy, dz, dk in OTHERS:
        if dx:
            continue
        for r in range(OWN):
            pltpu.make_async_remote_copy(
                fsend.at[2 * r + cores[dk], groups[dz][dy]], frecv.at[l * OWN + r], f_s, f_r,
                device_id=(groups[dz][dy] * 2 + cores[dk], c), device_id_type=MESH).start()
    for r in range(OWN):
        pltpu.make_async_copy(fsend.at[2 * r + blk, l // 2], frecv.at[l * OWN + r], f_r).start()
    sent_weights(0)
    pl.when(owner)(lambda: weights_1(0))
    sent_weights(1)
    weights_0(2)
    pl.when(owner)(lambda: weights_1(1))

    def send_state():
        for i in range(OWN):
            @pl.when(c != i)
            def _(i=i):
                a, b = to_owner(i)
                a.start()
                b.start()

            @pl.when(c == i)
            def _(i=i):
                pltpu.make_async_copy(state.at[i], xin.at[i], in_r.at[i]).start()
                pltpu.make_async_copy(small, smalls.at[i], sm_r.at[i]).start()

    def own_row():
        for j in range(NC):
            pltpu.make_async_copy(xin.at[j], xin.at[j], in_r.at[j]).wait()
            pltpu.make_async_copy(smalls.at[j], smalls.at[j], sm_r.at[j]).wait()
        par[0:5, :] = jnp.concatenate([smalls[j, 0:5, 0:192] for j in range(NC)], axis=1)
        v = jnp.concatenate([xin[j] for j in range(NC)], axis=1)
        x[0:W, :] = v + norm(v, par[0:1, :], par[2:3, :])
        x[W:R, :] = jnp.zeros((R - W, D), F32)

    def send_row():
        v = x[...]
        n = norm(v, par[0:1, :], par[2:3, :])
        x[...] = v + n
        hi, lo = parts(n)
        n3[0:R, :] = hi
        n3[R:2 * R, :] = hi
        n3[2 * R:3 * R, :] = lo
        lon = jnp.dot(fwd[...], n3[...], preferred_element_type=F32)
        for b in range(NB):
            fsend[b, :, :, 0:BS] = lon[:, b * BS:(b + 1) * BS].reshape(G, 8, BS).astype(BF)

        for dx, dy, dz, dk in OTHERS:
            pltpu.make_async_remote_copy(
                fsend.at[2 * xs[dx] + cores[dk], groups[dz][dy]], frecv.at[row], f_s, f_r,
                device_id=(groups[dz][dy] * 2 + cores[dk], xs[dx]), device_id_type=MESH).start()
        pltpu.make_async_copy(
            fsend.at[2 * c + blk, l // 2], frecv.at[row], f_r).start()

    def step(s, carry):
        pltpu.make_async_copy(frecv, frecv, f_r).wait()

        @pl.when(s == 0)
        def _():
            sent_weights(2)
            weights_0(3)

            @pl.when(owner)
            def _():
                weights_2(0)
                weights_1(2)


        g32[...] = frecv[...].reshape(H * 8, 128).astype(F32)
        got = jnp.concatenate(
            [jnp.concatenate([g32[pl.ds(4 * i + m, H, stride=8), :] for m in range(4)], axis=1) for i in range(2)],
            axis=0).astype(BF)
        got = jnp.concatenate([got, got], axis=0)
        spec = jnp.dot(t_to[...], got, preferred_element_type=F32) * SCALE
        spec = jnp.concatenate(
            [jnp.concatenate([spec[i * H:(i + 1) * H, m * 128:(m + 1) * 128] for i in range(2)], axis=1)
             for m in range(4)], axis=0)
        hi, lo = parts(spec)
        first = jnp.dot(jnp.concatenate([hi, hi, lo], axis=1), w1[...], preferred_element_type=F32) + b1[...]
        hi, lo = parts(jnp.maximum(first, 0.0))
        second = jnp.dot(jnp.concatenate([hi, hi, lo], axis=1), w2[...], preferred_element_type=F32) + b2[...]
        second = jnp.where(second > SHRINK, second - SHRINK,
                           jnp.where(second < -SHRINK, second + SHRINK, 0.0))
        second = jnp.concatenate(
            [jnp.concatenate([second[m * H:(m + 1) * H, i * 128:(i + 1) * 128] for m in range(4)], axis=1)
             for i in range(2)], axis=0)
        hi, lo = parts(second)
        rows = jnp.dot(t_fro[...], jnp.concatenate([hi, hi, lo], axis=0), preferred_element_type=F32)
        for i in range(2):
            for m in range(4):
                g32[pl.ds(4 * i + m, H, stride=8), :] = rows[i * H:(i + 1) * H, m * 128:(m + 1) * 128]
        bsend[...] = g32[...].reshape(H, 8, 128).astype(BF)

        for dx, dy, dz, dk in OTHERS:
            dl, dc = groups[dz][dy] * 2 + cores[dk], xs[dx]

            @pl.when(dc < OWN)
            def _(dl=dl, dc=dc):
                pltpu.make_async_remote_copy(
                    bsend.at[dl * OWN + dc], brecv.at[2 * c + blk, l // 2], b_s, b_r,
                    device_id=(dl, dc), device_id_type=MESH).start()

        @pl.when(owner)
        def _():
            pltpu.make_async_copy(bsend.at[row], brecv.at[2 * c + blk, l // 2], b_r).start()

            @pl.when(s == 0)
            def _():
                weights_2(1)
                weights_1(3)
                sent_weights(3)
                send_state()
                weights_2(2)
                weights_3(0)
                weights_3(1)
                weights_2(3)
                own_row()
                weights_3(2)

            pltpu.make_async_copy(brecv, brecv, b_r).wait()

            packed = jnp.concatenate(
                [brecv[b].reshape(128, 128)[:, 0:BS].astype(F32) for b in range(NB)], axis=1).astype(BF)
            packed = jnp.concatenate([packed, packed], axis=0)
            v = x[...] + jnp.dot(back[...], packed, preferred_element_type=F32) * SCALE
            x[...] = v
            nb[...] = norm(v, par[1:2, :], par[3:4, :]).astype(BF)

            @pl.when(s == 0)
            def _():
                weights_3(3)
                weights_4(0)

            for q in range(NC):
                for j in range(3):
                    cols = slice(j * 256, (j + 1) * 256)
                    weight = wts[q, 0, :, :, :, :, cols].reshape(D, 256)
                    pre = jnp.dot(nb[...], weight, preferred_element_type=F32) + smalls[q, 5:6, cols]
                    act = 0.5 * pre * (1.0 + lax.erf(pre * math.sqrt(0.5)))
                    hid[:, q * 768 + j * 256:q * 768 + (j + 1) * 256] = act.astype(BF)

            @pl.when(s == 0)
            def _():
                weights_4(1)

            for j in range(3):
                cols = slice(j * 256, (j + 1) * 256)
                weight = wts[:, 1, :, :, :, :, cols].reshape(FF, 256)
                x[:, cols] = x[:, cols] + jnp.dot(hid[...], weight, preferred_element_type=F32) + par[4:5, cols]

            @pl.when(s < STEPS - 1)
            def _():
                sent_f(s)
                send_row()

            pltpu.make_async_copy(bsend.at[0:95], bsend.at[0:95], b_s).wait()

        @pl.when(jnp.logical_not(owner))
        def _():
            @pl.when(s == 0)
            def _():
                sent_weights(3)
                send_state()
                sent_f(s)

            pltpu.make_async_copy(bsend, bsend, b_s).wait()

        return carry

    def sent_f(s):
        @pl.when(s == 0)
        def _():
            pltpu.make_async_copy(bsend.at[0:93], bsend.at[0:93], f_s).wait()

        @pl.when(s > 0)
        def _():
            pltpu.make_async_copy(fsend.at[0:7], fsend.at[0:7], f_s).wait()
            pltpu.make_async_copy(fsend.at[7, 0:15], fsend.at[7, 0:15], f_s).wait()

    lax.fori_loop(0, STEPS, step, 0)

    @pl.when(owner)
    def _():
        sent_f(1)
        ref = wts.at[pl.ds(0, 3), 0]
        pltpu.make_async_copy(ref, ref, wd_s).wait()
        for t in range(4):
            for axis in range(2):
                take(wb_s, t, axis)
            take(wc_s, t)

    for i in range(OWN):
        @pl.when(c != i)
        def _(i=i):
            a, b = to_owner(i)
            a.wait_send()
            b.wait_send()

    for j in range(NC):
        @pl.when(c != j)
        def _(j=j):
            pltpu.make_async_copy(stat, stat, st_s.at[j]).wait()

    @pl.when(owner)
    def _():
        for j in range(NC):
            xin[j] = x[0:W, j * 192:(j + 1) * 192]
        for j in range(NC):
            @pl.when(c != j)
            def _(j=j):
                pltpu.make_async_remote_copy(
                    xin.at[j], ends.at[c], o_s.at[j], o_r.at[c],
                    device_id=(l, j), device_id_type=MESH).start()

        pltpu.make_async_copy(xin.at[c], ends.at[c], o_r.at[c]).start()

    for i in range(OWN):
        pltpu.make_async_copy(ends.at[i], ends.at[i], o_r.at[i]).wait()
        out[i] = ends[i].reshape(W, 1, 192)

    @pl.when(owner)
    def _():
        for j in range(NC):
            @pl.when(c != j)
            def _(j=j):
                pltpu.make_async_copy(xin.at[0], xin.at[0], o_s.at[j]).wait()


def local(
    state, norm_gains, channel_biases, filter_in, filter_in_bias, filter_out, filter_out_bias,
    up_weight, up_bias, down_weight,
):
    up = up_weight.reshape(2, 4, 2, 48, 768)
    down = down_weight.reshape(2, 4, 2, 48, 768)
    fwd, back, t_to, t_fro = tables()
    vm = pl.BlockSpec(memory_space=pltpu.VMEM)
    hbm = pl.BlockSpec(memory_space=pltpu.HBM)
    sem = pltpu.SemaphoreType.DMA
    result = pl.pallas_call(
        kernel,
        out_shape=jax.ShapeDtypeStruct((OWN, W, 1, 192), F32),
        in_specs=[hbm] * 14,
        out_specs=vm,
        scratch_shapes=[
            pltpu.VMEM((OWN, W, 1, 192), F32),
            pltpu.VMEM((OWN, W, 192), F32),
            pltpu.VMEM((2, 192), BF),
            pltpu.VMEM((3, 192), BF),
            pltpu.VMEM((2, 2, BS, BS), F32),
            pltpu.VMEM((2, 2, BS), F32),
            pltpu.VMEM((2, 2, BS, BS), F32),
            pltpu.VMEM((2, 2, BS), F32),
            pltpu.VMEM((D,), BF),
            pltpu.VMEM((128, 3 * R), BF),
            pltpu.VMEM((R, 256), BF),
            pltpu.VMEM((192, 384), BF),
            pltpu.VMEM((192, 576), BF),
            pltpu.VMEM((8, D), F32),
            sem((12,)),
            pltpu.VMEM((NC, W, 192), F32),
            pltpu.VMEM((OWN, W, 192), F32),
            pltpu.VMEM((NC, 8, D), F32),
            pltpu.VMEM((R, D), F32),
            pltpu.VMEM((R, D), BF),
            pltpu.VMEM((NB, G, 8, 128), BF),
            pltpu.VMEM((H, 8, 128), BF),
            pltpu.VMEM((H, 8, 128), BF),
            pltpu.VMEM((NB, G, 8, 128), BF),
            pltpu.VMEM((768, 256), BF),
            pltpu.VMEM((1, 256), F32),
            pltpu.VMEM((768, 256), BF),
            pltpu.VMEM((1, 256), F32),
            pltpu.VMEM((8, D), F32),
            pltpu.VMEM((R, FF), BF),
            pltpu.VMEM((768, 128), F32),
            pltpu.VMEM((3 * R, D), BF),
            pltpu.VMEM((NC, 2, 2, 4, 2, 48, 768), BF),
            pltpu.VMEM((640, 128), F32),
            pltpu.VMEM((8, 640), F32),
            pltpu.VMEM((NC, 8, 640), F32),
            sem((OWN,)), sem((NC,)), sem((OWN,)), sem((NC,)),
            sem, sem, sem, sem, sem((NC,)), sem((OWN,)),
            sem((2,)), sem((4, OWN)), sem((4,)), sem((4, 2)), sem((4, 2)), sem((4,)), sem((4,)), sem, sem((4, 4)), sem((NC,)), sem((NC,)),
        ],
        compiler_params=pltpu.CompilerParams(
            collective_id=0, has_side_effects=True, vmem_limit_bytes=62 * 1024 * 1024),
        name="rollout",
    )(
        state.reshape(OWN, W, 1, 192), norm_gains, channel_biases, filter_in, filter_in_bias, filter_out, filter_out_bias,
        up, up_bias, down, jnp.asarray(fwd), jnp.asarray(back), jnp.asarray(t_to), jnp.asarray(t_fro),
    )
    return result.reshape(1, OWN, W, 192)


def solution(mesh):
    placed = (
        P(None, "lat", None, "ch"),
        P(None, "ch"),
        P(None, "ch"),
        P(None, "ch", None, None),
        P(None, "ch", None),
        P(None, "ch", None, None),
        P(None, "ch", None),
        P(None, "ch"),
        P("ch"),
        P("ch", None),
    )
    return jax.shard_map(
        local, mesh=mesh, in_specs=placed, out_specs=P(None, "lat", None, "ch"), check_vma=False
    )
```

```python
import itertools
import math

import jax
import jax.numpy as jnp
import numpy as np
from jax import lax
from jax.experimental import pallas as pl
from jax.experimental.pallas import tpu as pltpu
from jax.sharding import PartitionSpec as P

D = 768
FF = 3072
W = 180
R = 192
H = 96
M = 64
NB = 8
BS = 96
STEPS = 4
NL = 32
NC = 4
ND = NL * NC
OWN = 3
G = 16
SCALE = 1.0 / math.sqrt(H * W)
EPS = 1e-05
SHRINK = 0.01
HOPS = (0, 1, 2, 1)
OTHERS = sorted(
    (o for o in itertools.product(range(4), range(4), range(4), range(2)) if any(o)),
    key=lambda o: -(HOPS[o[0]] + HOPS[o[1]] + HOPS[o[2]] + 0.3 * o[3]),
)
MESH = pl.DeviceIdType.MESH
BF = jnp.bfloat16
F32 = jnp.float32


def tables():
    modes = np.arange(M)
    w = np.arange(W)
    ang = 2.0 * np.pi / W * ((w[:, None] * modes[None, :]) % W)
    c, s = np.cos(ang), np.sin(ang)
    dbl = np.where(modes == 0, 1.0, 2.0)
    fwd = np.zeros((G, 2, 4, R))
    fwd[:, 0, :, :W] = c.T.reshape(G, 4, W)
    fwd[:, 1, :, :W] = -s.T.reshape(G, 4, W)
    back = np.zeros((R, G, 2, 4))
    back[:W, :, 0, :] = (c * dbl).reshape(W, G, 4)
    back[:W, :, 1, :] = -(s * dbl).reshape(W, G, 4)
    h = np.arange(H)
    ang = 2.0 * np.pi / H * ((h[:, None] * h[None, :]) % H)
    c, s = np.cos(ang), np.sin(ang)
    to = np.block([[c, s], [-s, c]])
    fro = to.T
    fwd, back = halves(fwd.reshape(128, R)), halves(back.reshape(R, 128))
    return (
        np.concatenate([fwd[0], fwd[1], fwd[0]], axis=1),
        np.concatenate(back, axis=1),
        np.concatenate(halves(to), axis=1),
        np.concatenate([halves(fro)[0], halves(fro)[1], halves(fro)[0]], axis=1),
    )


def halves(a):
    a = np.asarray(a, np.float32)
    hi = a.astype(BF)
    return hi, (a - hi.astype(np.float32)).astype(BF)


def parts(v):
    hi = v.astype(BF)
    return hi, (v - hi.astype(F32)).astype(BF)


def norm(v, gain, shift):
    mean = jnp.sum(v, -1, keepdims=True) / D
    spread = jnp.sum(v * v, -1, keepdims=True) / D - mean * mean
    return (v - mean) * lax.rsqrt(spread + EPS) * gain + shift


def kernel(
    state_h, gains_h, biases_h, fin_h, finb_h, fout_h, foutb_h, up, upb_h, down, fwd_h, back_h, to_h, fro_h,
    out,
    lines, state, gains, biases, fin, finb, fout, foutb, upb, fwd, back, t_to, t_fro, small, h_s,
    xin, ends, smalls, x, nb, fsend, frecv, bsend, brecv, w1, b1, w2, b2, par, hid, g32, n3, wts, tall, stat, stats,
    in_s, in_r, sm_s, sm_r, f_s, f_r, b_s, b_r, o_s, o_r,
    own_r, wa_s, wa_r, wb_s, wb_r, wc_s, wc_r, wd_s, wd_r, st_s, st_r,
):
    l = lax.axis_index("lat")
    c = lax.axis_index("ch")
    me = l * NC + c
    row = l * OWN + c
    blk = lax.rem(l, 2)
    owner = c < OWN

    k = lax.rem(l, 2)
    cy = lax.rem(l // 2, 4)
    cz = l // 8
    xs = [lax.rem(c + i, 4) for i in range(4)]
    groups = [[lax.rem(cz + i, 4) * 4 + lax.rem(cy + j, 4) for j in range(4)] for i in range(4)]
    cores = (k, 1 - k)

    fetches = [
        pltpu.make_async_copy(src, dst, h_s.at[i])
        for i, (src, dst) in enumerate((
            (to_h, t_to), (fro_h, t_fro), (fin_h, fin), (fout_h, fout), (finb_h, finb), (foutb_h, foutb),
            (gains_h, gains), (biases_h, biases), (upb_h, upb), (fwd_h, fwd), (back_h, back), (state_h, lines)))
    ]
    for fetch in fetches:
        fetch.start()

    barrier = pltpu.get_barrier_semaphore()
    for dx, dy, dz, dk in OTHERS:
        pl.semaphore_signal(
            barrier, inc=1, device_id=(groups[dz][dy] * 2 + cores[dk], xs[dx]), device_id_type=MESH)

    def to_owner(i):
        return (
            pltpu.make_async_remote_copy(
                state.at[i], xin.at[c], in_s.at[i], in_r.at[c],
                device_id=(l, i), device_id_type=MESH),
            pltpu.make_async_remote_copy(
                small, smalls.at[c], sm_s.at[i], sm_r.at[c],
                device_id=(l, i), device_id_type=MESH),
        )

    py, pz = lax.rem(cy, 2), lax.rem(cz, 2)
    mine = 2 * pz + py
    at_y, at_z, at_d = 2 * pz + 1 - py, 2 * (1 - pz) + py, 2 * (1 - pz) + 1 - py
    shards = (up, down)

    def foreign(j):
        return lax.rem(c + 1 + j, NC)

    three = wts.at[0, 0, 0, pl.ds(0, 3), 0]

    def take(sems, *at):
        pltpu.make_async_copy(three, three, sems.at[at] if at else sems).wait()

    def pass_on(t, piece, axis, s_sem, r_sem):
        for j in range(3):
            for half, sign in ((0, 1), (1, 3)):
                ref = wts.at[foreign(j), t // 2, k, piece, t % 2, :, pl.ds(half * 384, 384)]
                to = groups[(0, sign)[axis]][(sign, 0)[axis]] * 2 + k
                pltpu.make_async_remote_copy(
                    ref, ref, s_sem, r_sem, device_id=(to, c), device_id_type=MESH).start()

    def share(t, piece, stage):
        for j in range(3):
            ref = wts.at[foreign(j), t // 2, k, piece, t % 2]
            pltpu.make_async_remote_copy(
                ref, ref, wd_s, wd_r.at[t, stage], device_id=(groups[0][0] * 2 + 1 - k, c),
                device_id_type=MESH).start()

    @pl.when(owner)
    def _():
        for m in range(2):
            pltpu.make_async_copy(shards[m], wts.at[c, m], own_r.at[m]).start()

    def weights_0(t):
        for i in range(OWN):
            @pl.when(c != i)
            def _(i=i):
                pltpu.make_async_remote_copy(
                    shards[t // 2].at[k, mine, t % 2], wts.at[c, t // 2, k, mine, t % 2],
                    wa_s.at[t, i], wa_r.at[t], device_id=(l, i), device_id_type=MESH).start()

    def sent_weights(t):
        for i in range(OWN):
            @pl.when(c != i)
            def _(i=i):
                ref = shards[t // 2].at[k, mine, t % 2]
                pltpu.make_async_copy(ref, ref, wa_s.at[t, i]).wait()

    def weights_1(t):
        take(wa_r, t)
        for axis in range(2):
            pass_on(t, mine, axis, wb_s.at[t, axis], wb_r.at[t, axis])
        share(t, mine, 0)

    def weights_2(t):
        u = t % 2
        take(wb_r, t, 1 - u)
        pass_on(t, (at_z, at_y)[u], u, wc_s.at[t], wc_r.at[t])
        share(t, (at_z, at_y)[u], 2)
        take(wb_r, t, u)
        share(t, (at_y, at_z)[u], 1)

    def weights_3(t):
        take(wc_r, t)
        share(t, at_d, 3)

    def weights_4(m):
        pltpu.make_async_copy(wts.at[c, m], wts.at[c, m], own_r.at[m]).wait()
        for t in (2 * m, 2 * m + 1):
            for stage in range(4):
                take(wd_r, t, stage)

    fsend[...] = jnp.zeros_like(fsend)
    n3[...] = jnp.zeros_like(n3)
    tall[...] = jnp.zeros_like(tall)
    small[...] = jnp.zeros_like(small)
    for fetch in fetches:
        fetch.wait()
    state[...] = lines[...].reshape(OWN, W, 192)
    small[0:2, 0:192] = gains[...].astype(F32)
    small[2:5, 0:192] = biases[...].astype(F32)
    small[5:6, :] = upb[...].astype(F32).reshape(1, D)
    for w_ref, b_ref, src, bsrc in ((w1, b1, fin, finb), (w2, b2, fout, foutb)):
        w_ref[...] = jnp.zeros_like(w_ref)
        b_ref[...] = jnp.zeros_like(b_ref)
        for at, re, im in zip((0, 256), parts(src[0, blk]), parts(src[1, blk])):
            w_ref[at:at + BS, 0:BS] = re
            w_ref[at:at + BS, 128:128 + BS] = im
            w_ref[at + 128:at + 128 + BS, 0:BS] = -im
            w_ref[at + 128:at + 128 + BS, 128:128 + BS] = re
        w_ref[512:768, :] = w_ref[0:256, :]
        b_ref[:, 0:BS] = bsrc[0, pl.ds(blk, 1), :]
        b_ref[:, 128:128 + BS] = bsrc[1, pl.ds(blk, 1), :]


    lane = lax.broadcasted_iota(jnp.int32, (W, 128), 1)
    for r in range(OWN):
        v = state[r]
        total = jnp.sum(v, -1, keepdims=True)
        squares = jnp.sum(v * v, -1, keepdims=True)
        tall[r * R:r * R + W, :] = jnp.where(lane == 0, total, jnp.where(lane == 1, squares, 0.0))
    stat[...] = tall[...].T[0:8, :]

    pl.semaphore_wait(barrier, ND - 1)
    for j in range(NC):
        @pl.when(c != j)
        def _(j=j):
            pltpu.make_async_remote_copy(
                stat, stats.at[c], st_s.at[j], st_r.at[c], device_id=(l, j), device_id_type=MESH).start()

        @pl.when(c == j)
        def _(j=j):
            pltpu.make_async_copy(stat, stats.at[j], st_r.at[j]).start()

    weights_0(0)
    for j in range(NC):
        pltpu.make_async_copy(stats.at[j], stats.at[j], st_r.at[j]).wait()
    weights_0(1)
    total = (stats[0] + stats[1]) + (stats[2] + stats[3])
    mean = total[0:1] / D
    spread = lax.rsqrt(total[1:2] / D - mean * mean + EPS)
    line = lax.broadcasted_iota(jnp.int32, (128, 640), 0)
    tall[...] = jnp.where(line == 0, mean, jnp.where(line == 1, spread, 0.0)).T
    for r in range(OWN):
        at = slice(r * R, r * R + W)
        n = (state[r] - tall[at, 0:1]) * tall[at, 1:2] * small[0:1, 0:192] + small[2:3, 0:192]
        hi, lo = parts(n)
        n3[0:W, 0:192] = hi
        n3[R:R + W, 0:192] = hi
        n3[2 * R:2 * R + W, 0:192] = lo
        lon = jnp.dot(fwd[...], n3[:, 0:192], preferred_element_type=F32)
        for j in range(2):
            fsend[2 * r + j, :, :, 0:BS] = lon[:, j * BS:(j + 1) * BS].reshape(G, 8, BS).astype(BF)

    for dx, dy, dz, dk in OTHERS:
        if dx:
            continue
        for r in range(OWN):
            pltpu.make_async_remote_copy(
                fsend.at[2 * r + cores[dk], groups[dz][dy]], frecv.at[l * OWN + r], f_s, f_r,
                device_id=(groups[dz][dy] * 2 + cores[dk], c), device_id_type=MESH).start()
    for r in range(OWN):
        pltpu.make_async_copy(fsend.at[2 * r + blk, l // 2], frecv.at[l * OWN + r], f_r).start()
    sent_weights(0)
    pl.when(owner)(lambda: weights_1(0))
    sent_weights(1)
    weights_0(2)
    pl.when(owner)(lambda: weights_1(1))

    def send_state():
        for i in range(OWN):
            @pl.when(c != i)
            def _(i=i):
                a, b = to_owner(i)
                a.start()
                b.start()

            @pl.when(c == i)
            def _(i=i):
                pltpu.make_async_copy(state.at[i], xin.at[i], in_r.at[i]).start()
                pltpu.make_async_copy(small, smalls.at[i], sm_r.at[i]).start()

    def own_row():
        for j in range(NC):
            pltpu.make_async_copy(xin.at[j], xin.at[j], in_r.at[j]).wait()
            pltpu.make_async_copy(smalls.at[j], smalls.at[j], sm_r.at[j]).wait()
        par[0:5, :] = jnp.concatenate([smalls[j, 0:5, 0:192] for j in range(NC)], axis=1)
        v = jnp.concatenate([xin[j] for j in range(NC)], axis=1)
        x[0:W, :] = v + norm(v, par[0:1, :], par[2:3, :])
        x[W:R, :] = jnp.zeros((R - W, D), F32)

    def send_row():
        v = x[...]
        n = norm(v, par[0:1, :], par[2:3, :])
        x[...] = v + n
        hi, lo = parts(n)
        n3[0:R, :] = hi
        n3[R:2 * R, :] = hi
        n3[2 * R:3 * R, :] = lo
        lon = jnp.dot(fwd[...], n3[...], preferred_element_type=F32)
        for b in range(NB):
            fsend[b, :, :, 0:BS] = lon[:, b * BS:(b + 1) * BS].reshape(G, 8, BS).astype(BF)

        for dx, dy, dz, dk in OTHERS:
            pltpu.make_async_remote_copy(
                fsend.at[2 * xs[dx] + cores[dk], groups[dz][dy]], frecv.at[row], f_s, f_r,
                device_id=(groups[dz][dy] * 2 + cores[dk], xs[dx]), device_id_type=MESH).start()
        pltpu.make_async_copy(
            fsend.at[2 * c + blk, l // 2], frecv.at[row], f_r).start()

    def step(s, carry):
        pltpu.make_async_copy(frecv, frecv, f_r).wait()

        @pl.when(s == 0)
        def _():
            sent_weights(2)
            weights_0(3)

            @pl.when(owner)
            def _():
                weights_2(0)
                weights_1(2)


        g32[...] = frecv[...].reshape(H * 8, 128).astype(F32)
        got = jnp.concatenate(
            [jnp.concatenate([g32[pl.ds(4 * i + m, H, stride=8), :] for m in range(4)], axis=1) for i in range(2)],
            axis=0).astype(BF)
        got = jnp.concatenate([got, got], axis=0)
        spec = jnp.dot(t_to[...], got, preferred_element_type=F32) * SCALE
        spec = jnp.concatenate(
            [jnp.concatenate([spec[i * H:(i + 1) * H, m * 128:(m + 1) * 128] for i in range(2)], axis=1)
             for m in range(4)], axis=0)
        hi, lo = parts(spec)
        first = jnp.dot(jnp.concatenate([hi, hi, lo], axis=1), w1[...], preferred_element_type=F32) + b1[...]
        hi, lo = parts(jnp.maximum(first, 0.0))
        second = jnp.dot(jnp.concatenate([hi, hi, lo], axis=1), w2[...], preferred_element_type=F32) + b2[...]
        second = jnp.where(second > SHRINK, second - SHRINK,
                           jnp.where(second < -SHRINK, second + SHRINK, 0.0))
        second = jnp.concatenate(
            [jnp.concatenate([second[m * H:(m + 1) * H, i * 128:(i + 1) * 128] for m in range(4)], axis=1)
             for i in range(2)], axis=0)
        hi, lo = parts(second)
        rows = jnp.dot(t_fro[...], jnp.concatenate([hi, hi, lo], axis=0), preferred_element_type=F32)
        for i in range(2):
            for m in range(4):
                g32[pl.ds(4 * i + m, H, stride=8), :] = rows[i * H:(i + 1) * H, m * 128:(m + 1) * 128]
        bsend[...] = g32[...].reshape(H, 8, 128).astype(BF)

        for dx, dy, dz, dk in OTHERS:
            dl, dc = groups[dz][dy] * 2 + cores[dk], xs[dx]

            @pl.when(dc < OWN)
            def _(dl=dl, dc=dc):
                pltpu.make_async_remote_copy(
                    bsend.at[dl * OWN + dc], brecv.at[2 * c + blk, l // 2], b_s, b_r,
                    device_id=(dl, dc), device_id_type=MESH).start()

        @pl.when(owner)
        def _():
            pltpu.make_async_copy(bsend.at[row], brecv.at[2 * c + blk, l // 2], b_r).start()

            @pl.when(s == 0)
            def _():
                weights_2(1)
                weights_1(3)
                sent_weights(3)
                send_state()
                weights_2(2)
                weights_3(0)
                weights_3(1)
                weights_2(3)
                own_row()
                weights_3(2)

            pltpu.make_async_copy(brecv, brecv, b_r).wait()

            packed = jnp.concatenate(
                [brecv[b].reshape(128, 128)[:, 0:BS].astype(F32) for b in range(NB)], axis=1).astype(BF)
            packed = jnp.concatenate([packed, packed], axis=0)
            v = x[...] + jnp.dot(back[...], packed, preferred_element_type=F32) * SCALE
            x[...] = v
            nb[...] = norm(v, par[1:2, :], par[3:4, :]).astype(BF)

            @pl.when(s == 0)
            def _():
                weights_3(3)
                weights_4(0)
                weights_4(1)

            def up_part(q):
                for j in range(3):
                    cols = slice(j * 256, (j + 1) * 256)
                    weight = wts[q, 0, :, :, :, :, cols].reshape(D, 256)
                    pre = jnp.dot(nb[...], weight, preferred_element_type=F32) + smalls[q, 5:6, cols]
                    act = 0.5 * pre * (1.0 + lax.erf(pre * math.sqrt(0.5)))
                    hid[:, q * 768 + j * 256:q * 768 + (j + 1) * 256] = act.astype(BF)

            def down_part(q):
                for j in range(3):
                    cols = slice(j * 256, (j + 1) * 256)
                    weight = wts[q, 1, :, :, :, :, cols].reshape(D, 256)
                    mixed = jnp.dot(hid[:, q * 768:(q + 1) * 768], weight, preferred_element_type=F32)
                    if q == 0:
                        mixed = mixed + par[4:5, cols]
                    x[:, cols] = x[:, cols] + mixed

            up_part(0)
            for q in range(1, NC):
                up_part(q)
                down_part(q - 1)
            down_part(NC - 1)

            @pl.when(s < STEPS - 1)
            def _():
                sent_f(s)
                send_row()

            pltpu.make_async_copy(bsend.at[0:95], bsend.at[0:95], b_s).wait()

        @pl.when(jnp.logical_not(owner))
        def _():
            @pl.when(s == 0)
            def _():
                sent_weights(3)
                send_state()
                sent_f(s)

            pltpu.make_async_copy(bsend, bsend, b_s).wait()

        return carry

    def sent_f(s):
        @pl.when(s == 0)
        def _():
            pltpu.make_async_copy(bsend.at[0:93], bsend.at[0:93], f_s).wait()

        @pl.when(s > 0)
        def _():
            pltpu.make_async_copy(fsend.at[0:7], fsend.at[0:7], f_s).wait()
            pltpu.make_async_copy(fsend.at[7, 0:15], fsend.at[7, 0:15], f_s).wait()

    lax.fori_loop(0, STEPS, step, 0)

    @pl.when(owner)
    def _():
        sent_f(1)
        ref = wts.at[pl.ds(0, 3), 0]
        pltpu.make_async_copy(ref, ref, wd_s).wait()
        for t in range(4):
            for axis in range(2):
                take(wb_s, t, axis)
            take(wc_s, t)

    for i in range(OWN):
        @pl.when(c != i)
        def _(i=i):
            a, b = to_owner(i)
            a.wait_send()
            b.wait_send()

    for j in range(NC):
        @pl.when(c != j)
        def _(j=j):
            pltpu.make_async_copy(stat, stat, st_s.at[j]).wait()

    @pl.when(owner)
    def _():
        for j in range(NC):
            xin[j] = x[0:W, j * 192:(j + 1) * 192]
        for j in range(NC):
            @pl.when(c != j)
            def _(j=j):
                pltpu.make_async_remote_copy(
                    xin.at[j], ends.at[c], o_s.at[j], o_r.at[c],
                    device_id=(l, j), device_id_type=MESH).start()

        pltpu.make_async_copy(xin.at[c], ends.at[c], o_r.at[c]).start()

    for i in range(OWN):
        pltpu.make_async_copy(ends.at[i], ends.at[i], o_r.at[i]).wait()
        out[i] = ends[i].reshape(W, 1, 192)

    @pl.when(owner)
    def _():
        for j in range(NC):
            @pl.when(c != j)
            def _(j=j):
                pltpu.make_async_copy(xin.at[0], xin.at[0], o_s.at[j]).wait()


def local(
    state, norm_gains, channel_biases, filter_in, filter_in_bias, filter_out, filter_out_bias,
    up_weight, up_bias, down_weight,
):
    up = up_weight.reshape(2, 4, 2, 48, 768)
    down = down_weight.reshape(2, 4, 2, 48, 768)
    fwd, back, t_to, t_fro = tables()
    vm = pl.BlockSpec(memory_space=pltpu.VMEM)
    hbm = pl.BlockSpec(memory_space=pltpu.HBM)
    sem = pltpu.SemaphoreType.DMA
    result = pl.pallas_call(
        kernel,
        out_shape=jax.ShapeDtypeStruct((OWN, W, 1, 192), F32),
        in_specs=[hbm] * 14,
        out_specs=vm,
        scratch_shapes=[
            pltpu.VMEM((OWN, W, 1, 192), F32),
            pltpu.VMEM((OWN, W, 192), F32),
            pltpu.VMEM((2, 192), BF),
            pltpu.VMEM((3, 192), BF),
            pltpu.VMEM((2, 2, BS, BS), F32),
            pltpu.VMEM((2, 2, BS), F32),
            pltpu.VMEM((2, 2, BS, BS), F32),
            pltpu.VMEM((2, 2, BS), F32),
            pltpu.VMEM((D,), BF),
            pltpu.VMEM((128, 3 * R), BF),
            pltpu.VMEM((R, 256), BF),
            pltpu.VMEM((192, 384), BF),
            pltpu.VMEM((192, 576), BF),
            pltpu.VMEM((8, D), F32),
            sem((12,)),
            pltpu.VMEM((NC, W, 192), F32),
            pltpu.VMEM((OWN, W, 192), F32),
            pltpu.VMEM((NC, 8, D), F32),
            pltpu.VMEM((R, D), F32),
            pltpu.VMEM((R, D), BF),
            pltpu.VMEM((NB, G, 8, 128), BF),
            pltpu.VMEM((H, 8, 128), BF),
            pltpu.VMEM((H, 8, 128), BF),
            pltpu.VMEM((NB, G, 8, 128), BF),
            pltpu.VMEM((768, 256), BF),
            pltpu.VMEM((1, 256), F32),
            pltpu.VMEM((768, 256), BF),
            pltpu.VMEM((1, 256), F32),
            pltpu.VMEM((8, D), F32),
            pltpu.VMEM((R, FF), BF),
            pltpu.VMEM((768, 128), F32),
            pltpu.VMEM((3 * R, D), BF),
            pltpu.VMEM((NC, 2, 2, 4, 2, 48, 768), BF),
            pltpu.VMEM((640, 128), F32),
            pltpu.VMEM((8, 640), F32),
            pltpu.VMEM((NC, 8, 640), F32),
            sem((OWN,)), sem((NC,)), sem((OWN,)), sem((NC,)),
            sem, sem, sem, sem, sem((NC,)), sem((OWN,)),
            sem((2,)), sem((4, OWN)), sem((4,)), sem((4, 2)), sem((4, 2)), sem((4,)), sem((4,)), sem, sem((4, 4)), sem((NC,)), sem((NC,)),
        ],
        compiler_params=pltpu.CompilerParams(
            collective_id=0, has_side_effects=True, vmem_limit_bytes=62 * 1024 * 1024),
        name="rollout",
    )(
        state.reshape(OWN, W, 1, 192), norm_gains, channel_biases, filter_in, filter_in_bias, filter_out, filter_out_bias,
        up, up_bias, down, jnp.asarray(fwd), jnp.asarray(back), jnp.asarray(t_to), jnp.asarray(t_fro),
    )
    return result.reshape(1, OWN, W, 192)


def solution(mesh):
    placed = (
        P(None, "lat", None, "ch"),
        P(None, "ch"),
        P(None, "ch"),
        P(None, "ch", None, None),
        P(None, "ch", None),
        P(None, "ch", None, None),
        P(None, "ch", None),
        P(None, "ch"),
        P("ch"),
        P("ch", None),
    )
    return jax.shard_map(
        local, mesh=mesh, in_specs=placed, out_specs=P(None, "lat", None, "ch"), check_vma=False
    )
```

```python
import itertools
import math

import jax
import jax.numpy as jnp
import numpy as np
from jax import lax
from jax.experimental import pallas as pl
from jax.experimental.pallas import tpu as pltpu
from jax.sharding import PartitionSpec as P

D = 768
FF = 3072
W = 180
R = 192
H = 96
M = 64
NB = 8
BS = 96
STEPS = 4
NL = 32
NC = 4
ND = NL * NC
OWN = 3
G = 16
SCALE = 1.0 / math.sqrt(H * W)
EPS = 1e-05
SHRINK = 0.01
HOPS = (0, 1, 2, 1)
OTHERS = sorted(
    (o for o in itertools.product(range(4), range(4), range(4), range(2)) if any(o)),
    key=lambda o: -(HOPS[o[0]] + HOPS[o[1]] + HOPS[o[2]] + 0.3 * o[3]),
)
MESH = pl.DeviceIdType.MESH
BF = jnp.bfloat16
F32 = jnp.float32


def tables():
    modes = np.arange(M)
    w = np.arange(W)
    ang = 2.0 * np.pi / W * ((w[:, None] * modes[None, :]) % W)
    c, s = np.cos(ang), np.sin(ang)
    dbl = np.where(modes == 0, 1.0, 2.0)
    fwd = np.zeros((G, 2, 4, R))
    fwd[:, 0, :, :W] = c.T.reshape(G, 4, W)
    fwd[:, 1, :, :W] = -s.T.reshape(G, 4, W)
    back = np.zeros((R, G, 2, 4))
    back[:W, :, 0, :] = (c * dbl).reshape(W, G, 4)
    back[:W, :, 1, :] = -(s * dbl).reshape(W, G, 4)
    h = np.arange(H)
    ang = 2.0 * np.pi / H * ((h[:, None] * h[None, :]) % H)
    c, s = np.cos(ang), np.sin(ang)
    to = np.block([[c, s], [-s, c]])
    fro = to.T
    fwd, back = halves(fwd.reshape(128, R)), halves(back.reshape(R, 128))
    return (
        np.concatenate([fwd[0], fwd[1], fwd[0]], axis=1),
        np.concatenate(back, axis=1),
        np.concatenate(halves(to), axis=1),
        np.concatenate([halves(fro)[0], halves(fro)[1], halves(fro)[0]], axis=1),
    )


def halves(a):
    a = np.asarray(a, np.float32)
    hi = a.astype(BF)
    return hi, (a - hi.astype(np.float32)).astype(BF)


def parts(v):
    hi = v.astype(BF)
    return hi, (v - hi.astype(F32)).astype(BF)


def norm(v, gain, shift):
    mean = jnp.sum(v, -1, keepdims=True) / D
    spread = jnp.sum(v * v, -1, keepdims=True) / D - mean * mean
    return (v - mean) * lax.rsqrt(spread + EPS) * gain + shift


def kernel(
    state_h, gains_h, biases_h, fin_h, finb_h, fout_h, foutb_h, up, upb_h, down, fwd_h, back_h, to_h, fro_h,
    out,
    lines, state, gains, biases, fin, finb, fout, foutb, upb, fwd, back, t_to, t_fro, small, h_s,
    xin, early, late, earlies, lates, smalls, x, nb, fsend, frecv, bsend, brecv, w1, b1, w2, b2, par, hid, g32, n3, wts, tall, stat, stats,
    in_s, in_r, sm_s, sm_r, f_s, f_r, b_s, b_r, o_s, o_r,
    own_r, wa_s, wa_r, wb_s, wb_r, wc_s, wc_r, wd_s, wd_r, st_s, st_r, e_s, e_r,
):
    l = lax.axis_index("lat")
    c = lax.axis_index("ch")
    me = l * NC + c
    row = l * OWN + c
    blk = lax.rem(l, 2)
    owner = c < OWN

    k = lax.rem(l, 2)
    cy = lax.rem(l // 2, 4)
    cz = l // 8
    xs = [lax.rem(c + i, 4) for i in range(4)]
    groups = [[lax.rem(cz + i, 4) * 4 + lax.rem(cy + j, 4) for j in range(4)] for i in range(4)]
    cores = (k, 1 - k)

    fetches = [
        pltpu.make_async_copy(src, dst, h_s.at[i])
        for i, (src, dst) in enumerate((
            (to_h, t_to), (fro_h, t_fro), (fin_h, fin), (fout_h, fout), (finb_h, finb), (foutb_h, foutb),
            (gains_h, gains), (biases_h, biases), (upb_h, upb), (fwd_h, fwd), (back_h, back), (state_h, lines)))
    ]
    for fetch in fetches:
        fetch.start()

    barrier = pltpu.get_barrier_semaphore()
    for dx, dy, dz, dk in OTHERS:
        pl.semaphore_signal(
            barrier, inc=1, device_id=(groups[dz][dy] * 2 + cores[dk], xs[dx]), device_id_type=MESH)

    def to_owner(i):
        return (
            pltpu.make_async_remote_copy(
                state.at[i], xin.at[c], in_s.at[i], in_r.at[c],
                device_id=(l, i), device_id_type=MESH),
            pltpu.make_async_remote_copy(
                small, smalls.at[c], sm_s.at[i], sm_r.at[c],
                device_id=(l, i), device_id_type=MESH),
        )

    py, pz = lax.rem(cy, 2), lax.rem(cz, 2)
    mine = 2 * pz + py
    at_y, at_z, at_d = 2 * pz + 1 - py, 2 * (1 - pz) + py, 2 * (1 - pz) + 1 - py
    shards = (up, down)

    def foreign(j):
        return lax.rem(c + 1 + j, NC)

    three = wts.at[0, 0, 0, pl.ds(0, 3), 0]

    def take(sems, *at):
        pltpu.make_async_copy(three, three, sems.at[at] if at else sems).wait()

    def pass_on(t, piece, axis, s_sem, r_sem):
        for j in range(3):
            for half, sign in ((0, 1), (1, 3)):
                ref = wts.at[foreign(j), t // 2, k, piece, t % 2, :, pl.ds(half * 384, 384)]
                to = groups[(0, sign)[axis]][(sign, 0)[axis]] * 2 + k
                pltpu.make_async_remote_copy(
                    ref, ref, s_sem, r_sem, device_id=(to, c), device_id_type=MESH).start()

    def share(t, piece, stage):
        for j in range(3):
            ref = wts.at[foreign(j), t // 2, k, piece, t % 2]
            pltpu.make_async_remote_copy(
                ref, ref, wd_s, wd_r.at[t, stage], device_id=(groups[0][0] * 2 + 1 - k, c),
                device_id_type=MESH).start()

    @pl.when(owner)
    def _():
        for m in range(2):
            pltpu.make_async_copy(shards[m], wts.at[c, m], own_r.at[m]).start()

    def weights_0(t):
        for i in range(OWN):
            @pl.when(c != i)
            def _(i=i):
                pltpu.make_async_remote_copy(
                    shards[t // 2].at[k, mine, t % 2], wts.at[c, t // 2, k, mine, t % 2],
                    wa_s.at[t, i], wa_r.at[t], device_id=(l, i), device_id_type=MESH).start()

    def sent_weights(t):
        for i in range(OWN):
            @pl.when(c != i)
            def _(i=i):
                ref = shards[t // 2].at[k, mine, t % 2]
                pltpu.make_async_copy(ref, ref, wa_s.at[t, i]).wait()

    def weights_1(t):
        take(wa_r, t)
        for axis in range(2):
            pass_on(t, mine, axis, wb_s.at[t, axis], wb_r.at[t, axis])
        share(t, mine, 0)

    def weights_2(t):
        u = t % 2
        take(wb_r, t, 1 - u)
        pass_on(t, (at_z, at_y)[u], u, wc_s.at[t], wc_r.at[t])
        share(t, (at_z, at_y)[u], 2)
        take(wb_r, t, u)
        share(t, (at_y, at_z)[u], 1)

    def weights_3(t):
        take(wc_r, t)
        share(t, at_d, 3)

    def weights_4(m):
        pltpu.make_async_copy(wts.at[c, m], wts.at[c, m], own_r.at[m]).wait()
        for t in (2 * m, 2 * m + 1):
            for stage in range(4):
                take(wd_r, t, stage)

    fsend[...] = jnp.zeros_like(fsend)
    n3[...] = jnp.zeros_like(n3)
    tall[...] = jnp.zeros_like(tall)
    small[...] = jnp.zeros_like(small)
    for fetch in fetches:
        fetch.wait()
    state[...] = lines[...].reshape(OWN, W, 192)
    small[0:2, 0:192] = gains[...].astype(F32)
    small[2:5, 0:192] = biases[...].astype(F32)
    small[5:6, :] = upb[...].astype(F32).reshape(1, D)
    for w_ref, b_ref, src, bsrc in ((w1, b1, fin, finb), (w2, b2, fout, foutb)):
        w_ref[...] = jnp.zeros_like(w_ref)
        b_ref[...] = jnp.zeros_like(b_ref)
        for at, re, im in zip((0, 256), parts(src[0, blk]), parts(src[1, blk])):
            w_ref[at:at + BS, 0:BS] = re
            w_ref[at:at + BS, 128:128 + BS] = im
            w_ref[at + 128:at + 128 + BS, 0:BS] = -im
            w_ref[at + 128:at + 128 + BS, 128:128 + BS] = re
        w_ref[512:768, :] = w_ref[0:256, :]
        b_ref[:, 0:BS] = bsrc[0, pl.ds(blk, 1), :]
        b_ref[:, 128:128 + BS] = bsrc[1, pl.ds(blk, 1), :]


    lane = lax.broadcasted_iota(jnp.int32, (W, 128), 1)
    for r in range(OWN):
        v = state[r]
        total = jnp.sum(v, -1, keepdims=True)
        squares = jnp.sum(v * v, -1, keepdims=True)
        tall[r * R:r * R + W, :] = jnp.where(lane == 0, total, jnp.where(lane == 1, squares, 0.0))
    stat[...] = tall[...].T[0:8, :]

    pl.semaphore_wait(barrier, ND - 1)
    for j in range(NC):
        @pl.when(c != j)
        def _(j=j):
            pltpu.make_async_remote_copy(
                stat, stats.at[c], st_s.at[j], st_r.at[c], device_id=(l, j), device_id_type=MESH).start()

        @pl.when(c == j)
        def _(j=j):
            pltpu.make_async_copy(stat, stats.at[j], st_r.at[j]).start()

    weights_0(0)
    for j in range(NC):
        pltpu.make_async_copy(stats.at[j], stats.at[j], st_r.at[j]).wait()
    weights_0(1)
    total = (stats[0] + stats[1]) + (stats[2] + stats[3])
    mean = total[0:1] / D
    spread = lax.rsqrt(total[1:2] / D - mean * mean + EPS)
    line = lax.broadcasted_iota(jnp.int32, (128, 640), 0)
    tall[...] = jnp.where(line == 0, mean, jnp.where(line == 1, spread, 0.0)).T
    for r in range(OWN):
        at = slice(r * R, r * R + W)
        n = (state[r] - tall[at, 0:1]) * tall[at, 1:2] * small[0:1, 0:192] + small[2:3, 0:192]
        hi, lo = parts(n)
        n3[0:W, 0:192] = hi
        n3[R:R + W, 0:192] = hi
        n3[2 * R:2 * R + W, 0:192] = lo
        lon = jnp.dot(fwd[...], n3[:, 0:192], preferred_element_type=F32)
        for j in range(2):
            fsend[2 * r + j, :, :, 0:BS] = lon[:, j * BS:(j + 1) * BS].reshape(G, 8, BS).astype(BF)

    for dx, dy, dz, dk in OTHERS:
        if dx:
            continue
        for r in range(OWN):
            pltpu.make_async_remote_copy(
                fsend.at[2 * r + cores[dk], groups[dz][dy]], frecv.at[l * OWN + r], f_s, f_r,
                device_id=(groups[dz][dy] * 2 + cores[dk], c), device_id_type=MESH).start()
    for r in range(OWN):
        pltpu.make_async_copy(fsend.at[2 * r + blk, l // 2], frecv.at[l * OWN + r], f_r).start()
    sent_weights(0)
    pl.when(owner)(lambda: weights_1(0))
    sent_weights(1)
    weights_0(2)
    pl.when(owner)(lambda: weights_1(1))

    def hand_out(src, dst, s_sems, r_sems):
        for j in range(NC):
            src[j] = (x[0:W, j * 192:(j + 1) * 192] - xin[j]).astype(BF)
        for j in range(NC):
            @pl.when(c != j)
            def _(j=j):
                pltpu.make_async_remote_copy(
                    src.at[j], dst.at[c], s_sems.at[j], r_sems.at[c],
                    device_id=(l, j), device_id_type=MESH).start()

        pltpu.make_async_copy(src.at[c], dst.at[c], r_sems.at[c]).start()

    def send_state():
        for i in range(OWN):
            @pl.when(c != i)
            def _(i=i):
                a, b = to_owner(i)
                a.start()
                b.start()

            @pl.when(c == i)
            def _(i=i):
                pltpu.make_async_copy(state.at[i], xin.at[i], in_r.at[i]).start()
                pltpu.make_async_copy(small, smalls.at[i], sm_r.at[i]).start()

    def own_row():
        for j in range(NC):
            pltpu.make_async_copy(xin.at[j], xin.at[j], in_r.at[j]).wait()
            pltpu.make_async_copy(smalls.at[j], smalls.at[j], sm_r.at[j]).wait()
        par[0:5, :] = jnp.concatenate([smalls[j, 0:5, 0:192] for j in range(NC)], axis=1)
        v = jnp.concatenate([xin[j] for j in range(NC)], axis=1)
        x[0:W, :] = v + norm(v, par[0:1, :], par[2:3, :])
        x[W:R, :] = jnp.zeros((R - W, D), F32)

    def send_row():
        v = x[...]
        n = norm(v, par[0:1, :], par[2:3, :])
        x[...] = v + n
        hi, lo = parts(n)
        n3[0:R, :] = hi
        n3[R:2 * R, :] = hi
        n3[2 * R:3 * R, :] = lo
        lon = jnp.dot(fwd[...], n3[...], preferred_element_type=F32)
        for b in range(NB):
            fsend[b, :, :, 0:BS] = lon[:, b * BS:(b + 1) * BS].reshape(G, 8, BS).astype(BF)

        for dx, dy, dz, dk in OTHERS:
            pltpu.make_async_remote_copy(
                fsend.at[2 * xs[dx] + cores[dk], groups[dz][dy]], frecv.at[row], f_s, f_r,
                device_id=(groups[dz][dy] * 2 + cores[dk], xs[dx]), device_id_type=MESH).start()
        pltpu.make_async_copy(
            fsend.at[2 * c + blk, l // 2], frecv.at[row], f_r).start()

    def step(s, carry):
        pltpu.make_async_copy(frecv, frecv, f_r).wait()

        @pl.when(s == 0)
        def _():
            sent_weights(2)
            weights_0(3)

            @pl.when(owner)
            def _():
                weights_2(0)
                weights_1(2)


        g32[...] = frecv[...].reshape(H * 8, 128).astype(F32)
        got = jnp.concatenate(
            [jnp.concatenate([g32[pl.ds(4 * i + m, H, stride=8), :] for m in range(4)], axis=1) for i in range(2)],
            axis=0).astype(BF)
        got = jnp.concatenate([got, got], axis=0)
        spec = jnp.dot(t_to[...], got, preferred_element_type=F32) * SCALE
        spec = jnp.concatenate(
            [jnp.concatenate([spec[i * H:(i + 1) * H, m * 128:(m + 1) * 128] for i in range(2)], axis=1)
             for m in range(4)], axis=0)
        hi, lo = parts(spec)
        first = jnp.dot(jnp.concatenate([hi, hi, lo], axis=1), w1[...], preferred_element_type=F32) + b1[...]
        hi, lo = parts(jnp.maximum(first, 0.0))
        second = jnp.dot(jnp.concatenate([hi, hi, lo], axis=1), w2[...], preferred_element_type=F32) + b2[...]
        second = jnp.where(second > SHRINK, second - SHRINK,
                           jnp.where(second < -SHRINK, second + SHRINK, 0.0))
        second = jnp.concatenate(
            [jnp.concatenate([second[m * H:(m + 1) * H, i * 128:(i + 1) * 128] for m in range(4)], axis=1)
             for i in range(2)], axis=0)
        hi, lo = parts(second)
        rows = jnp.dot(t_fro[...], jnp.concatenate([hi, hi, lo], axis=0), preferred_element_type=F32)
        for i in range(2):
            for m in range(4):
                g32[pl.ds(4 * i + m, H, stride=8), :] = rows[i * H:(i + 1) * H, m * 128:(m + 1) * 128]
        bsend[...] = g32[...].reshape(H, 8, 128).astype(BF)

        for dx, dy, dz, dk in OTHERS:
            dl, dc = groups[dz][dy] * 2 + cores[dk], xs[dx]

            @pl.when(dc < OWN)
            def _(dl=dl, dc=dc):
                pltpu.make_async_remote_copy(
                    bsend.at[dl * OWN + dc], brecv.at[2 * c + blk, l // 2], b_s, b_r,
                    device_id=(dl, dc), device_id_type=MESH).start()

        @pl.when(owner)
        def _():
            pltpu.make_async_copy(bsend.at[row], brecv.at[2 * c + blk, l // 2], b_r).start()

            @pl.when(s == 0)
            def _():
                weights_2(1)
                weights_1(3)
                sent_weights(3)
                send_state()
                weights_2(2)
                weights_3(0)
                weights_3(1)
                weights_2(3)
                own_row()
                weights_3(2)

            pltpu.make_async_copy(brecv, brecv, b_r).wait()

            packed = jnp.concatenate(
                [brecv[b].reshape(128, 128)[:, 0:BS].astype(F32) for b in range(NB)], axis=1).astype(BF)
            packed = jnp.concatenate([packed, packed], axis=0)
            v = x[...] + jnp.dot(back[...], packed, preferred_element_type=F32) * SCALE
            x[...] = v
            @pl.when(s == STEPS - 2)
            def _():
                hand_out(early, earlies, e_s, e_r)
                for j in range(NC):
                    xin[j] = xin[j] + early[j].astype(F32)

            nb[...] = norm(v, par[1:2, :], par[3:4, :]).astype(BF)

            @pl.when(s == 0)
            def _():
                weights_3(3)
                weights_4(0)
                weights_4(1)

            def up_part(q):
                for j in range(3):
                    cols = slice(j * 256, (j + 1) * 256)
                    weight = wts[q, 0, :, :, :, :, cols].reshape(D, 256)
                    pre = jnp.dot(nb[...], weight, preferred_element_type=F32) + smalls[q, 5:6, cols]
                    act = 0.5 * pre * (1.0 + lax.erf(pre * math.sqrt(0.5)))
                    hid[:, q * 768 + j * 256:q * 768 + (j + 1) * 256] = act.astype(BF)

            def down_part(q):
                for j in range(3):
                    cols = slice(j * 256, (j + 1) * 256)
                    weight = wts[q, 1, :, :, :, :, cols].reshape(D, 256)
                    mixed = jnp.dot(hid[:, q * 768:(q + 1) * 768], weight, preferred_element_type=F32)
                    if q == 0:
                        mixed = mixed + par[4:5, cols]
                    x[:, cols] = x[:, cols] + mixed

            up_part(0)
            for q in range(1, NC):
                up_part(q)
                down_part(q - 1)
            down_part(NC - 1)

            @pl.when(s < STEPS - 1)
            def _():
                sent_f(s)
                send_row()

            pltpu.make_async_copy(bsend.at[0:95], bsend.at[0:95], b_s).wait()

        @pl.when(jnp.logical_not(owner))
        def _():
            @pl.when(s == 0)
            def _():
                sent_weights(3)
                send_state()
                sent_f(s)

            pltpu.make_async_copy(bsend, bsend, b_s).wait()

        return carry

    def sent_f(s):
        @pl.when(s == 0)
        def _():
            pltpu.make_async_copy(bsend.at[0:93], bsend.at[0:93], f_s).wait()

        @pl.when(s > 0)
        def _():
            pltpu.make_async_copy(fsend.at[0:7], fsend.at[0:7], f_s).wait()
            pltpu.make_async_copy(fsend.at[7, 0:15], fsend.at[7, 0:15], f_s).wait()

    lax.fori_loop(0, STEPS, step, 0)

    @pl.when(owner)
    def _():
        sent_f(1)
        ref = wts.at[pl.ds(0, 3), 0]
        pltpu.make_async_copy(ref, ref, wd_s).wait()
        for t in range(4):
            for axis in range(2):
                take(wb_s, t, axis)
            take(wc_s, t)

    for i in range(OWN):
        @pl.when(c != i)
        def _(i=i):
            a, b = to_owner(i)
            a.wait_send()
            b.wait_send()

    for j in range(NC):
        @pl.when(c != j)
        def _(j=j):
            pltpu.make_async_copy(stat, stat, st_s.at[j]).wait()

    @pl.when(owner)
    def _():
        hand_out(late, lates, o_s, o_r)

    for i in range(OWN):
        pltpu.make_async_copy(earlies.at[i], earlies.at[i], e_r.at[i]).wait()
        state[i] = state[i] + earlies[i].astype(F32)
    for i in range(OWN):
        pltpu.make_async_copy(lates.at[i], lates.at[i], o_r.at[i]).wait()
        out[i] = (state[i] + lates[i].astype(F32)).reshape(W, 1, 192)

    @pl.when(owner)
    def _():
        for j in range(NC):
            @pl.when(c != j)
            def _(j=j):
                pltpu.make_async_copy(early.at[0], early.at[0], e_s.at[j]).wait()
                pltpu.make_async_copy(late.at[0], late.at[0], o_s.at[j]).wait()


def local(
    state, norm_gains, channel_biases, filter_in, filter_in_bias, filter_out, filter_out_bias,
    up_weight, up_bias, down_weight,
):
    up = up_weight.reshape(2, 4, 2, 48, 768)
    down = down_weight.reshape(2, 4, 2, 48, 768)
    fwd, back, t_to, t_fro = tables()
    vm = pl.BlockSpec(memory_space=pltpu.VMEM)
    hbm = pl.BlockSpec(memory_space=pltpu.HBM)
    sem = pltpu.SemaphoreType.DMA
    result = pl.pallas_call(
        kernel,
        out_shape=jax.ShapeDtypeStruct((OWN, W, 1, 192), F32),
        in_specs=[hbm] * 14,
        out_specs=vm,
        scratch_shapes=[
            pltpu.VMEM((OWN, W, 1, 192), F32),
            pltpu.VMEM((OWN, W, 192), F32),
            pltpu.VMEM((2, 192), BF),
            pltpu.VMEM((3, 192), BF),
            pltpu.VMEM((2, 2, BS, BS), F32),
            pltpu.VMEM((2, 2, BS), F32),
            pltpu.VMEM((2, 2, BS, BS), F32),
            pltpu.VMEM((2, 2, BS), F32),
            pltpu.VMEM((D,), BF),
            pltpu.VMEM((128, 3 * R), BF),
            pltpu.VMEM((R, 256), BF),
            pltpu.VMEM((192, 384), BF),
            pltpu.VMEM((192, 576), BF),
            pltpu.VMEM((8, D), F32),
            sem((12,)),
            pltpu.VMEM((NC, W, 192), F32),
            pltpu.VMEM((NC, W, 192), BF),
            pltpu.VMEM((NC, W, 192), BF),
            pltpu.VMEM((OWN, W, 192), BF),
            pltpu.VMEM((OWN, W, 192), BF),
            pltpu.VMEM((NC, 8, D), F32),
            pltpu.VMEM((R, D), F32),
            pltpu.VMEM((R, D), BF),
            pltpu.VMEM((NB, G, 8, 128), BF),
            pltpu.VMEM((H, 8, 128), BF),
            pltpu.VMEM((H, 8, 128), BF),
            pltpu.VMEM((NB, G, 8, 128), BF),
            pltpu.VMEM((768, 256), BF),
            pltpu.VMEM((1, 256), F32),
            pltpu.VMEM((768, 256), BF),
            pltpu.VMEM((1, 256), F32),
            pltpu.VMEM((8, D), F32),
            pltpu.VMEM((R, FF), BF),
            pltpu.VMEM((768, 128), F32),
            pltpu.VMEM((3 * R, D), BF),
            pltpu.VMEM((NC, 2, 2, 4, 2, 48, 768), BF),
            pltpu.VMEM((640, 128), F32),
            pltpu.VMEM((8, 640), F32),
            pltpu.VMEM((NC, 8, 640), F32),
            sem((OWN,)), sem((NC,)), sem((OWN,)), sem((NC,)),
            sem, sem, sem, sem, sem((NC,)), sem((OWN,)),
            sem((2,)), sem((4, OWN)), sem((4,)), sem((4, 2)), sem((4, 2)), sem((4,)), sem((4,)), sem, sem((4, 4)), sem((NC,)), sem((NC,)), sem((NC,)), sem((OWN,)),
        ],
        compiler_params=pltpu.CompilerParams(
            collective_id=0, has_side_effects=True, vmem_limit_bytes=62 * 1024 * 1024),
        name="rollout",
    )(
        state.reshape(OWN, W, 1, 192), norm_gains, channel_biases, filter_in, filter_in_bias, filter_out, filter_out_bias,
        up, up_bias, down, jnp.asarray(fwd), jnp.asarray(back), jnp.asarray(t_to), jnp.asarray(t_fro),
    )
    return result.reshape(1, OWN, W, 192)


def solution(mesh):
    placed = (
        P(None, "lat", None, "ch"),
        P(None, "ch"),
        P(None, "ch"),
        P(None, "ch", None, None),
        P(None, "ch", None),
        P(None, "ch", None, None),
        P(None, "ch", None),
        P(None, "ch"),
        P("ch"),
        P("ch", None),
    )
    return jax.shard_map(
        local, mesh=mesh, in_specs=placed, out_specs=P(None, "lat", None, "ch"), check_vma=False
    )
```

```python
import itertools
import math

import jax
import jax.numpy as jnp
import numpy as np
from jax import lax
from jax.experimental import pallas as pl
from jax.experimental.pallas import tpu as pltpu
from jax.sharding import PartitionSpec as P

D = 768
FF = 3072
W = 180
R = 192
H = 96
M = 64
NB = 8
BS = 96
STEPS = 4
NL = 32
NC = 4
ND = NL * NC
OWN = 3
G = 16
SCALE = 1.0 / math.sqrt(H * W)
EPS = 1e-05
SHRINK = 0.01
HOPS = (0, 1, 2, 1)
OTHERS = sorted(
    (o for o in itertools.product(range(4), range(4), range(4), range(2)) if any(o)),
    key=lambda o: -(HOPS[o[0]] + HOPS[o[1]] + HOPS[o[2]] + 0.3 * o[3]),
)
MESH = pl.DeviceIdType.MESH
BF = jnp.bfloat16
F32 = jnp.float32


def tables():
    modes = np.arange(M)
    w = np.arange(W)
    ang = 2.0 * np.pi / W * ((w[:, None] * modes[None, :]) % W)
    c, s = np.cos(ang), np.sin(ang)
    dbl = np.where(modes == 0, 1.0, 2.0)
    fwd = np.zeros((G, 2, 4, R))
    fwd[:, 0, :, :W] = c.T.reshape(G, 4, W)
    fwd[:, 1, :, :W] = -s.T.reshape(G, 4, W)
    back = np.zeros((R, G, 2, 4))
    back[:W, :, 0, :] = (c * dbl).reshape(W, G, 4)
    back[:W, :, 1, :] = -(s * dbl).reshape(W, G, 4)
    h = np.arange(H)
    ang = 2.0 * np.pi / H * ((h[:, None] * h[None, :]) % H)
    c, s = np.cos(ang), np.sin(ang)
    to = np.block([[c, s], [-s, c]])
    fro = to.T
    fwd, back = halves(fwd.reshape(128, R)), halves(back.reshape(R, 128))
    return (
        np.concatenate([fwd[0], fwd[1], fwd[0]], axis=1),
        np.concatenate(back, axis=1),
        np.concatenate(halves(to), axis=1),
        np.concatenate([halves(fro)[0], halves(fro)[1], halves(fro)[0]], axis=1),
    )


def halves(a):
    a = np.asarray(a, np.float32)
    hi = a.astype(BF)
    return hi, (a - hi.astype(np.float32)).astype(BF)


def parts(v):
    hi = v.astype(BF)
    return hi, (v - hi.astype(F32)).astype(BF)


def norm(v, gain, shift):
    mean = jnp.sum(v, -1, keepdims=True) / D
    spread = jnp.sum(v * v, -1, keepdims=True) / D - mean * mean
    return (v - mean) * lax.rsqrt(spread + EPS) * gain + shift


def kernel(
    state_h, gains_h, biases_h, fin_h, finb_h, fout_h, foutb_h, up, upb_h, down, fwd_h, back_h, to_h, fro_h,
    out,
    lines, state, gains, biases, fin, finb, fout, foutb, upb, fwd, back, t_to, t_fro, small, h_s,
    xin, early, late, earlies, lates, smalls, x, nb, fsend, frecv, bsend, brecv, w1, b1, w2, b2, par, hid, g32, n3, wts, tall, stat, stats,
    in_s, in_r, sm_s, sm_r, f_s, f_r, b_s, b_r, o_s, o_r,
    own_r, wa_s, wa_r, wb_s, wb_r, wc_s, wc_r, wd_s, wd_r, st_s, st_r, e_s, e_r,
):
    l = lax.axis_index("lat")
    c = lax.axis_index("ch")
    me = l * NC + c
    row = l * OWN + c
    blk = lax.rem(l, 2)
    owner = c < OWN

    k = lax.rem(l, 2)
    cy = lax.rem(l // 2, 4)
    cz = l // 8
    xs = [lax.rem(c + i, 4) for i in range(4)]
    groups = [[lax.rem(cz + i, 4) * 4 + lax.rem(cy + j, 4) for j in range(4)] for i in range(4)]
    cores = (k, 1 - k)

    fetches = [
        pltpu.make_async_copy(src, dst, h_s.at[i])
        for i, (src, dst) in enumerate((
            (to_h, t_to), (fro_h, t_fro), (fin_h, fin), (fout_h, fout), (finb_h, finb), (foutb_h, foutb),
            (gains_h, gains), (biases_h, biases), (upb_h, upb), (fwd_h, fwd), (back_h, back), (state_h, lines)))
    ]
    for fetch in fetches:
        fetch.start()

    barrier = pltpu.get_barrier_semaphore()
    for dx, dy, dz, dk in OTHERS:
        pl.semaphore_signal(
            barrier, inc=1, device_id=(groups[dz][dy] * 2 + cores[dk], xs[dx]), device_id_type=MESH)

    def to_owner(i):
        return (
            pltpu.make_async_remote_copy(
                state.at[i], xin.at[c], in_s.at[i], in_r.at[c],
                device_id=(l, i), device_id_type=MESH),
            pltpu.make_async_remote_copy(
                small, smalls.at[c], sm_s.at[i], sm_r.at[c],
                device_id=(l, i), device_id_type=MESH),
        )

    py, pz = lax.rem(cy, 2), lax.rem(cz, 2)
    mine = 2 * pz + py
    at_y, at_z, at_d = 2 * pz + 1 - py, 2 * (1 - pz) + py, 2 * (1 - pz) + 1 - py
    shards = (up, down)

    def foreign(j):
        return lax.rem(c + 1 + j, NC)

    three = wts.at[0, 0, 0, pl.ds(0, 3), 0]

    def take(sems, *at):
        pltpu.make_async_copy(three, three, sems.at[at] if at else sems).wait()

    def pass_on(t, piece, axis, s_sem, r_sem):
        for j in range(3):
            for half, sign in ((0, 1), (1, 3)):
                ref = wts.at[foreign(j), t // 2, k, piece, t % 2, :, pl.ds(half * 384, 384)]
                to = groups[(0, sign)[axis]][(sign, 0)[axis]] * 2 + k
                pltpu.make_async_remote_copy(
                    ref, ref, s_sem, r_sem, device_id=(to, c), device_id_type=MESH).start()

    def share(t, piece, stage):
        for j in range(3):
            ref = wts.at[foreign(j), t // 2, k, piece, t % 2]
            pltpu.make_async_remote_copy(
                ref, ref, wd_s, wd_r.at[t, stage], device_id=(groups[0][0] * 2 + 1 - k, c),
                device_id_type=MESH).start()

    @pl.when(owner)
    def _():
        for m in range(2):
            pltpu.make_async_copy(shards[m], wts.at[c, m], own_r.at[m]).start()

    def weights_0(t):
        for i in range(OWN):
            @pl.when(c != i)
            def _(i=i):
                pltpu.make_async_remote_copy(
                    shards[t // 2].at[k, mine, t % 2], wts.at[c, t // 2, k, mine, t % 2],
                    wa_s.at[t, i], wa_r.at[t], device_id=(l, i), device_id_type=MESH).start()

    def sent_weights(t):
        for i in range(OWN):
            @pl.when(c != i)
            def _(i=i):
                ref = shards[t // 2].at[k, mine, t % 2]
                pltpu.make_async_copy(ref, ref, wa_s.at[t, i]).wait()

    def weights_1(t):
        take(wa_r, t)
        for axis in range(2):
            pass_on(t, mine, axis, wb_s.at[t, axis], wb_r.at[t, axis])
        share(t, mine, 0)

    def weights_2(t):
        u = t % 2
        take(wb_r, t, 1 - u)
        pass_on(t, (at_z, at_y)[u], u, wc_s.at[t], wc_r.at[t])
        share(t, (at_z, at_y)[u], 2)
        take(wb_r, t, u)
        share(t, (at_y, at_z)[u], 1)

    def weights_3(t):
        take(wc_r, t)
        share(t, at_d, 3)

    def weights_4(m):
        pltpu.make_async_copy(wts.at[c, m], wts.at[c, m], own_r.at[m]).wait()
        for t in (2 * m, 2 * m + 1):
            for stage in range(4):
                take(wd_r, t, stage)

    fsend[...] = jnp.zeros_like(fsend)
    n3[...] = jnp.zeros_like(n3)
    tall[...] = jnp.zeros_like(tall)
    small[...] = jnp.zeros_like(small)
    for fetch in fetches:
        fetch.wait()
    state[...] = lines[...].reshape(OWN, W, 192)
    small[0:2, 0:192] = gains[...].astype(F32)
    small[2:5, 0:192] = biases[...].astype(F32)
    small[5:6, :] = upb[...].astype(F32).reshape(1, D)
    for w_ref, b_ref, src, bsrc in ((w1, b1, fin, finb), (w2, b2, fout, foutb)):
        w_ref[...] = jnp.zeros_like(w_ref)
        b_ref[...] = jnp.zeros_like(b_ref)
        for at, re, im in zip((0, 256), parts(src[0, blk]), parts(src[1, blk])):
            w_ref[at:at + BS, 0:BS] = re
            w_ref[at:at + BS, 128:128 + BS] = im
            w_ref[at + 128:at + 128 + BS, 0:BS] = -im
            w_ref[at + 128:at + 128 + BS, 128:128 + BS] = re
        w_ref[512:768, :] = w_ref[0:256, :]
        b_ref[:, 0:BS] = bsrc[0, pl.ds(blk, 1), :]
        b_ref[:, 128:128 + BS] = bsrc[1, pl.ds(blk, 1), :]


    lane = lax.broadcasted_iota(jnp.int32, (W, 128), 1)
    for r in range(OWN):
        v = state[r]
        total = jnp.sum(v, -1, keepdims=True)
        squares = jnp.sum(v * v, -1, keepdims=True)
        tall[r * R:r * R + W, :] = jnp.where(lane == 0, total, jnp.where(lane == 1, squares, 0.0))
    stat[...] = tall[...].T[0:8, :]

    pl.semaphore_wait(barrier, ND - 1)
    for j in range(NC):
        @pl.when(c != j)
        def _(j=j):
            pltpu.make_async_remote_copy(
                stat, stats.at[c], st_s.at[j], st_r.at[c], device_id=(l, j), device_id_type=MESH).start()

        @pl.when(c == j)
        def _(j=j):
            pltpu.make_async_copy(stat, stats.at[j], st_r.at[j]).start()

    weights_0(0)
    for j in range(NC):
        pltpu.make_async_copy(stats.at[j], stats.at[j], st_r.at[j]).wait()
    weights_0(1)
    total = (stats[0] + stats[1]) + (stats[2] + stats[3])
    mean = total[0:1] / D
    spread = lax.rsqrt(total[1:2] / D - mean * mean + EPS)
    line = lax.broadcasted_iota(jnp.int32, (128, 640), 0)
    tall[...] = jnp.where(line == 0, mean, jnp.where(line == 1, spread, 0.0)).T
    for r in range(OWN):
        at = slice(r * R, r * R + W)
        n = (state[r] - tall[at, 0:1]) * tall[at, 1:2] * small[0:1, 0:192] + small[2:3, 0:192]
        hi, lo = parts(n)
        n3[0:W, 0:192] = hi
        n3[R:R + W, 0:192] = hi
        n3[2 * R:2 * R + W, 0:192] = lo
        lon = jnp.dot(fwd[...], n3[:, 0:192], preferred_element_type=F32)
        for j in range(2):
            fsend[2 * r + j, :, :, 0:BS] = lon[:, j * BS:(j + 1) * BS].reshape(G, 8, BS).astype(BF)

    for dx, dy, dz, dk in OTHERS:
        if dx:
            continue
        for r in range(OWN):
            pltpu.make_async_remote_copy(
                fsend.at[2 * r + cores[dk], groups[dz][dy]], frecv.at[l * OWN + r], f_s, f_r,
                device_id=(groups[dz][dy] * 2 + cores[dk], c), device_id_type=MESH).start()
    for r in range(OWN):
        pltpu.make_async_copy(fsend.at[2 * r + blk, l // 2], frecv.at[l * OWN + r], f_r).start()
    sent_weights(0)
    pl.when(owner)(lambda: weights_1(0))
    sent_weights(1)
    weights_0(2)
    pl.when(owner)(lambda: weights_1(1))

    def hand_out(src, dst, s_sems, r_sems):
        for j in range(NC):
            src[j] = (x[0:W, j * 192:(j + 1) * 192] - xin[j]).astype(BF)
        for j in range(NC):
            @pl.when(c != j)
            def _(j=j):
                pltpu.make_async_remote_copy(
                    src.at[j], dst.at[c], s_sems.at[j], r_sems.at[c],
                    device_id=(l, j), device_id_type=MESH).start()

        pltpu.make_async_copy(src.at[c], dst.at[c], r_sems.at[c]).start()

    def send_state():
        for i in range(OWN):
            @pl.when(c != i)
            def _(i=i):
                a, b = to_owner(i)
                a.start()
                b.start()

            @pl.when(c == i)
            def _(i=i):
                pltpu.make_async_copy(state.at[i], xin.at[i], in_r.at[i]).start()
                pltpu.make_async_copy(small, smalls.at[i], sm_r.at[i]).start()

    def own_row():
        for j in range(NC):
            pltpu.make_async_copy(xin.at[j], xin.at[j], in_r.at[j]).wait()
            pltpu.make_async_copy(smalls.at[j], smalls.at[j], sm_r.at[j]).wait()
        par[0:5, :] = jnp.concatenate([smalls[j, 0:5, 0:192] for j in range(NC)], axis=1)
        v = jnp.concatenate([xin[j] for j in range(NC)], axis=1)
        x[0:W, :] = v + norm(v, par[0:1, :], par[2:3, :])
        x[W:R, :] = jnp.zeros((R - W, D), F32)

    def send_row():
        v = x[...]
        n = norm(v, par[0:1, :], par[2:3, :])
        x[...] = v + n
        hi, lo = parts(n)
        n3[0:R, :] = hi
        n3[R:2 * R, :] = hi
        n3[2 * R:3 * R, :] = lo
        lon = jnp.dot(fwd[...], n3[...], preferred_element_type=F32)
        for b in range(NB):
            fsend[b, :, :, 0:BS] = lon[:, b * BS:(b + 1) * BS].reshape(G, 8, BS).astype(BF)

        for dx, dy, dz, dk in OTHERS:
            pltpu.make_async_remote_copy(
                fsend.at[2 * xs[dx] + cores[dk], groups[dz][dy]], frecv.at[row], f_s, f_r,
                device_id=(groups[dz][dy] * 2 + cores[dk], xs[dx]), device_id_type=MESH).start()
        pltpu.make_async_copy(
            fsend.at[2 * c + blk, l // 2], frecv.at[row], f_r).start()

    def step(s, carry):
        pltpu.make_async_copy(frecv, frecv, f_r).wait()

        @pl.when(s == 0)
        def _():
            sent_weights(2)
            weights_0(3)

            @pl.when(owner)
            def _():
                weights_2(0)
                weights_1(2)


        g32[...] = frecv[...].reshape(H * 8, 128).astype(F32)
        got = jnp.concatenate(
            [jnp.concatenate([g32[pl.ds(4 * i + m, H, stride=8), :] for m in range(4)], axis=1) for i in range(2)],
            axis=0).astype(BF)
        got = jnp.concatenate([got, got], axis=0)
        spec = jnp.dot(t_to[...], got, preferred_element_type=F32) * SCALE
        spec = jnp.concatenate(
            [jnp.concatenate([spec[i * H:(i + 1) * H, m * 128:(m + 1) * 128] for i in range(2)], axis=1)
             for m in range(4)], axis=0)
        hi, lo = parts(spec)
        first = jnp.dot(jnp.concatenate([hi, hi, lo], axis=1), w1[...], preferred_element_type=F32) + b1[...]
        hi, lo = parts(jnp.maximum(first, 0.0))
        second = jnp.dot(jnp.concatenate([hi, hi, lo], axis=1), w2[...], preferred_element_type=F32) + b2[...]
        second = jnp.where(second > SHRINK, second - SHRINK,
                           jnp.where(second < -SHRINK, second + SHRINK, 0.0))
        second = jnp.concatenate(
            [jnp.concatenate([second[m * H:(m + 1) * H, i * 128:(i + 1) * 128] for m in range(4)], axis=1)
             for i in range(2)], axis=0)
        hi, lo = parts(second)
        rows = jnp.dot(t_fro[...], jnp.concatenate([hi, hi, lo], axis=0), preferred_element_type=F32)
        for i in range(2):
            for m in range(4):
                g32[pl.ds(4 * i + m, H, stride=8), :] = rows[i * H:(i + 1) * H, m * 128:(m + 1) * 128]
        bsend[...] = g32[...].reshape(H, 8, 128).astype(BF)

        for dx, dy, dz, dk in OTHERS:
            dl, dc = groups[dz][dy] * 2 + cores[dk], xs[dx]

            @pl.when(dc < OWN)
            def _(dl=dl, dc=dc):
                pltpu.make_async_remote_copy(
                    bsend.at[dl * OWN + dc], brecv.at[2 * c + blk, l // 2], b_s, b_r,
                    device_id=(dl, dc), device_id_type=MESH).start()

        @pl.when(owner)
        def _():
            pltpu.make_async_copy(bsend.at[row], brecv.at[2 * c + blk, l // 2], b_r).start()

            @pl.when(s == 0)
            def _():
                weights_2(1)
                weights_1(3)
                sent_weights(3)
                send_state()
                weights_2(2)
                weights_3(0)
                weights_3(1)
                weights_2(3)
                own_row()
                weights_3(2)

            pltpu.make_async_copy(brecv, brecv, b_r).wait()

            packed = jnp.concatenate(
                [brecv[b].reshape(128, 128)[:, 0:BS].astype(F32) for b in range(NB)], axis=1).astype(BF)
            packed = jnp.concatenate([packed, packed], axis=0)
            v = x[...] + jnp.dot(back[...], packed, preferred_element_type=F32) * SCALE
            x[...] = v
            @pl.when(s == STEPS - 1)
            def _():
                hand_out(early, earlies, e_s, e_r)
                for j in range(NC):
                    xin[j] = xin[j] + early[j].astype(F32)

            nb[...] = norm(v, par[1:2, :], par[3:4, :]).astype(BF)

            @pl.when(s == 0)
            def _():
                weights_3(3)
                weights_4(0)
                weights_4(1)

            def up_part(q):
                for j in range(3):
                    cols = slice(j * 256, (j + 1) * 256)
                    weight = wts[q, 0, :, :, :, :, cols].reshape(D, 256)
                    pre = jnp.dot(nb[...], weight, preferred_element_type=F32) + smalls[q, 5:6, cols]
                    act = 0.5 * pre * (1.0 + lax.erf(pre * math.sqrt(0.5)))
                    hid[:, q * 768 + j * 256:q * 768 + (j + 1) * 256] = act.astype(BF)

            def down_part(q):
                for j in range(3):
                    cols = slice(j * 256, (j + 1) * 256)
                    weight = wts[q, 1, :, :, :, :, cols].reshape(D, 256)
                    mixed = jnp.dot(hid[:, q * 768:(q + 1) * 768], weight, preferred_element_type=F32)
                    if q == 0:
                        mixed = mixed + par[4:5, cols]
                    x[:, cols] = x[:, cols] + mixed

            up_part(0)
            for q in range(1, NC):
                up_part(q)
                down_part(q - 1)
            down_part(NC - 1)

            @pl.when(s < STEPS - 1)
            def _():
                sent_f(s)
                send_row()

            pltpu.make_async_copy(bsend.at[0:95], bsend.at[0:95], b_s).wait()

        @pl.when(jnp.logical_not(owner))
        def _():
            @pl.when(s == 0)
            def _():
                sent_weights(3)
                send_state()
                sent_f(s)

            pltpu.make_async_copy(bsend, bsend, b_s).wait()

        return carry

    def sent_f(s):
        @pl.when(s == 0)
        def _():
            pltpu.make_async_copy(bsend.at[0:93], bsend.at[0:93], f_s).wait()

        @pl.when(s > 0)
        def _():
            pltpu.make_async_copy(fsend.at[0:7], fsend.at[0:7], f_s).wait()
            pltpu.make_async_copy(fsend.at[7, 0:15], fsend.at[7, 0:15], f_s).wait()

    lax.fori_loop(0, STEPS, step, 0)

    @pl.when(owner)
    def _():
        sent_f(1)
        ref = wts.at[pl.ds(0, 3), 0]
        pltpu.make_async_copy(ref, ref, wd_s).wait()
        for t in range(4):
            for axis in range(2):
                take(wb_s, t, axis)
            take(wc_s, t)

    for i in range(OWN):
        @pl.when(c != i)
        def _(i=i):
            a, b = to_owner(i)
            a.wait_send()
            b.wait_send()

    for j in range(NC):
        @pl.when(c != j)
        def _(j=j):
            pltpu.make_async_copy(stat, stat, st_s.at[j]).wait()

    @pl.when(owner)
    def _():
        hand_out(late, lates, o_s, o_r)

    for i in range(OWN):
        pltpu.make_async_copy(earlies.at[i], earlies.at[i], e_r.at[i]).wait()
        state[i] = state[i] + earlies[i].astype(F32)
    for i in range(OWN):
        pltpu.make_async_copy(lates.at[i], lates.at[i], o_r.at[i]).wait()
        out[i] = (state[i] + lates[i].astype(F32)).reshape(W, 1, 192)

    @pl.when(owner)
    def _():
        for j in range(NC):
            @pl.when(c != j)
            def _(j=j):
                pltpu.make_async_copy(early.at[0], early.at[0], e_s.at[j]).wait()
                pltpu.make_async_copy(late.at[0], late.at[0], o_s.at[j]).wait()


def local(
    state, norm_gains, channel_biases, filter_in, filter_in_bias, filter_out, filter_out_bias,
    up_weight, up_bias, down_weight,
):
    up = up_weight.reshape(2, 4, 2, 48, 768)
    down = down_weight.reshape(2, 4, 2, 48, 768)
    fwd, back, t_to, t_fro = tables()
    vm = pl.BlockSpec(memory_space=pltpu.VMEM)
    hbm = pl.BlockSpec(memory_space=pltpu.HBM)
    sem = pltpu.SemaphoreType.DMA
    result = pl.pallas_call(
        kernel,
        out_shape=jax.ShapeDtypeStruct((OWN, W, 1, 192), F32),
        in_specs=[hbm] * 14,
        out_specs=vm,
        scratch_shapes=[
            pltpu.VMEM((OWN, W, 1, 192), F32),
            pltpu.VMEM((OWN, W, 192), F32),
            pltpu.VMEM((2, 192), BF),
            pltpu.VMEM((3, 192), BF),
            pltpu.VMEM((2, 2, BS, BS), F32),
            pltpu.VMEM((2, 2, BS), F32),
            pltpu.VMEM((2, 2, BS, BS), F32),
            pltpu.VMEM((2, 2, BS), F32),
            pltpu.VMEM((D,), BF),
            pltpu.VMEM((128, 3 * R), BF),
            pltpu.VMEM((R, 256), BF),
            pltpu.VMEM((192, 384), BF),
            pltpu.VMEM((192, 576), BF),
            pltpu.VMEM((8, D), F32),
            sem((12,)),
            pltpu.VMEM((NC, W, 192), F32),
            pltpu.VMEM((NC, W, 192), BF),
            pltpu.VMEM((NC, W, 192), BF),
            pltpu.VMEM((OWN, W, 192), BF),
            pltpu.VMEM((OWN, W, 192), BF),
            pltpu.VMEM((NC, 8, D), F32),
            pltpu.VMEM((R, D), F32),
            pltpu.VMEM((R, D), BF),
            pltpu.VMEM((NB, G, 8, 128), BF),
            pltpu.VMEM((H, 8, 128), BF),
            pltpu.VMEM((H, 8, 128), BF),
            pltpu.VMEM((NB, G, 8, 128), BF),
            pltpu.VMEM((768, 256), BF),
            pltpu.VMEM((1, 256), F32),
            pltpu.VMEM((768, 256), BF),
            pltpu.VMEM((1, 256), F32),
            pltpu.VMEM((8, D), F32),
            pltpu.VMEM((R, FF), BF),
            pltpu.VMEM((768, 128), F32),
            pltpu.VMEM((3 * R, D), BF),
            pltpu.VMEM((NC, 2, 2, 4, 2, 48, 768), BF),
            pltpu.VMEM((640, 128), F32),
            pltpu.VMEM((8, 640), F32),
            pltpu.VMEM((NC, 8, 640), F32),
            sem((OWN,)), sem((NC,)), sem((OWN,)), sem((NC,)),
            sem, sem, sem, sem, sem((NC,)), sem((OWN,)),
            sem((2,)), sem((4, OWN)), sem((4,)), sem((4, 2)), sem((4, 2)), sem((4,)), sem((4,)), sem, sem((4, 4)), sem((NC,)), sem((NC,)), sem((NC,)), sem((OWN,)),
        ],
        compiler_params=pltpu.CompilerParams(
            collective_id=0, has_side_effects=True, vmem_limit_bytes=62 * 1024 * 1024),
        name="rollout",
    )(
        state.reshape(OWN, W, 1, 192), norm_gains, channel_biases, filter_in, filter_in_bias, filter_out, filter_out_bias,
        up, up_bias, down, jnp.asarray(fwd), jnp.asarray(back), jnp.asarray(t_to), jnp.asarray(t_fro),
    )
    return result.reshape(1, OWN, W, 192)


def solution(mesh):
    placed = (
        P(None, "lat", None, "ch"),
        P(None, "ch"),
        P(None, "ch"),
        P(None, "ch", None, None),
        P(None, "ch", None),
        P(None, "ch", None, None),
        P(None, "ch", None),
        P(None, "ch"),
        P("ch"),
        P("ch", None),
    )
    return jax.shard_map(
        local, mesh=mesh, in_specs=placed, out_specs=P(None, "lat", None, "ch"), check_vma=False
    )
```

```python
import itertools
import math

import jax
import jax.numpy as jnp
import numpy as np
from jax import lax
from jax.experimental import pallas as pl
from jax.experimental.pallas import tpu as pltpu
from jax.sharding import PartitionSpec as P

D = 768
FF = 3072
W = 180
R = 192
H = 96
M = 64
NB = 8
BS = 96
STEPS = 4
NL = 32
NC = 4
ND = NL * NC
OWN = 3
G = 16
SCALE = 1.0 / math.sqrt(H * W)
EPS = 1e-05
SHRINK = 0.01
HOPS = (0, 1, 2, 1)
OTHERS = sorted(
    (o for o in itertools.product(range(4), range(4), range(4), range(2)) if any(o)),
    key=lambda o: -(HOPS[o[0]] + HOPS[o[1]] + HOPS[o[2]] + 0.3 * o[3]),
)
MESH = pl.DeviceIdType.MESH
BF = jnp.bfloat16
F32 = jnp.float32


def tables():
    modes = np.arange(M)
    w = np.arange(W)
    ang = 2.0 * np.pi / W * ((w[:, None] * modes[None, :]) % W)
    c, s = np.cos(ang), np.sin(ang)
    dbl = np.where(modes == 0, 1.0, 2.0)
    fwd = np.zeros((G, 2, 4, R))
    fwd[:, 0, :, :W] = c.T.reshape(G, 4, W)
    fwd[:, 1, :, :W] = -s.T.reshape(G, 4, W)
    back = np.zeros((R, G, 2, 4))
    back[:W, :, 0, :] = (c * dbl).reshape(W, G, 4)
    back[:W, :, 1, :] = -(s * dbl).reshape(W, G, 4)
    h = np.arange(H)
    ang = 2.0 * np.pi / H * ((h[:, None] * h[None, :]) % H)
    c, s = np.cos(ang), np.sin(ang)
    to = np.block([[c, s], [-s, c]])
    fro = to.T
    fwd, back = halves(fwd.reshape(128, R)), halves(back.reshape(R, 128))
    return (
        np.concatenate([fwd[0], fwd[1], fwd[0]], axis=1),
        np.concatenate(back, axis=1),
        np.concatenate(halves(to), axis=1),
        np.concatenate([halves(fro)[0], halves(fro)[1], halves(fro)[0]], axis=1),
    )


def halves(a):
    a = np.asarray(a, np.float32)
    hi = a.astype(BF)
    return hi, (a - hi.astype(np.float32)).astype(BF)


def parts(v):
    hi = v.astype(BF)
    return hi, (v - hi.astype(F32)).astype(BF)


def norm(v, gain, shift):
    mean = jnp.sum(v, -1, keepdims=True) / D
    spread = jnp.sum(v * v, -1, keepdims=True) / D - mean * mean
    return (v - mean) * lax.rsqrt(spread + EPS) * gain + shift


def kernel(
    state_h, gains_h, biases_h, fin_h, finb_h, fout_h, foutb_h, up, upb_h, down, fwd_h, back_h, to_h, fro_h,
    out,
    lines, state, gains, biases, fin, finb, fout, foutb, upb, fwd, back, t_to, t_fro, small, h_s,
    xin, early, late, earlies, lates, smalls, x, nb, fsend, frecv, bsend, brecv, w1, b1, w2, b2, par, hid, g32, n3, wts, tall, stat, stats,
    in_s, in_r, sm_s, sm_r, f_s, f_r, b_s, b_r, o_s, o_r,
    own_r, wa_s, wa_r, wb_s, wb_r, wc_s, wc_r, wd_s, wd_r, st_s, st_r, e_s, e_r,
):
    l = lax.axis_index("lat")
    c = lax.axis_index("ch")
    me = l * NC + c
    row = l * OWN + c
    blk = lax.rem(l, 2)
    owner = c < OWN

    k = lax.rem(l, 2)
    cy = lax.rem(l // 2, 4)
    cz = l // 8
    xs = [lax.rem(c + i, 4) for i in range(4)]
    groups = [[lax.rem(cz + i, 4) * 4 + lax.rem(cy + j, 4) for j in range(4)] for i in range(4)]
    cores = (k, 1 - k)

    fetches = [
        pltpu.make_async_copy(src, dst, h_s.at[i])
        for i, (src, dst) in enumerate((
            (to_h, t_to), (fro_h, t_fro), (fin_h, fin), (fout_h, fout), (finb_h, finb), (foutb_h, foutb),
            (gains_h, gains), (biases_h, biases), (upb_h, upb), (fwd_h, fwd), (back_h, back), (state_h, lines)))
    ]
    for fetch in fetches:
        fetch.start()

    barrier = pltpu.get_barrier_semaphore()
    for dx, dy, dz, dk in OTHERS:
        pl.semaphore_signal(
            barrier, inc=1, device_id=(groups[dz][dy] * 2 + cores[dk], xs[dx]), device_id_type=MESH)

    def to_owner(i):
        return (
            pltpu.make_async_remote_copy(
                state.at[i], xin.at[c], in_s.at[i], in_r.at[c],
                device_id=(l, i), device_id_type=MESH),
            pltpu.make_async_remote_copy(
                small, smalls.at[c], sm_s.at[i], sm_r.at[c],
                device_id=(l, i), device_id_type=MESH),
        )

    py, pz = lax.rem(cy, 2), lax.rem(cz, 2)
    mine = 2 * pz + py
    at_y, at_z, at_d = 2 * pz + 1 - py, 2 * (1 - pz) + py, 2 * (1 - pz) + 1 - py
    shards = (up, down)

    def foreign(j):
        return lax.rem(c + 1 + j, NC)

    three = wts.at[0, 0, 0, pl.ds(0, 3), 0]

    def take(sems, *at):
        pltpu.make_async_copy(three, three, sems.at[at] if at else sems).wait()

    def pass_on(t, piece, axis, s_sem, r_sem):
        for j in range(3):
            for half, sign in ((0, 1), (1, 3)):
                ref = wts.at[foreign(j), t // 2, k, piece, t % 2, :, pl.ds(half * 384, 384)]
                to = groups[(0, sign)[axis]][(sign, 0)[axis]] * 2 + k
                pltpu.make_async_remote_copy(
                    ref, ref, s_sem, r_sem, device_id=(to, c), device_id_type=MESH).start()

    def share(t, piece, stage):
        for j in range(3):
            ref = wts.at[foreign(j), t // 2, k, piece, t % 2]
            pltpu.make_async_remote_copy(
                ref, ref, wd_s, wd_r.at[t, stage], device_id=(groups[0][0] * 2 + 1 - k, c),
                device_id_type=MESH).start()

    @pl.when(owner)
    def _():
        for m in range(2):
            pltpu.make_async_copy(shards[m], wts.at[c, m], own_r.at[m]).start()

    def weights_0(t):
        for i in range(OWN):
            @pl.when(c != i)
            def _(i=i):
                pltpu.make_async_remote_copy(
                    shards[t // 2].at[k, mine, t % 2], wts.at[c, t // 2, k, mine, t % 2],
                    wa_s.at[t, i], wa_r.at[t], device_id=(l, i), device_id_type=MESH).start()

    def sent_weights(t):
        for i in range(OWN):
            @pl.when(c != i)
            def _(i=i):
                ref = shards[t // 2].at[k, mine, t % 2]
                pltpu.make_async_copy(ref, ref, wa_s.at[t, i]).wait()

    def weights_1(t):
        take(wa_r, t)
        for axis in range(2):
            pass_on(t, mine, axis, wb_s.at[t, axis], wb_r.at[t, axis])
        share(t, mine, 0)

    def weights_2(t):
        u = t % 2
        take(wb_r, t, 1 - u)
        pass_on(t, (at_z, at_y)[u], u, wc_s.at[t], wc_r.at[t])
        share(t, (at_z, at_y)[u], 2)
        take(wb_r, t, u)
        share(t, (at_y, at_z)[u], 1)

    def weights_3(t):
        take(wc_r, t)
        share(t, at_d, 3)

    def weights_4(m):
        pltpu.make_async_copy(wts.at[c, m], wts.at[c, m], own_r.at[m]).wait()
        for t in (2 * m, 2 * m + 1):
            for stage in range(4):
                take(wd_r, t, stage)

    fsend[...] = jnp.zeros_like(fsend)
    n3[...] = jnp.zeros_like(n3)
    tall[...] = jnp.zeros_like(tall)
    small[...] = jnp.zeros_like(small)
    for fetch in fetches:
        fetch.wait()
    state[...] = lines[...].reshape(OWN, W, 192)
    small[0:2, 0:192] = gains[...].astype(F32)
    small[2:5, 0:192] = biases[...].astype(F32)
    small[5:6, :] = upb[...].astype(F32).reshape(1, D)
    for w_ref, b_ref, src, bsrc in ((w1, b1, fin, finb), (w2, b2, fout, foutb)):
        w_ref[...] = jnp.zeros_like(w_ref)
        b_ref[...] = jnp.zeros_like(b_ref)
        for at, re, im in zip((0, 256), parts(src[0, blk]), parts(src[1, blk])):
            w_ref[at:at + BS, 0:BS] = re
            w_ref[at:at + BS, 128:128 + BS] = im
            w_ref[at + 128:at + 128 + BS, 0:BS] = -im
            w_ref[at + 128:at + 128 + BS, 128:128 + BS] = re
        w_ref[512:768, :] = w_ref[0:256, :]
        b_ref[:, 0:BS] = bsrc[0, pl.ds(blk, 1), :]
        b_ref[:, 128:128 + BS] = bsrc[1, pl.ds(blk, 1), :]


    lane = lax.broadcasted_iota(jnp.int32, (W, 128), 1)
    for r in range(OWN):
        v = state[r]
        total = jnp.sum(v, -1, keepdims=True)
        squares = jnp.sum(v * v, -1, keepdims=True)
        tall[r * R:r * R + W, :] = jnp.where(lane == 0, total, jnp.where(lane == 1, squares, 0.0))
    stat[...] = tall[...].T[0:8, :]

    pl.semaphore_wait(barrier, ND - 1)
    for j in range(NC):
        @pl.when(c != j)
        def _(j=j):
            pltpu.make_async_remote_copy(
                stat, stats.at[c], st_s.at[j], st_r.at[c], device_id=(l, j), device_id_type=MESH).start()

        @pl.when(c == j)
        def _(j=j):
            pltpu.make_async_copy(stat, stats.at[j], st_r.at[j]).start()

    weights_0(0)
    for j in range(NC):
        pltpu.make_async_copy(stats.at[j], stats.at[j], st_r.at[j]).wait()
    weights_0(1)
    total = (stats[0] + stats[1]) + (stats[2] + stats[3])
    mean = total[0:1] / D
    spread = lax.rsqrt(total[1:2] / D - mean * mean + EPS)
    line = lax.broadcasted_iota(jnp.int32, (128, 640), 0)
    tall[...] = jnp.where(line == 0, mean, jnp.where(line == 1, spread, 0.0)).T
    for r in range(OWN):
        at = slice(r * R, r * R + W)
        n = (state[r] - tall[at, 0:1]) * tall[at, 1:2] * small[0:1, 0:192] + small[2:3, 0:192]
        hi, lo = parts(n)
        n3[0:W, 0:192] = hi
        n3[R:R + W, 0:192] = hi
        n3[2 * R:2 * R + W, 0:192] = lo
        lon = jnp.dot(fwd[...], n3[:, 0:192], preferred_element_type=F32)
        for j in range(2):
            fsend[2 * r + j, :, :, 0:BS] = lon[:, j * BS:(j + 1) * BS].reshape(G, 8, BS).astype(BF)

    for dx, dy, dz, dk in OTHERS:
        if dx:
            continue
        for r in range(OWN):
            pltpu.make_async_remote_copy(
                fsend.at[2 * r + cores[dk], groups[dz][dy]], frecv.at[l * OWN + r], f_s, f_r,
                device_id=(groups[dz][dy] * 2 + cores[dk], c), device_id_type=MESH).start()
    for r in range(OWN):
        pltpu.make_async_copy(fsend.at[2 * r + blk, l // 2], frecv.at[l * OWN + r], f_r).start()
    sent_weights(0)
    pl.when(owner)(lambda: weights_1(0))
    sent_weights(1)
    weights_0(2)
    pl.when(owner)(lambda: weights_1(1))

    def hand_out(src, dst, s_sems, r_sems, sent=None):
        for j in range(NC):
            have = xin[j] if sent is None else xin[j] + sent[j].astype(F32)
            src[j] = (x[0:W, j * 192:(j + 1) * 192] - have).astype(BF)
        for j in range(NC):
            @pl.when(c != j)
            def _(j=j):
                pltpu.make_async_remote_copy(
                    src.at[j], dst.at[c], s_sems.at[j], r_sems.at[c],
                    device_id=(l, j), device_id_type=MESH).start()

        pltpu.make_async_copy(src.at[c], dst.at[c], r_sems.at[c]).start()

    def send_state():
        for i in range(OWN):
            @pl.when(c != i)
            def _(i=i):
                a, b = to_owner(i)
                a.start()
                b.start()

            @pl.when(c == i)
            def _(i=i):
                pltpu.make_async_copy(state.at[i], xin.at[i], in_r.at[i]).start()
                pltpu.make_async_copy(small, smalls.at[i], sm_r.at[i]).start()

    def own_row():
        for j in range(NC):
            pltpu.make_async_copy(xin.at[j], xin.at[j], in_r.at[j]).wait()
            pltpu.make_async_copy(smalls.at[j], smalls.at[j], sm_r.at[j]).wait()
        par[0:5, :] = jnp.concatenate([smalls[j, 0:5, 0:192] for j in range(NC)], axis=1)
        v = jnp.concatenate([xin[j] for j in range(NC)], axis=1)
        x[0:W, :] = v + norm(v, par[0:1, :], par[2:3, :])
        x[W:R, :] = jnp.zeros((R - W, D), F32)

    def send_row():
        v = x[...]
        n = norm(v, par[0:1, :], par[2:3, :])
        x[...] = v + n
        hi, lo = parts(n)
        n3[0:R, :] = hi
        n3[R:2 * R, :] = hi
        n3[2 * R:3 * R, :] = lo
        lon = jnp.dot(fwd[...], n3[...], preferred_element_type=F32)
        for b in range(NB):
            fsend[b, :, :, 0:BS] = lon[:, b * BS:(b + 1) * BS].reshape(G, 8, BS).astype(BF)

        for dx, dy, dz, dk in OTHERS:
            pltpu.make_async_remote_copy(
                fsend.at[2 * xs[dx] + cores[dk], groups[dz][dy]], frecv.at[row], f_s, f_r,
                device_id=(groups[dz][dy] * 2 + cores[dk], xs[dx]), device_id_type=MESH).start()
        pltpu.make_async_copy(
            fsend.at[2 * c + blk, l // 2], frecv.at[row], f_r).start()

    def step(s, carry):
        pltpu.make_async_copy(frecv, frecv, f_r).wait()

        @pl.when(s == 0)
        def _():
            sent_weights(2)
            weights_0(3)

            @pl.when(owner)
            def _():
                weights_2(0)
                weights_1(2)


        g32[...] = frecv[...].reshape(H * 8, 128).astype(F32)
        got = jnp.concatenate(
            [jnp.concatenate([g32[pl.ds(4 * i + m, H, stride=8), :] for m in range(4)], axis=1) for i in range(2)],
            axis=0).astype(BF)
        got = jnp.concatenate([got, got], axis=0)
        spec = jnp.dot(t_to[...], got, preferred_element_type=F32) * SCALE
        spec = jnp.concatenate(
            [jnp.concatenate([spec[i * H:(i + 1) * H, m * 128:(m + 1) * 128] for i in range(2)], axis=1)
             for m in range(4)], axis=0)
        hi, lo = parts(spec)
        first = jnp.dot(jnp.concatenate([hi, hi, lo], axis=1), w1[...], preferred_element_type=F32) + b1[...]
        hi, lo = parts(jnp.maximum(first, 0.0))
        second = jnp.dot(jnp.concatenate([hi, hi, lo], axis=1), w2[...], preferred_element_type=F32) + b2[...]
        second = jnp.where(second > SHRINK, second - SHRINK,
                           jnp.where(second < -SHRINK, second + SHRINK, 0.0))
        second = jnp.concatenate(
            [jnp.concatenate([second[m * H:(m + 1) * H, i * 128:(i + 1) * 128] for m in range(4)], axis=1)
             for i in range(2)], axis=0)
        hi, lo = parts(second)
        rows = jnp.dot(t_fro[...], jnp.concatenate([hi, hi, lo], axis=0), preferred_element_type=F32)
        for i in range(2):
            for m in range(4):
                g32[pl.ds(4 * i + m, H, stride=8), :] = rows[i * H:(i + 1) * H, m * 128:(m + 1) * 128]
        bsend[...] = g32[...].reshape(H, 8, 128).astype(BF)

        for dx, dy, dz, dk in OTHERS:
            dl, dc = groups[dz][dy] * 2 + cores[dk], xs[dx]

            @pl.when(dc < OWN)
            def _(dl=dl, dc=dc):
                pltpu.make_async_remote_copy(
                    bsend.at[dl * OWN + dc], brecv.at[2 * c + blk, l // 2], b_s, b_r,
                    device_id=(dl, dc), device_id_type=MESH).start()

        @pl.when(owner)
        def _():
            pltpu.make_async_copy(bsend.at[row], brecv.at[2 * c + blk, l // 2], b_r).start()

            @pl.when(s == 0)
            def _():
                weights_2(1)
                weights_1(3)
                sent_weights(3)
                send_state()
                weights_2(2)
                weights_3(0)
                weights_3(1)
                weights_2(3)
                own_row()
                weights_3(2)

            pltpu.make_async_copy(brecv, brecv, b_r).wait()

            packed = jnp.concatenate(
                [brecv[b].reshape(128, 128)[:, 0:BS].astype(F32) for b in range(NB)], axis=1).astype(BF)
            packed = jnp.concatenate([packed, packed], axis=0)
            v = x[...] + jnp.dot(back[...], packed, preferred_element_type=F32) * SCALE
            x[...] = v
            @pl.when(s == STEPS - 1)
            def _():
                hand_out(early, earlies, e_s, e_r)

            nb[...] = norm(v, par[1:2, :], par[3:4, :]).astype(BF)

            @pl.when(s == 0)
            def _():
                weights_3(3)
                weights_4(0)
                weights_4(1)

            def up_part(q):
                for j in range(3):
                    cols = slice(j * 256, (j + 1) * 256)
                    weight = wts[q, 0, :, :, :, :, cols].reshape(D, 256)
                    pre = jnp.dot(nb[...], weight, preferred_element_type=F32) + smalls[q, 5:6, cols]
                    act = 0.5 * pre * (1.0 + lax.erf(pre * math.sqrt(0.5)))
                    hid[:, q * 768 + j * 256:q * 768 + (j + 1) * 256] = act.astype(BF)

            def down_part(q):
                for j in range(3):
                    cols = slice(j * 256, (j + 1) * 256)
                    weight = wts[q, 1, :, :, :, :, cols].reshape(D, 256)
                    mixed = jnp.dot(hid[:, q * 768:(q + 1) * 768], weight, preferred_element_type=F32)
                    if q == 0:
                        mixed = mixed + par[4:5, cols]
                    x[:, cols] = x[:, cols] + mixed

            up_part(0)
            for q in range(1, NC):
                up_part(q)
                down_part(q - 1)
            down_part(NC - 1)

            @pl.when(s < STEPS - 1)
            def _():
                sent_f(s)
                send_row()

            pltpu.make_async_copy(bsend.at[0:95], bsend.at[0:95], b_s).wait()

        @pl.when(jnp.logical_not(owner))
        def _():
            @pl.when(s == 0)
            def _():
                sent_weights(3)
                send_state()
                sent_f(s)

            pltpu.make_async_copy(bsend, bsend, b_s).wait()

        return carry

    def sent_f(s):
        @pl.when(s == 0)
        def _():
            pltpu.make_async_copy(bsend.at[0:93], bsend.at[0:93], f_s).wait()

        @pl.when(s > 0)
        def _():
            pltpu.make_async_copy(fsend.at[0:7], fsend.at[0:7], f_s).wait()
            pltpu.make_async_copy(fsend.at[7, 0:15], fsend.at[7, 0:15], f_s).wait()

    lax.fori_loop(0, STEPS, step, 0)

    @pl.when(owner)
    def _():
        sent_f(1)
        ref = wts.at[pl.ds(0, 3), 0]
        pltpu.make_async_copy(ref, ref, wd_s).wait()
        for t in range(4):
            for axis in range(2):
                take(wb_s, t, axis)
            take(wc_s, t)

    for i in range(OWN):
        @pl.when(c != i)
        def _(i=i):
            a, b = to_owner(i)
            a.wait_send()
            b.wait_send()

    for j in range(NC):
        @pl.when(c != j)
        def _(j=j):
            pltpu.make_async_copy(stat, stat, st_s.at[j]).wait()

    @pl.when(owner)
    def _():
        hand_out(late, lates, o_s, o_r, early)

    for i in range(OWN):
        pltpu.make_async_copy(earlies.at[i], earlies.at[i], e_r.at[i]).wait()
        state[i] = state[i] + earlies[i].astype(F32)
    for i in range(OWN):
        pltpu.make_async_copy(lates.at[i], lates.at[i], o_r.at[i]).wait()
        out[i] = (state[i] + lates[i].astype(F32)).reshape(W, 1, 192)

    @pl.when(owner)
    def _():
        for j in range(NC):
            @pl.when(c != j)
            def _(j=j):
                pltpu.make_async_copy(early.at[0], early.at[0], e_s.at[j]).wait()
                pltpu.make_async_copy(late.at[0], late.at[0], o_s.at[j]).wait()


def local(
    state, norm_gains, channel_biases, filter_in, filter_in_bias, filter_out, filter_out_bias,
    up_weight, up_bias, down_weight,
):
    up = up_weight.reshape(2, 4, 2, 48, 768)
    down = down_weight.reshape(2, 4, 2, 48, 768)
    fwd, back, t_to, t_fro = tables()
    vm = pl.BlockSpec(memory_space=pltpu.VMEM)
    hbm = pl.BlockSpec(memory_space=pltpu.HBM)
    sem = pltpu.SemaphoreType.DMA
    result = pl.pallas_call(
        kernel,
        out_shape=jax.ShapeDtypeStruct((OWN, W, 1, 192), F32),
        in_specs=[hbm] * 14,
        out_specs=vm,
        scratch_shapes=[
            pltpu.VMEM((OWN, W, 1, 192), F32),
            pltpu.VMEM((OWN, W, 192), F32),
            pltpu.VMEM((2, 192), BF),
            pltpu.VMEM((3, 192), BF),
            pltpu.VMEM((2, 2, BS, BS), F32),
            pltpu.VMEM((2, 2, BS), F32),
            pltpu.VMEM((2, 2, BS, BS), F32),
            pltpu.VMEM((2, 2, BS), F32),
            pltpu.VMEM((D,), BF),
            pltpu.VMEM((128, 3 * R), BF),
            pltpu.VMEM((R, 256), BF),
            pltpu.VMEM((192, 384), BF),
            pltpu.VMEM((192, 576), BF),
            pltpu.VMEM((8, D), F32),
            sem((12,)),
            pltpu.VMEM((NC, W, 192), F32),
            pltpu.VMEM((NC, W, 192), BF),
            pltpu.VMEM((NC, W, 192), BF),
            pltpu.VMEM((OWN, W, 192), BF),
            pltpu.VMEM((OWN, W, 192), BF),
            pltpu.VMEM((NC, 8, D), F32),
            pltpu.VMEM((R, D), F32),
            pltpu.VMEM((R, D), BF),
            pltpu.VMEM((NB, G, 8, 128), BF),
            pltpu.VMEM((H, 8, 128), BF),
            pltpu.VMEM((H, 8, 128), BF),
            pltpu.VMEM((NB, G, 8, 128), BF),
            pltpu.VMEM((768, 256), BF),
            pltpu.VMEM((1, 256), F32),
            pltpu.VMEM((768, 256), BF),
            pltpu.VMEM((1, 256), F32),
            pltpu.VMEM((8, D), F32),
            pltpu.VMEM((R, FF), BF),
            pltpu.VMEM((768, 128), F32),
            pltpu.VMEM((3 * R, D), BF),
            pltpu.VMEM((NC, 2, 2, 4, 2, 48, 768), BF),
            pltpu.VMEM((640, 128), F32),
            pltpu.VMEM((8, 640), F32),
            pltpu.VMEM((NC, 8, 640), F32),
            sem((OWN,)), sem((NC,)), sem((OWN,)), sem((NC,)),
            sem, sem, sem, sem, sem((NC,)), sem((OWN,)),
            sem((2,)), sem((4, OWN)), sem((4,)), sem((4, 2)), sem((4, 2)), sem((4,)), sem((4,)), sem, sem((4, 4)), sem((NC,)), sem((NC,)), sem((NC,)), sem((OWN,)),
        ],
        compiler_params=pltpu.CompilerParams(
            collective_id=0, has_side_effects=True, vmem_limit_bytes=62 * 1024 * 1024),
        name="rollout",
    )(
        state.reshape(OWN, W, 1, 192), norm_gains, channel_biases, filter_in, filter_in_bias, filter_out, filter_out_bias,
        up, up_bias, down, jnp.asarray(fwd), jnp.asarray(back), jnp.asarray(t_to), jnp.asarray(t_fro),
    )
    return result.reshape(1, OWN, W, 192)


def solution(mesh):
    placed = (
        P(None, "lat", None, "ch"),
        P(None, "ch"),
        P(None, "ch"),
        P(None, "ch", None, None),
        P(None, "ch", None),
        P(None, "ch", None, None),
        P(None, "ch", None),
        P(None, "ch"),
        P("ch"),
        P("ch", None),
    )
    return jax.shard_map(
        local, mesh=mesh, in_specs=placed, out_specs=P(None, "lat", None, "ch"), check_vma=False
    )
```
